8 devices in a mesh: ens: 1 (over z), part: 2 (over y), feat: 4 (over x, core).
Axes of the slice: x: 2, y: 2, z: 1, core: 2. Of those that a mesh axis runs over, the one named last changes fastest.
Arguments:
- particles: float32 [2048, 28672], P(('ens', 'part'), 'feat')
- prec_diag: float32 [28672], P(('ens', 'feat'))
- target_mean: float32 [28672], P(('ens', 'feat'))
- low_factor: bfloat16 [28672, 32], P(('ens', 'feat'))
Outputs:
- output: float32 [2048, 28672], P(('ens', 'part'), 'feat')
All inputs are finite; a program needn't handle non-finite values.
Results may differ from the reference program's by a relative error of at most 0.00356208.
Values are sent between devices in bfloat16 or wider.
A program may use at most 1 GiB of HBM per device.

```python
import math
import jax
import jax.numpy as jnp

NUM_PARTICLES = 2048
FEAT_DIM = 28672
LOW_RANK = 32
NUM_STEPS = 3

KERN_WIDTH = 2.0 * FEAT_DIM / math.log(NUM_PARTICLES)
STEP_SIZE = 0.15 * NUM_PARTICLES * FEAT_DIM / math.log(NUM_PARTICLES)


def setup_inputs(seed: int = 0, part: int = 0) -> dict:
    part_key = jax.random.fold_in(jax.random.key(seed), part)
    sub_keys = jax.random.split(part_key, 6)
    scale_c = math.log(NUM_PARTICLES) / FEAT_DIM
    prec_diag = scale_c * jax.random.uniform(sub_keys[0], (FEAT_DIM,), jnp.float32, 0.5, 1.5)
    low_f32 = (math.sqrt(math.log(NUM_PARTICLES)) / FEAT_DIM) * jax.random.normal(sub_keys[1], (FEAT_DIM, LOW_RANK), jnp.float32)
    low_factor = low_f32.astype(jnp.bfloat16)
    target_mean = 0.5 * jax.random.normal(sub_keys[2], (FEAT_DIM,), jnp.float32)
    offset = 0.5 * jax.random.normal(sub_keys[3], (FEAT_DIM,), jnp.float32)
    spread = math.sqrt(0.5) * jax.random.normal(sub_keys[4], (NUM_PARTICLES, FEAT_DIM), jnp.float32)
    low_coeff = (FEAT_DIM / math.sqrt(2.0 * LOW_RANK * math.log(NUM_PARTICLES))) * jax.random.normal(sub_keys[5], (NUM_PARTICLES, LOW_RANK), jnp.float32)
    low_part = jnp.dot(low_coeff, low_factor.astype(jnp.float32).T)
    particles = target_mean[None, :] + offset[None, :] + spread + low_part
    return {"particles": particles, "prec_diag": prec_diag, "target_mean": target_mean, "low_factor": low_factor}


def svgd_step(cur_theta, prec_diag, target_mean, low_factor):
    x_dev = cur_theta - target_mean[None, :]
    proj_low = jnp.dot(x_dev.astype(jnp.bfloat16), low_factor, preferred_element_type=jnp.float32)
    low_term = jnp.dot(proj_low.astype(jnp.bfloat16), low_factor.T, preferred_element_type=jnp.float32)
    grad_b = (-(x_dev * prec_diag[None, :] + low_term)).astype(jnp.bfloat16)
    theta_b = cur_theta.astype(jnp.bfloat16)
    gram_mat = jnp.dot(theta_b, theta_b.T, preferred_element_type=jnp.float32)
    sq_norm = jnp.sum(jnp.square(theta_b.astype(jnp.float32)), axis=1)
    sq_dist = jnp.maximum(sq_norm[:, None] + sq_norm[None, :] - 2.0 * gram_mat, 0.0)
    kern_b = jnp.exp(-sq_dist / KERN_WIDTH).astype(jnp.bfloat16)
    row_mass = jnp.sum(kern_b.astype(jnp.float32), axis=1)
    drive_term = jnp.dot(kern_b, grad_b, preferred_element_type=jnp.float32)
    pull_term = jnp.dot(kern_b, theta_b, preferred_element_type=jnp.float32)
    update_dir = (drive_term + (2.0 / KERN_WIDTH) * (row_mass[:, None] * theta_b.astype(jnp.float32) - pull_term)) / NUM_PARTICLES
    return cur_theta + STEP_SIZE * update_dir


def reference(particles, prec_diag, target_mean, low_factor):
    cur_theta = particles
    for step_idx in range(NUM_STEPS):
        cur_theta = svgd_step(cur_theta, prec_diag, target_mean, low_factor)
    return cur_theta
```

```python
import functools
import math
import jax
import jax.numpy as jnp
from jax import lax
from jax.experimental import pallas as pl
from jax.experimental.pallas import tpu as pltpu
from jax.sharding import PartitionSpec as P

NUM_STEPS = 3
BLK = 256
BANDS = 5
MESH = pl.DeviceIdType.MESH
F32 = jnp.float32
BF16 = jnp.bfloat16
ANY = pl.BlockSpec(memory_space=pl.ANY)
VMEM = pl.BlockSpec(memory_space=pltpu.VMEM)
VMEM_LIMIT = 63 * 1024 * 1024
NT = (((1,), (1,)), ((), ()))


def band_dot(tb, row_blk, n_blk):
    rows = tb[row_blk * BLK:(row_blk + 1) * BLK, :]
    first = min(BANDS, n_blk - row_blk)
    parts = [(0, row_blk * BLK, first * BLK)]
    if first < BANDS:
        parts.append((first * BLK, 0, (BANDS - first) * BLK))
    for dst, src, width in parts:
        yield dst, width, lax.dot_general(rows, tb[src:src + width, :], NT, preferred_element_type=F32)


def exchange_kernel(n_chunk, theta_ref, mean_ref, fact_ref, col_ref, gram_ref, proj_ref,
                    buf, tb, send_sem, recv_sem, own_sem, put_sem, other_sem):
    part = lax.axis_index("part")
    other = 1 - part
    feat = lax.axis_index("feat")
    peer = (lax.axis_index("ens"), other, feat)
    rows, width = theta_ref.shape[0], col_ref.shape[1]
    n_rows = col_ref.shape[0]
    cw = width // n_chunk
    n_blk = n_rows // BLK
    barrier = pltpu.get_barrier_semaphore()
    pl.semaphore_signal(barrier, inc=1, device_id=peer, device_id_type=MESH)
    pl.semaphore_wait(barrier, 1)
    own_rows = pl.ds(pl.multiple_of(part * rows, BLK), rows)
    other_rows = pl.ds(pl.multiple_of(other * rows, BLK), rows)

    def remote(c):
        return pltpu.make_async_remote_copy(
            src_ref=theta_ref.at[:, pl.ds(pl.multiple_of(other * width + c * cw, 128), cw)],
            dst_ref=col_ref.at[own_rows, pl.ds(pl.multiple_of(c * cw, 128), cw)],
            send_sem=send_sem.at[c], recv_sem=recv_sem.at[c], device_id=peer, device_id_type=MESH)

    def fetch_own(c):
        return pltpu.make_async_copy(
            theta_ref.at[:, pl.ds(pl.multiple_of(part * width + c * cw, 128), cw)],
            buf.at[own_rows, :], own_sem)

    def put_own(c):
        return pltpu.make_async_copy(
            buf.at[own_rows, :], col_ref.at[own_rows, pl.ds(pl.multiple_of(c * cw, 128), cw)], put_sem)

    def fetch_other(c):
        return pltpu.make_async_copy(
            col_ref.at[other_rows, pl.ds(pl.multiple_of(c * cw, 128), cw)], buf.at[other_rows, :], other_sem)

    @pl.loop(0, n_chunk)
    def _(c):
        remote(c).start()

    gram_ref[...] = jnp.zeros_like(gram_ref)
    proj_ref[...] = jnp.zeros_like(proj_ref)

    @pl.loop(0, n_chunk)
    def _(c):
        fetch_own(c).start()
        fetch_own(c).wait()
        put_own(c).start()
        remote(c).wait_recv()
        fetch_other(c).start()
        fetch_other(c).wait()
        cols = pl.ds(pl.multiple_of(c * cw, 128), cw)
        fact = fact_ref[:, cols]
        mean = mean_ref[:, cols]

        @pl.loop(0, n_blk)
        def _(b):
            rs = pl.ds(pl.multiple_of(b * BLK, BLK), BLK)
            th = buf[rs, :]
            tb[rs, :] = th.astype(BF16)
            proj_ref[:, rs] += lax.dot_general(fact, (th - mean).astype(BF16), NT, preferred_element_type=F32)

        for b in range(n_blk):
            for dst, wd, val in band_dot(tb, b, n_blk):
                gram_ref[b, :, dst:dst + wd] += val
        put_own(c).wait()

    @pl.loop(0, n_chunk)
    def _(c):
        remote(c).wait_send()


def exchange(theta, mean, fact_t, n_chunk):
    rows, feat = theta.shape
    width = feat // 2
    n_rows = rows * 2
    rank = fact_t.shape[0]
    return pl.pallas_call(
        functools.partial(exchange_kernel, n_chunk),
        out_shape=(jax.ShapeDtypeStruct((n_rows, width), F32),
                   jax.ShapeDtypeStruct((n_rows // BLK, BLK, BANDS * BLK), F32),
                   jax.ShapeDtypeStruct((rank, n_rows), F32)),
        in_specs=[ANY, VMEM, VMEM], out_specs=(ANY, VMEM, VMEM),
        scratch_shapes=[
            pltpu.VMEM((n_rows, width // n_chunk), F32),
            pltpu.VMEM((n_rows, width // n_chunk), BF16),
            pltpu.SemaphoreType.DMA((n_chunk,)), pltpu.SemaphoreType.DMA((n_chunk,)),
            pltpu.SemaphoreType.DMA, pltpu.SemaphoreType.DMA, pltpu.SemaphoreType.DMA],
        compiler_params=pltpu.CompilerParams(collective_id=0, has_side_effects=True, vmem_limit_bytes=VMEM_LIMIT),
        name="exchange",
    )(theta, mean, fact_t)


def build_rhs(theta_ref, mean, prec, fact, zb_ref, rhs, rs):
    tile = theta_ref.shape[1]
    th = theta_ref[rs, :]
    low = jnp.dot(zb_ref[rs, :], fact, preferred_element_type=F32)
    rhs[rs, :tile] = (-((th - mean) * prec + low)).astype(BF16)
    rhs[rs, tile:] = th.astype(BF16)


def stepped(theta_ref, kern_ref, mass_ref, rhs, rs, inv_n, two_over_h, step_size):
    tile = theta_ref.shape[1]
    th = theta_ref[rs, :]
    acc = jnp.dot(kern_ref[rs, :], rhs[...], preferred_element_type=F32)
    pull = mass_ref[rs, :] * th.astype(BF16).astype(F32) - acc[:, tile:]
    return th + step_size * ((acc[:, :tile] + two_over_h * pull) * inv_n)


def update_kernel(consts, theta_ref, kern_ref, mass_ref, zb_ref, mean_ref, prec_ref, fact_ref,
                  out_ref, tb_ref, proj_ref, rhs):
    n_blk = theta_ref.shape[0] // BLK
    fact, mean, prec = fact_ref[...], mean_ref[...], prec_ref[...]

    @pl.when(pl.program_id(0) == 0)
    def _():
        proj_ref[...] = jnp.zeros_like(proj_ref)

    @pl.loop(0, n_blk)
    def _(b):
        build_rhs(theta_ref, mean, prec, fact, zb_ref, rhs, pl.ds(pl.multiple_of(b * BLK, BLK), BLK))

    @pl.loop(0, n_blk)
    def _(b):
        rs = pl.ds(pl.multiple_of(b * BLK, BLK), BLK)
        new = stepped(theta_ref, kern_ref, mass_ref, rhs, rs, *consts)
        out_ref[rs, :] = new
        tb_ref[rs, :] = new.astype(BF16)
        proj_ref[:, rs] += lax.dot_general(fact, (new - mean).astype(BF16), NT, preferred_element_type=F32)


def update(consts, theta, kern, mass, zb, mean, prec, fact_t, tile):
    n_rows, width = theta.shape
    rank = fact_t.shape[0]
    col = lambda r: pl.BlockSpec((r, tile), lambda i: (0, i))
    return pl.pallas_call(
        functools.partial(update_kernel, consts),
        grid=(width // tile,),
        out_shape=(jax.ShapeDtypeStruct((n_rows, width), F32),
                   jax.ShapeDtypeStruct((n_rows, width), BF16),
                   jax.ShapeDtypeStruct((rank, n_rows), F32)),
        in_specs=[col(n_rows), VMEM, VMEM, VMEM, col(1), col(1), col(rank)],
        out_specs=(col(n_rows), col(n_rows), VMEM),
        scratch_shapes=[pltpu.VMEM((n_rows, 2 * tile), BF16)],
        compiler_params=pltpu.CompilerParams(vmem_limit_bytes=VMEM_LIMIT),
        cost_estimate=pl.CostEstimate(flops=4 * n_rows * n_rows * width, bytes_accessed=10 * n_rows * width, transcendentals=0),
        name="update",
    )(theta, kern, mass, zb, mean, prec, fact_t)


def last_kernel(consts, pos_ref, theta_ref, kern_ref, mass_ref, zb_ref, mean_ref, prec_ref, fact_ref, *rest):
    out_ref, send_ref, rhs = rest[-3:]
    rows = out_ref.shape[0]
    n_blk = theta_ref.shape[0] // BLK
    part = pos_ref[0]
    fact, mean, prec = fact_ref[...], mean_ref[...], prec_ref[...]

    @pl.loop(0, n_blk)
    def _(b):
        build_rhs(theta_ref, mean, prec, fact, zb_ref, rhs, pl.ds(pl.multiple_of(b * BLK, BLK), BLK))

    for dst, which in ((send_ref, 1 - part), (out_ref, part)):
        @pl.loop(0, rows // BLK)
        def _(b):
            rs = pl.ds(pl.multiple_of(which * rows + b * BLK, BLK), BLK)
            dst[pl.ds(pl.multiple_of(b * BLK, BLK), BLK), :] = stepped(theta_ref, kern_ref, mass_ref, rhs, rs, *consts)


def last_update(consts, pos, theta, kern, mass, zb, mean, prec, fact_t, out, chunk, tile):
    n_rows, width = theta.shape
    rank = fact_t.shape[0]
    rows, feat = n_rows // 2, width * 2
    per = width // tile
    col = lambda r: pl.BlockSpec((r, tile), lambda i, pos: (0, chunk))
    in_specs = [col(n_rows), VMEM, VMEM, VMEM, col(1), col(1), col(rank)]
    args = [theta, kern, mass, zb, mean, prec, fact_t]
    alias = {}
    if out is not None:
        in_specs.append(ANY)
        args.append(out)
        alias = {8: 0}
    return pl.pallas_call(
        functools.partial(last_kernel, consts),
        grid_spec=pltpu.PrefetchScalarGridSpec(
            num_scalar_prefetch=1, grid=(1,), in_specs=in_specs,
            out_specs=(pl.BlockSpec((rows, tile), lambda i, pos: (0, pos[0] * per + chunk)),
                       pl.BlockSpec((rows, tile), lambda i, pos: (0, 0))),
            scratch_shapes=[pltpu.VMEM((n_rows, 2 * tile), BF16)]),
        out_shape=(jax.ShapeDtypeStruct((rows, feat), F32), jax.ShapeDtypeStruct((rows, tile), F32)),
        input_output_aliases=alias,
        compiler_params=pltpu.CompilerParams(vmem_limit_bytes=VMEM_LIMIT),
        cost_estimate=pl.CostEstimate(flops=4 * n_rows * n_rows * tile, bytes_accessed=10 * n_rows * tile, transcendentals=0),
        name=f"last_update_{chunk}",
    )(pos, *args)


def place_kernel(pos_ref, recv_ref, base_ref, out_ref):
    out_ref[...] = recv_ref[...]


def place(pos, recv, out, chunk):
    rows, tile = recv.shape
    per = out.shape[1] // (2 * tile)
    sub = tile // 128
    return pl.pallas_call(
        place_kernel,
        grid_spec=pltpu.PrefetchScalarGridSpec(
            num_scalar_prefetch=1, grid=(sub,), in_specs=[pl.BlockSpec((rows, 128), lambda i, pos: (0, i)), ANY],
            out_specs=pl.BlockSpec((rows, 128), lambda i, pos: (0, ((1 - pos[0]) * per + chunk) * sub + i))),
        out_shape=jax.ShapeDtypeStruct(out.shape, out.dtype),
        input_output_aliases={2: 0},
        cost_estimate=pl.CostEstimate(flops=1000 * rows * tile, bytes_accessed=8 * rows * tile, transcendentals=0),
        name=f"place_{chunk}",
    )(pos, recv, out)


def gram_kernel(tb_ref, gram_ref):
    n_blk = tb_ref.shape[0] // BLK
    for b in range(n_blk):
        @pl.when(pl.program_id(0) == b)
        def _():
            for dst, wd, val in band_dot(tb_ref, b, n_blk):
                gram_ref[0, :, dst:dst + wd] = val


def gram_bands(tb):
    n_rows, width = tb.shape
    n_blk = n_rows // BLK
    return pl.pallas_call(
        gram_kernel, grid=(n_blk,),
        out_shape=jax.ShapeDtypeStruct((n_blk, BLK, BANDS * BLK), F32),
        in_specs=[VMEM], out_specs=pl.BlockSpec((1, BLK, BANDS * BLK), lambda i: (i, 0, 0)),
        compiler_params=pltpu.CompilerParams(vmem_limit_bytes=VMEM_LIMIT),
        name="gram",
    )(tb)


def solution(mesh):
    part_size = mesh.shape["part"]
    feat_size = mesh.shape["feat"]

    def local_steps(theta, prec_loc, mean_loc, factor_loc):
        rows, feat_loc = theta.shape
        n_total = rows * part_size
        feat_total = feat_loc * feat_size
        width = feat_loc // part_size
        n_blk = n_total // BLK
        kern_width = 2.0 * feat_total / math.log(n_total)
        step_size = 0.15 * n_total * feat_total / math.log(n_total)
        consts = (1.0 / n_total, 2.0 / kern_width, step_size)
        part = lax.axis_index("part")
        me = part * feat_size + lax.axis_index("feat")
        pos = part.astype(jnp.int32).reshape(1)
        mean = lax.dynamic_slice_in_dim(mean_loc, part * width, width).reshape(1, width)
        prec = lax.dynamic_slice_in_dim(prec_loc, part * width, width).reshape(1, width)
        fact_t = lax.dynamic_slice_in_dim(factor_loc, part * width, width, axis=0).T
        tile = width // 7
        everyone = ("part", "feat")

        def kernel_matrix(gram, proj):
            diag = jnp.sum(gram[:, :, :BLK] * jnp.eye(BLK, dtype=F32), axis=1).reshape(1, n_total)
            sums = lax.psum(jnp.concatenate([proj, diag], axis=0), everyone)
            zb = sums[:-1].T.astype(BF16)
            sq = sums[-1]
            own = lax.psum_scatter(gram, everyone, scatter_dimension=0)
            sq_own = lax.dynamic_slice_in_dim(sq, me * BLK, BLK)
            sq_band = lax.dynamic_slice_in_dim(jnp.concatenate([sq, sq]), me * BLK, BANDS * BLK)
            dist = jnp.maximum(sq_own[:, None] + sq_band[None, :] - 2.0 * own, 0.0)
            kern_band = jnp.exp(-dist / kern_width).astype(BF16)
            bands = lax.all_gather(kern_band, everyone)
            kern_rows = []
            for i in range(n_blk):
                row = []
                for j in range(n_blk):
                    k = (j - i) % n_blk
                    if k < BANDS:
                        row.append(bands[i, :, k * BLK:(k + 1) * BLK])
                    else:
                        k = (i - j) % n_blk
                        row.append(bands[j, :, k * BLK:(k + 1) * BLK].T)
                kern_rows.append(jnp.concatenate(row, axis=1))
            kern = jnp.concatenate(kern_rows, axis=0)
            mass = jnp.sum(kern, axis=1, dtype=F32).reshape(n_total, 1)
            return kern, mass, zb

        cur, gram, proj = exchange(theta, mean, fact_t, 7)
        for step in range(NUM_STEPS - 1):
            kern, mass, zb = kernel_matrix(gram, proj)
            cur, tb, proj = update(consts, cur, kern, mass, zb, mean, prec, fact_t, tile)
            gram = gram_bands(tb)
        kern, mass, zb = kernel_matrix(gram, proj)
        out = None
        received = []
        for chunk in range(width // tile):
            out, send = last_update(consts, pos, cur, kern, mass, zb, mean, prec, fact_t, out, chunk, tile)
            received.append(lax.ppermute(send, "part", [(0, 1), (1, 0)]))
        for chunk, recv in enumerate(received):
            out = place(pos, recv, out, chunk)
        return out

    row_spec = P(("ens", "part"), "feat")
    vec_spec = P(("ens", "feat"))
    fac_spec = P(("ens", "feat"), None)
    return jax.shard_map(local_steps, mesh=mesh, in_specs=(row_spec, vec_spec, vec_spec, fac_spec), out_specs=row_spec, check_vma=False)
```

```python
import functools
import math
import jax
import jax.numpy as jnp
from jax import lax
from jax.experimental import pallas as pl
from jax.experimental.pallas import tpu as pltpu
from jax.sharding import PartitionSpec as P

NUM_STEPS = 3
BLK = 256
BANDS = 5
MESH = pl.DeviceIdType.MESH
F32 = jnp.float32
BF16 = jnp.bfloat16
ANY = pl.BlockSpec(memory_space=pl.ANY)
VMEM = pl.BlockSpec(memory_space=pltpu.VMEM)
VMEM_LIMIT = 63 * 1024 * 1024
NT = (((1,), (1,)), ((), ()))


def band_dot(tb, row_blk, n_blk):
    rows = tb[row_blk * BLK:(row_blk + 1) * BLK, :]
    first = min(BANDS, n_blk - row_blk)
    parts = [(0, row_blk * BLK, first * BLK)]
    if first < BANDS:
        parts.append((first * BLK, 0, (BANDS - first) * BLK))
    for dst, src, width in parts:
        yield dst, width, lax.dot_general(rows, tb[src:src + width, :], NT, preferred_element_type=F32)


def exchange_kernel(n_chunk, theta_ref, mean_ref, fact_ref, col_ref, gram_ref, proj_ref,
                    buf, tb, send_sem, recv_sem, own_sem, put_sem, other_sem):
    part = lax.axis_index("part")
    other = 1 - part
    feat = lax.axis_index("feat")
    peer = (lax.axis_index("ens"), other, feat)
    rows, width = theta_ref.shape[0], col_ref.shape[1]
    n_rows = col_ref.shape[0]
    cw = width // n_chunk
    n_blk = n_rows // BLK
    barrier = pltpu.get_barrier_semaphore()
    pl.semaphore_signal(barrier, inc=1, device_id=peer, device_id_type=MESH)
    pl.semaphore_wait(barrier, 1)
    own_rows = pl.ds(pl.multiple_of(part * rows, BLK), rows)
    other_rows = pl.ds(pl.multiple_of(other * rows, BLK), rows)

    def remote(c):
        return pltpu.make_async_remote_copy(
            src_ref=theta_ref.at[:, pl.ds(pl.multiple_of(other * width + c * cw, 128), cw)],
            dst_ref=col_ref.at[own_rows, pl.ds(pl.multiple_of(c * cw, 128), cw)],
            send_sem=send_sem.at[c], recv_sem=recv_sem.at[c], device_id=peer, device_id_type=MESH)

    def fetch_own(c):
        return pltpu.make_async_copy(
            theta_ref.at[:, pl.ds(pl.multiple_of(part * width + c * cw, 128), cw)],
            buf.at[own_rows, :], own_sem)

    def put_own(c):
        return pltpu.make_async_copy(
            buf.at[own_rows, :], col_ref.at[own_rows, pl.ds(pl.multiple_of(c * cw, 128), cw)], put_sem)

    def fetch_other(c):
        return pltpu.make_async_copy(
            col_ref.at[other_rows, pl.ds(pl.multiple_of(c * cw, 128), cw)], buf.at[other_rows, :], other_sem)

    @pl.loop(0, n_chunk)
    def _(c):
        remote(c).start()

    gram_ref[...] = jnp.zeros_like(gram_ref)
    proj_ref[...] = jnp.zeros_like(proj_ref)

    @pl.loop(0, n_chunk)
    def _(c):
        fetch_own(c).start()
        fetch_own(c).wait()
        put_own(c).start()
        remote(c).wait_recv()
        fetch_other(c).start()
        fetch_other(c).wait()
        cols = pl.ds(pl.multiple_of(c * cw, 128), cw)
        fact = fact_ref[:, cols]
        mean = mean_ref[:, cols]

        @pl.loop(0, n_blk)
        def _(b):
            rs = pl.ds(pl.multiple_of(b * BLK, BLK), BLK)
            th = buf[rs, :]
            tb[rs, :] = th.astype(BF16)
            proj_ref[:, rs] += lax.dot_general(fact, (th - mean).astype(BF16), NT, preferred_element_type=F32)

        for b in range(n_blk):
            for dst, wd, val in band_dot(tb, b, n_blk):
                gram_ref[b, :, dst:dst + wd] += val
        put_own(c).wait()

    @pl.loop(0, n_chunk)
    def _(c):
        remote(c).wait_send()


def exchange(theta, mean, fact_t, n_chunk):
    rows, feat = theta.shape
    width = feat // 2
    n_rows = rows * 2
    rank = fact_t.shape[0]
    return pl.pallas_call(
        functools.partial(exchange_kernel, n_chunk),
        out_shape=(jax.ShapeDtypeStruct((n_rows, width), F32),
                   jax.ShapeDtypeStruct((n_rows // BLK, BLK, BANDS * BLK), F32),
                   jax.ShapeDtypeStruct((rank, n_rows), F32)),
        in_specs=[ANY, VMEM, VMEM], out_specs=(ANY, VMEM, VMEM),
        scratch_shapes=[
            pltpu.VMEM((n_rows, width // n_chunk), F32),
            pltpu.VMEM((n_rows, width // n_chunk), BF16),
            pltpu.SemaphoreType.DMA((n_chunk,)), pltpu.SemaphoreType.DMA((n_chunk,)),
            pltpu.SemaphoreType.DMA, pltpu.SemaphoreType.DMA, pltpu.SemaphoreType.DMA],
        compiler_params=pltpu.CompilerParams(collective_id=0, has_side_effects=True, vmem_limit_bytes=VMEM_LIMIT),
        name="exchange",
    )(theta, mean, fact_t)


def build_rhs(theta_ref, mean, prec, fact, zb_ref, rhs, rs):
    tile = theta_ref.shape[1]
    th = theta_ref[rs, :]
    low = jnp.dot(zb_ref[rs, :], fact, preferred_element_type=F32)
    rhs[rs, :tile] = (-((th - mean) * prec + low)).astype(BF16)
    rhs[rs, tile:] = th.astype(BF16)


def stepped(theta_ref, kern_ref, mass_ref, rhs, rs, inv_n, two_over_h, step_size):
    tile = theta_ref.shape[1]
    th = theta_ref[rs, :]
    acc = jnp.dot(kern_ref[rs, :], rhs[...], preferred_element_type=F32)
    pull = mass_ref[rs, :] * th.astype(BF16).astype(F32) - acc[:, tile:]
    return th + step_size * ((acc[:, :tile] + two_over_h * pull) * inv_n)


def update_kernel(consts, theta_ref, kern_ref, mass_ref, zb_ref, mean_ref, prec_ref, fact_ref,
                  out_ref, tb_ref, proj_ref, rhs):
    n_blk = theta_ref.shape[0] // BLK
    fact, mean, prec = fact_ref[...], mean_ref[...], prec_ref[...]

    @pl.when(pl.program_id(0) == 0)
    def _():
        proj_ref[...] = jnp.zeros_like(proj_ref)

    @pl.loop(0, n_blk)
    def _(b):
        build_rhs(theta_ref, mean, prec, fact, zb_ref, rhs, pl.ds(pl.multiple_of(b * BLK, BLK), BLK))

    @pl.loop(0, n_blk)
    def _(b):
        rs = pl.ds(pl.multiple_of(b * BLK, BLK), BLK)
        new = stepped(theta_ref, kern_ref, mass_ref, rhs, rs, *consts)
        out_ref[rs, :] = new
        tb_ref[rs, :] = new.astype(BF16)
        proj_ref[:, rs] += lax.dot_general(fact, (new - mean).astype(BF16), NT, preferred_element_type=F32)


def update(consts, theta, kern, mass, zb, mean, prec, fact_t, tile):
    n_rows, width = theta.shape
    rank = fact_t.shape[0]
    col = lambda r: pl.BlockSpec((r, tile), lambda i: (0, i))
    return pl.pallas_call(
        functools.partial(update_kernel, consts),
        grid=(width // tile,),
        out_shape=(jax.ShapeDtypeStruct((n_rows, width), F32),
                   jax.ShapeDtypeStruct((n_rows, width), BF16),
                   jax.ShapeDtypeStruct((rank, n_rows), F32)),
        in_specs=[col(n_rows), VMEM, VMEM, VMEM, col(1), col(1), col(rank)],
        out_specs=(col(n_rows), col(n_rows), VMEM),
        scratch_shapes=[pltpu.VMEM((n_rows, 2 * tile), BF16)],
        compiler_params=pltpu.CompilerParams(vmem_limit_bytes=VMEM_LIMIT),
        cost_estimate=pl.CostEstimate(flops=4 * n_rows * n_rows * width, bytes_accessed=10 * n_rows * width, transcendentals=0),
        name="update",
    )(theta, kern, mass, zb, mean, prec, fact_t)


def last_kernel(consts, pos_ref, theta_ref, kern_ref, mass_ref, zb_ref, mean_ref, prec_ref, fact_ref, *rest):
    out_ref, send_ref, rhs = rest[-3:]
    rows = out_ref.shape[0]
    n_blk = theta_ref.shape[0] // BLK
    part = pos_ref[0]
    fact, mean, prec = fact_ref[...], mean_ref[...], prec_ref[...]

    @pl.loop(0, n_blk)
    def _(b):
        build_rhs(theta_ref, mean, prec, fact, zb_ref, rhs, pl.ds(pl.multiple_of(b * BLK, BLK), BLK))

    for dst, which in ((send_ref, 1 - part), (out_ref, part)):
        @pl.loop(0, rows // BLK)
        def _(b):
            rs = pl.ds(pl.multiple_of(which * rows + b * BLK, BLK), BLK)
            dst[pl.ds(pl.multiple_of(b * BLK, BLK), BLK), :] = stepped(theta_ref, kern_ref, mass_ref, rhs, rs, *consts)


def last_update(consts, pos, theta, kern, mass, zb, mean, prec, fact_t, out, chunk, tile):
    n_rows, width = theta.shape
    rank = fact_t.shape[0]
    rows, feat = n_rows // 2, width * 2
    per = width // tile
    col = lambda r: pl.BlockSpec((r, tile), lambda i, pos: (0, chunk))
    in_specs = [col(n_rows), VMEM, VMEM, VMEM, col(1), col(1), col(rank)]
    args = [theta, kern, mass, zb, mean, prec, fact_t]
    alias = {}
    if out is not None:
        in_specs.append(ANY)
        args.append(out)
        alias = {8: 0}
    return pl.pallas_call(
        functools.partial(last_kernel, consts),
        grid_spec=pltpu.PrefetchScalarGridSpec(
            num_scalar_prefetch=1, grid=(1,), in_specs=in_specs,
            out_specs=(pl.BlockSpec((rows, tile), lambda i, pos: (0, pos[0] * per + chunk)),
                       pl.BlockSpec((rows, tile), lambda i, pos: (0, 0))),
            scratch_shapes=[pltpu.VMEM((n_rows, 2 * tile), BF16)]),
        out_shape=(jax.ShapeDtypeStruct((rows, feat), F32), jax.ShapeDtypeStruct((rows, tile), F32)),
        input_output_aliases=alias,
        compiler_params=pltpu.CompilerParams(vmem_limit_bytes=VMEM_LIMIT),
        cost_estimate=pl.CostEstimate(flops=4 * n_rows * n_rows * tile, bytes_accessed=10 * n_rows * tile, transcendentals=0),
        name=f"last_update_{chunk}",
    )(pos, *args)


def place_kernel(pos_ref, recv_ref, base_ref, out_ref):
    out_ref[...] = recv_ref[...]


def place(pos, recv, out, chunk):
    rows, tile = recv.shape
    per = out.shape[1] // (2 * tile)
    sub = tile // 128
    return pl.pallas_call(
        place_kernel,
        grid_spec=pltpu.PrefetchScalarGridSpec(
            num_scalar_prefetch=1, grid=(sub,), in_specs=[pl.BlockSpec((rows, 128), lambda i, pos: (0, i)), ANY],
            out_specs=pl.BlockSpec((rows, 128), lambda i, pos: (0, ((1 - pos[0]) * per + chunk) * sub + i))),
        out_shape=jax.ShapeDtypeStruct(out.shape, out.dtype),
        input_output_aliases={2: 0},
        cost_estimate=pl.CostEstimate(flops=1000 * rows * tile, bytes_accessed=8 * rows * tile, transcendentals=0),
        name=f"place_{chunk}",
    )(pos, recv, out)


def kmat_kernel(from_gram, two_over_h, src_ref, proj_ref, kern_ref, zb_ref, *scratch):
    if from_gram:
        tb, sib_out = None, None
    else:
        tb, sib_out, load_sem = scratch[-3:]
    (gbuf, sib_in, r_x1, r_y1, r_x2, r_y2, sq_parts, sq, z_in, z_all, kbuf,
     sib_send, sib_recv, rs_send, rs_recv, sq_send, sq_recv, z_send, z_recv, zb_send, zb_recv,
     k_send, k_recv, loc_sem) = scratch[:24]
    n_rows = kern_ref.shape[0]
    n_blk = n_rows // BLK
    half = BLK // 2
    ens, part, feat = lax.axis_index("ens"), lax.axis_index("part"), lax.axis_index("feat")
    x, core = feat // 2, lax.rem(feat, 2)

    def chip(rel):
        return lax.rem(part + rel // 2, 2), lax.rem(x + rel % 2, 2)

    def block(rel, flip):
        cy, cx = chip(rel)
        return cy * 4 + cx * 2 + lax.rem(core + flip, 2)

    def device(rel, flip):
        cy, cx = chip(rel)
        return (ens, cy, cx * 2 + lax.rem(core + flip, 2))

    me = block(0, 0)
    sibling, dev_x, dev_y = device(0, 1), device(1, 0), device(2, 0)
    others = [(rel, flip) for rel in (3, 1, 2, 0) for flip in (0, 1) if (rel, flip) != (0, 0)]

    def rcopy(src, dst, ssem, rsem, dev):
        return pltpu.make_async_remote_copy(src_ref=src, dst_ref=dst, send_sem=ssem, recv_sem=rsem,
                                            device_id=dev, device_id_type=MESH)

    barrier = pltpu.get_barrier_semaphore()
    for rel, flip in others:
        pl.semaphore_signal(barrier, inc=1, device_id=device(rel, flip), device_id_type=MESH)

    def load(b):
        rs = pl.ds(b * BLK, BLK)
        return pltpu.make_async_copy(src_ref.at[rs, :], tb.at[rs, :], load_sem.at[b])

    def own_gram(rel):
        return pltpu.make_async_copy(src_ref.at[block(rel, 0)], gbuf.at[rel], loc_sem.at[rel])

    if from_gram:
        for rel in (3, 2, 1, 0):
            own_gram(rel).start()
    else:
        for b in range(n_blk):
            load(b).start()
    pl.semaphore_wait(barrier, len(others))

    def z_cols(b):
        return proj_ref.at[:, pl.ds(pl.multiple_of(b * BLK, BLK), BLK)]

    def z_copy(i):
        rel, flip = others[i]
        return rcopy(z_cols(block(rel, flip)), z_in.at[me], z_send.at[i], z_recv.at[me], device(rel, flip))

    for i in range(len(others)):
        z_copy(i).start()
    z_own = pltpu.make_async_copy(z_cols(me), z_in.at[me], z_recv.at[me])
    z_own.start()

    def sib_copy(rel):
        src = src_ref.at[block(rel, 1)] if from_gram else sib_out.at[rel]
        return rcopy(src, sib_in.at[rel], sib_send.at[rel], sib_recv.at[rel], sibling)

    lo, hi = pl.ds(0, half), pl.ds(half, half)
    rs_copies = {
        "d_lo": rcopy(gbuf.at[3, lo], r_x1.at[0], rs_send.at[0], rs_recv.at[0], dev_x),
        "d_hi": rcopy(gbuf.at[3, hi], r_y1.at[0], rs_send.at[1], rs_recv.at[1], dev_y),
        "y_hi": rcopy(gbuf.at[2, hi], r_y1.at[1], rs_send.at[2], rs_recv.at[2], dev_y),
        "x_lo": rcopy(gbuf.at[1, lo], r_x1.at[1], rs_send.at[3], rs_recv.at[3], dev_x),
        "y_lo": rcopy(gbuf.at[2, lo], r_y2, rs_send.at[4], rs_recv.at[4], dev_y),
        "x_hi": rcopy(gbuf.at[1, hi], r_x2, rs_send.at[5], rs_recv.at[5], dev_x),
    }
    eye = (lax.broadcasted_iota(jnp.int32, (BLK, BLK), 0) == lax.broadcasted_iota(jnp.int32, (BLK, BLK), 1)).astype(F32)

    def merge(rel):
        sib_copy(rel).wait_recv()
        gbuf[rel] += sib_in[rel]

    def first_sends(rel):
        for name in {3: ("d_lo", "d_hi"), 2: ("y_hi",), 1: ("x_lo",), 0: ()}[rel]:
            rs_copies[name].start()

    if from_gram:
        for rel in (3, 2, 1, 0):
            sib_copy(rel).start()
        for rel in (3, 2, 1, 0):
            own_gram(rel).wait()
            merge(rel)
            first_sends(rel)
    else:
        def bands_of(b, dst):
            rows = tb[pl.ds(pl.multiple_of(b * BLK, BLK), BLK), :]
            for k in range(BANDS):
                j = lax.rem(b + k, n_blk)
                dst[:, k * BLK:(k + 1) * BLK] = lax.dot_general(
                    rows, tb[pl.ds(pl.multiple_of(j * BLK, BLK), BLK), :], NT, preferred_element_type=F32)

        for b in range(n_blk):
            load(b).wait()

        @pl.loop(0, 4)
        def _(i):
            rel = 3 - i
            cy, cx = lax.rem(part + rel // 2, 2), lax.rem(x + lax.rem(rel, 2), 2)
            base = cy * 4 + cx * 2
            bands_of(base + 1 - core, sib_out.at[rel])
            rcopy(sib_out.at[rel], sib_in.at[rel], sib_send.at[rel], sib_recv.at[rel], sibling).start()
            bands_of(base + core, gbuf.at[rel])
            rcopy(sib_out.at[rel], sib_in.at[rel], sib_send.at[rel], sib_recv.at[rel], sibling).wait_recv()
            gbuf[rel] += sib_in[rel]
            for r in (3, 2, 1):
                @pl.when(rel == r)
                def _():
                    first_sends(r)

    for rel in range(4):
        cy, cx = chip(rel)
        sq_parts[me, cy * 2 + cx] = jnp.sum(gbuf[rel, :, :BLK] * eye, axis=0, keepdims=True)

    def sq_copy(i):
        rel, flip = others[i]
        return rcopy(sq_parts.at[me], sq_parts.at[me], sq_send.at[i], sq_recv.at[me], device(rel, flip))

    def recv_from(buf, sem, rel, flip):
        b = block(rel, flip)
        return rcopy(buf.at[b], buf.at[b], sq_send.at[0], sem.at[b], sibling)

    for i in range(len(others)):
        sq_copy(i).start()

    rs_copies["d_lo"].wait_recv()
    gbuf[2, :half] += r_x1[0]
    rs_copies["y_lo"].start()
    rs_copies["d_hi"].wait_recv()
    gbuf[1, half:] += r_y1[0]
    rs_copies["x_hi"].start()

    z_own.wait()
    for rel, flip in others:
        recv_from(z_in, z_recv, rel, flip).wait_recv()
    z_sum = z_in[0]
    for b in range(1, n_blk):
        z_sum = z_sum + z_in[b]
    z_all[me] = z_sum.astype(BF16)

    def zb_copy(i):
        rel, flip = others[i]
        return rcopy(z_all.at[me], z_all.at[me], zb_send.at[i], zb_recv.at[me], device(rel, flip))

    for i in range(len(others)):
        zb_copy(i).start()
    for rel, flip in others:
        recv_from(sq_parts, sq_recv, rel, flip).wait_recv()
    for c in range(2):
        for q in range(4):
            s = sq_parts[c, q] + sq_parts[2 + c, q] + sq_parts[4 + c, q] + sq_parts[6 + c, q]
            b = 2 * q + c
            sq[:, b * BLK:(b + 1) * BLK] = s
            if b < BANDS - 1:
                sq[:, n_rows + b * BLK:n_rows + (b + 1) * BLK] = s
    sq_row = sq[:, pl.ds(pl.multiple_of(me * BLK, BLK), BANDS * BLK)]
    sq_col = jnp.sum(eye * sq_row[:, :BLK], axis=1, keepdims=True)

    def kernel_of(gram, col):
        return jnp.exp(-jnp.maximum(col + sq_row - 2.0 * gram, 0.0) * (0.5 * two_over_h)).astype(BF16)

    slots = iter(range(14))
    sent = []

    def send_band(idx, dev):
        s = next(slots)
        cp = rcopy(kbuf.at[idx], kbuf.at[idx], k_send.at[s], k_recv.at[idx], dev)
        cp.start()
        sent.append(cp)

    def wait_band(idx):
        rcopy(kbuf.at[idx], kbuf.at[idx], k_send.at[0], k_recv.at[idx], sibling).wait_recv()

    def spread(b, h):
        idx = 2 * b + h
        row0 = pl.multiple_of(b * BLK + h * half, half)
        for k in range(BANDS):
            j = lax.rem(b + k, n_blk)
            tile = kbuf[idx, :, k * BLK:(k + 1) * BLK]
            col0 = pl.multiple_of(j * BLK, BLK)
            kern_ref[pl.ds(row0, half), pl.ds(col0, BLK)] = tile
            if 0 < k < BANDS - 1:
                kern_ref[pl.ds(col0, BLK), pl.ds(row0, half)] = tile.T

    rs_copies["x_lo"].wait_recv()
    rs_copies["y_lo"].wait_recv()
    kbuf[2 * me] = kernel_of(gbuf[0, :half] + (r_x1[1] + r_y2[...]), sq_col[:half])
    for dev in (dev_y, sibling):
        send_band(2 * me, dev)
    rs_copies["y_hi"].wait_recv()
    rs_copies["x_hi"].wait_recv()
    kbuf[2 * me + 1] = kernel_of(gbuf[0, half:] + (r_y1[1] + r_x2[...]), sq_col[half:])
    for dev in (dev_x, sibling):
        send_band(2 * me + 1, dev)
    send_band(2 * me, dev_x)
    send_band(2 * me + 1, dev_y)
    spread(me, 0)
    spread(me, 1)
    sib = block(0, 1)
    for h in range(2):
        wait_band(2 * sib + h)
        spread(sib, h)
    bx, by, bd = block(1, 0), block(2, 0), block(3, 0)
    wait_band(2 * by)
    send_band(2 * by, dev_x)
    send_band(2 * by, sibling)
    wait_band(2 * bx + 1)
    send_band(2 * bx + 1, dev_y)
    send_band(2 * bx + 1, sibling)
    spread(by, 0)
    spread(bx, 1)
    for b, h in ((bx, 0), (by, 1), (bd, 0), (bd, 1)):
        wait_band(2 * b + h)
        send_band(2 * b + h, sibling)
        spread(b, h)
    for rel, h in ((2, 0), (1, 1), (1, 0), (2, 1), (3, 0), (3, 1)):
        b = block(rel, 1)
        wait_band(2 * b + h)
        spread(b, h)
    for rel, flip in others:
        recv_from(z_all, zb_recv, rel, flip).wait_recv()
    for b in range(n_blk):
        zb_ref[b * BLK:(b + 1) * BLK, :] = z_all[b].astype(F32).T.astype(BF16)
    for rel in range(4):
        sib_copy(rel).wait_send()
    for cp in rs_copies.values():
        cp.wait_send()
    for i in range(len(others)):
        z_copy(i).wait_send()
        sq_copy(i).wait_send()
        zb_copy(i).wait_send()
    for cp in sent:
        cp.wait_send()


def kernel_matrix(src, proj, two_over_h, collective_id, from_gram):
    rank, n_rows = proj.shape
    n_blk = n_rows // BLK
    wide = BANDS * BLK
    dma = lambda *n: pltpu.SemaphoreType.DMA(n)
    scratch = [
        pltpu.VMEM((4, BLK, wide), F32), pltpu.VMEM((4, BLK, wide), F32),
        pltpu.VMEM((2, BLK // 2, wide), F32), pltpu.VMEM((2, BLK // 2, wide), F32),
        pltpu.VMEM((BLK // 2, wide), F32), pltpu.VMEM((BLK // 2, wide), F32),
        pltpu.VMEM((8, 4, 1, BLK), F32), pltpu.VMEM((1, n_rows + (BANDS - 1) * BLK), F32),
        pltpu.VMEM((n_blk, rank, BLK), F32), pltpu.VMEM((n_blk, rank, BLK), BF16),
        pltpu.VMEM((2 * n_blk, BLK // 2, wide), BF16),
        dma(4), dma(4), dma(6), dma(6), dma(7), dma(8), dma(7), dma(8), dma(7), dma(8), dma(14), dma(16), dma(4)]
    if not from_gram:
        scratch += [pltpu.VMEM(src.shape, BF16), pltpu.VMEM((4, BLK, wide), F32), dma(n_blk)]
    return pl.pallas_call(
        functools.partial(kmat_kernel, from_gram, two_over_h),
        out_shape=(jax.ShapeDtypeStruct((n_rows, n_rows), BF16), jax.ShapeDtypeStruct((n_rows, rank), BF16)),
        in_specs=[ANY, VMEM], out_specs=(VMEM, VMEM), scratch_shapes=scratch,
        compiler_params=pltpu.CompilerParams(collective_id=collective_id, has_side_effects=True, vmem_limit_bytes=VMEM_LIMIT),
        name=f"kernel_matrix_{collective_id}",
    )(src, proj)


def solution(mesh):
    part_size = mesh.shape["part"]
    feat_size = mesh.shape["feat"]

    def local_steps(theta, prec_loc, mean_loc, factor_loc):
        rows, feat_loc = theta.shape
        n_total = rows * part_size
        feat_total = feat_loc * feat_size
        width = feat_loc // part_size
        kern_width = 2.0 * feat_total / math.log(n_total)
        step_size = 0.15 * n_total * feat_total / math.log(n_total)
        consts = (1.0 / n_total, 2.0 / kern_width, step_size)
        part = lax.axis_index("part")
        pos = part.astype(jnp.int32).reshape(1)
        mean = lax.dynamic_slice_in_dim(mean_loc, part * width, width).reshape(1, width)
        prec = lax.dynamic_slice_in_dim(prec_loc, part * width, width).reshape(1, width)
        fact_t = lax.dynamic_slice_in_dim(factor_loc, part * width, width, axis=0).T
        tile = width // 7

        cur, gram, proj = exchange(theta, mean, fact_t, 7)
        src = gram
        for step in range(NUM_STEPS):
            kern, zb = kernel_matrix(src, proj, consts[1], 1 + step, step == 0)
            mass = jnp.sum(kern, axis=1, dtype=F32).reshape(n_total, 1)
            if step < NUM_STEPS - 1:
                cur, src, proj = update(consts, cur, kern, mass, zb, mean, prec, fact_t, tile)
        out = None
        received = []
        for chunk in range(width // tile):
            out, send = last_update(consts, pos, cur, kern, mass, zb, mean, prec, fact_t, out, chunk, tile)
            received.append(lax.ppermute(send, "part", [(0, 1), (1, 0)]))
        for chunk, recv in enumerate(received):
            out = place(pos, recv, out, chunk)
        return out

    row_spec = P(("ens", "part"), "feat")
    vec_spec = P(("ens", "feat"))
    fac_spec = P(("ens", "feat"), None)
    return jax.shard_map(local_steps, mesh=mesh, in_specs=(row_spec, vec_spec, vec_spec, fac_spec), out_specs=row_spec, check_vma=False)
```

```python
import functools
import math
import jax
import jax.numpy as jnp
from jax import lax
from jax.experimental import pallas as pl
from jax.experimental.pallas import tpu as pltpu
from jax.sharding import PartitionSpec as P

NUM_STEPS = 3
BLK = 256
HALF = BLK // 2
REACH = 5
WIDE = 9 * HALF
MESH = pl.DeviceIdType.MESH
F32 = jnp.float32
BF16 = jnp.bfloat16
ANY = pl.BlockSpec(memory_space=pl.ANY)
VMEM = pl.BlockSpec(memory_space=pltpu.VMEM)
VMEM_LIMIT = 63 * 1024 * 1024
NT = (((1,), (1,)), ((), ()))


def band_parts(k, val):
    top, low = val[:HALF], val[HALF:]
    if k == 0:
        return (0, 0, top), (1, 0, low[:, HALF:])
    if k == REACH - 1:
        top = top[:, :HALF]
    return (0, k * BLK, top), (1, k * BLK - HALF, low)


def exchange_kernel(n_chunk, theta_ref, mean_ref, fact_ref, col_ref, gram_ref, proj_ref,
                    buf, tb, send_sem, recv_sem, own_sem, put_sem, other_sem):
    part = lax.axis_index("part")
    other = 1 - part
    feat = lax.axis_index("feat")
    peer = (lax.axis_index("ens"), other, feat)
    rows, width = theta_ref.shape[0], col_ref.shape[1]
    n_rows = col_ref.shape[0]
    cw = width // n_chunk
    n_blk = n_rows // BLK
    barrier = pltpu.get_barrier_semaphore()
    pl.semaphore_signal(barrier, inc=1, device_id=peer, device_id_type=MESH)
    pl.semaphore_wait(barrier, 1)
    own_rows = pl.ds(pl.multiple_of(part * rows, BLK), rows)
    other_rows = pl.ds(pl.multiple_of(other * rows, BLK), rows)

    def remote(c):
        return pltpu.make_async_remote_copy(
            src_ref=theta_ref.at[:, pl.ds(pl.multiple_of(other * width + c * cw, 128), cw)],
            dst_ref=col_ref.at[own_rows, pl.ds(pl.multiple_of(c * cw, 128), cw)],
            send_sem=send_sem.at[c], recv_sem=recv_sem.at[c], device_id=peer, device_id_type=MESH)

    def fetch_own(c):
        return pltpu.make_async_copy(
            theta_ref.at[:, pl.ds(pl.multiple_of(part * width + c * cw, 128), cw)],
            buf.at[own_rows, :], own_sem)

    def put_own(c):
        return pltpu.make_async_copy(
            buf.at[own_rows, :], col_ref.at[own_rows, pl.ds(pl.multiple_of(c * cw, 128), cw)], put_sem)

    def fetch_other(c):
        return pltpu.make_async_copy(
            col_ref.at[other_rows, pl.ds(pl.multiple_of(c * cw, 128), cw)], buf.at[other_rows, :], other_sem)

    @pl.loop(0, n_chunk)
    def _(c):
        remote(c).start()

    gram_ref[...] = jnp.zeros_like(gram_ref)
    proj_ref[...] = jnp.zeros_like(proj_ref)

    @pl.loop(0, n_chunk)
    def _(c):
        fetch_own(c).start()
        fetch_own(c).wait()
        put_own(c).start()
        remote(c).wait_recv()
        fetch_other(c).start()
        fetch_other(c).wait()
        cols = pl.ds(pl.multiple_of(c * cw, 128), cw)
        fact = fact_ref[:, cols]
        mean = mean_ref[:, cols]

        @pl.loop(0, n_blk)
        def _(b):
            rs = pl.ds(pl.multiple_of(b * BLK, BLK), BLK)
            th = buf[rs, :]
            tb[rs, :] = th.astype(BF16)
            proj_ref[:, rs] += lax.dot_general(fact, (th - mean).astype(BF16), NT, preferred_element_type=F32)

        for b in range(n_blk):
            rows_b = tb[b * BLK:(b + 1) * BLK, :]
            for k in range(REACH):
                j = (b + k) % n_blk
                val = lax.dot_general(rows_b, tb[j * BLK:(j + 1) * BLK, :], NT, preferred_element_type=F32)
                for h, col, piece in band_parts(k, val):
                    gram_ref[b, h, :, col:col + piece.shape[1]] += piece
        put_own(c).wait()

    @pl.loop(0, n_chunk)
    def _(c):
        remote(c).wait_send()


def exchange(theta, mean, fact_t, n_chunk):
    rows, feat = theta.shape
    width = feat // 2
    n_rows = rows * 2
    rank = fact_t.shape[0]
    return pl.pallas_call(
        functools.partial(exchange_kernel, n_chunk),
        out_shape=(jax.ShapeDtypeStruct((n_rows, width), F32),
                   jax.ShapeDtypeStruct((n_rows // BLK, 2, HALF, WIDE), F32),
                   jax.ShapeDtypeStruct((rank, n_rows), F32)),
        in_specs=[ANY, VMEM, VMEM], out_specs=(ANY, VMEM, VMEM),
        scratch_shapes=[
            pltpu.VMEM((n_rows, width // n_chunk), F32),
            pltpu.VMEM((n_rows, width // n_chunk), BF16),
            pltpu.SemaphoreType.DMA((n_chunk,)), pltpu.SemaphoreType.DMA((n_chunk,)),
            pltpu.SemaphoreType.DMA, pltpu.SemaphoreType.DMA, pltpu.SemaphoreType.DMA],
        compiler_params=pltpu.CompilerParams(collective_id=0, has_side_effects=True, vmem_limit_bytes=VMEM_LIMIT),
        name="exchange",
    )(theta, mean, fact_t)


def build_rhs(theta_ref, mean, prec, fact, zb_ref, rhs, rs):
    tile = theta_ref.shape[1]
    th = theta_ref[rs, :]
    low = jnp.dot(zb_ref[rs, :], fact, preferred_element_type=F32)
    rhs[rs, :tile] = (-((th - mean) * prec + low)).astype(BF16)
    rhs[rs, tile:] = th.astype(BF16)


def stepped(theta_ref, acc, mass_ref, rs, inv_n, two_over_h, step_size):
    tile = theta_ref.shape[1]
    th = theta_ref[rs, :]
    pull = mass_ref[rs, :] * th.astype(BF16).astype(F32) - acc[:, tile:]
    return th + step_size * ((acc[:, :tile] + two_over_h * pull) * inv_n)


def update_kernel(consts, theta_ref, next_ref, kern_ref, mass_ref, zb_ref, mean_ref, prec_ref, fact_ref,
                  mean_n, prec_n, fact_n, out_ref, tb_ref, proj_ref, rhs):
    n_rows = theta_ref.shape[0]
    big = n_rows // 2
    slot = lax.rem(pl.program_id(0), 2)

    @pl.when(pl.program_id(0) == 0)
    def _():
        proj_ref[...] = jnp.zeros_like(proj_ref)

        @pl.loop(0, n_rows // BLK)
        def _(b):
            build_rhs(theta_ref, mean_ref[...], prec_ref[...], fact_ref[...], zb_ref, rhs.at[0],
                      pl.ds(pl.multiple_of(b * BLK, BLK), BLK))

    @pl.loop(0, 2)
    def _(b):
        rs = pl.ds(pl.multiple_of(b * big, big), big)
        acc = jnp.dot(kern_ref[rs, :], rhs[slot], preferred_element_type=F32)
        build_rhs(next_ref, mean_n[...], prec_n[...], fact_n[...], zb_ref, rhs.at[1 - slot], rs)
        new = stepped(theta_ref, acc, mass_ref, rs, *consts)
        out_ref[rs, :] = new
        tb_ref[rs, :] = new.astype(BF16)
        proj_ref[:, rs] += lax.dot_general(fact_ref[...], (new - mean_ref[...]).astype(BF16), NT, preferred_element_type=F32)


def update(consts, theta, kern, mass, zb, mean, prec, fact_t, tile):
    n_rows, width = theta.shape
    rank = fact_t.shape[0]
    steps = width // tile
    col = lambda r: pl.BlockSpec((r, tile), lambda i: (0, i))
    nxt = lambda r: pl.BlockSpec((r, tile), lambda i: (0, jnp.minimum(i + 1, steps - 1)))
    return pl.pallas_call(
        functools.partial(update_kernel, consts),
        grid=(steps,),
        out_shape=(jax.ShapeDtypeStruct((n_rows, width), F32),
                   jax.ShapeDtypeStruct((n_rows, width), BF16),
                   jax.ShapeDtypeStruct((rank, n_rows), F32)),
        in_specs=[col(n_rows), nxt(n_rows), VMEM, VMEM, VMEM, col(1), col(1), col(rank), nxt(1), nxt(1), nxt(rank)],
        out_specs=(col(n_rows), col(n_rows), VMEM),
        scratch_shapes=[pltpu.VMEM((2, n_rows, 2 * tile), BF16)],
        compiler_params=pltpu.CompilerParams(vmem_limit_bytes=VMEM_LIMIT),
        cost_estimate=pl.CostEstimate(flops=4 * n_rows * n_rows * width, bytes_accessed=10 * n_rows * width, transcendentals=0),
        name="update",
    )(theta, theta, kern, mass, zb, mean, prec, fact_t, mean, prec, fact_t)


def last_kernel(consts, pos_ref, theta_ref, kern_ref, mass_ref, zb_ref, mean_ref, prec_ref, fact_ref, *rest):
    out_ref, send_ref, rhs = rest[-3:]
    rows = out_ref.shape[0]
    n_blk = theta_ref.shape[0] // BLK
    part = pos_ref[0]
    fact, mean, prec = fact_ref[...], mean_ref[...], prec_ref[...]

    @pl.loop(0, n_blk)
    def _(b):
        build_rhs(theta_ref, mean, prec, fact, zb_ref, rhs, pl.ds(pl.multiple_of(b * BLK, BLK), BLK))

    for dst, which in ((send_ref, 1 - part), (out_ref, part)):
        @pl.loop(0, rows // BLK)
        def _(b):
            rs = pl.ds(pl.multiple_of(which * rows + b * BLK, BLK), BLK)
            acc = jnp.dot(kern_ref[rs, :], rhs[...], preferred_element_type=F32)
            dst[pl.ds(pl.multiple_of(b * BLK, BLK), BLK), :] = stepped(theta_ref, acc, mass_ref, rs, *consts)


def last_update(consts, pos, theta, kern, mass, zb, mean, prec, fact_t, out, start, tile):
    n_rows, width = theta.shape
    chunk = start // tile
    rank = fact_t.shape[0]
    rows, feat = n_rows // 2, width * 2
    per = width // tile
    col = lambda r: pl.BlockSpec((r, tile), lambda i, pos: (0, chunk))
    in_specs = [col(n_rows), VMEM, VMEM, VMEM, col(1), col(1), col(rank)]
    args = [theta, kern, mass, zb, mean, prec, fact_t]
    alias = {}
    if out is not None:
        in_specs.append(ANY)
        args.append(out)
        alias = {8: 0}
    return pl.pallas_call(
        functools.partial(last_kernel, consts),
        grid_spec=pltpu.PrefetchScalarGridSpec(
            num_scalar_prefetch=1, grid=(1,), in_specs=in_specs,
            out_specs=(pl.BlockSpec((rows, tile), lambda i, pos: (0, pos[0] * per + chunk)),
                       pl.BlockSpec((rows, tile), lambda i, pos: (0, 0))),
            scratch_shapes=[pltpu.VMEM((n_rows, 2 * tile), BF16)]),
        out_shape=(jax.ShapeDtypeStruct((rows, feat), F32), jax.ShapeDtypeStruct((rows, tile), F32)),
        input_output_aliases=alias,
        compiler_params=pltpu.CompilerParams(vmem_limit_bytes=VMEM_LIMIT),
        cost_estimate=pl.CostEstimate(flops=4 * n_rows * n_rows * tile, bytes_accessed=10 * n_rows * tile, transcendentals=0),
    )(pos, *args)


def place_kernel(pos_ref, recv_ref, base_ref, out_ref):
    out_ref[...] = recv_ref[...]


def place(pos, recv, out, start):
    rows, tile = recv.shape
    per = out.shape[1] // 256
    sub = tile // 128
    first = start // 128
    return pl.pallas_call(
        place_kernel,
        grid_spec=pltpu.PrefetchScalarGridSpec(
            num_scalar_prefetch=1, grid=(sub,), in_specs=[pl.BlockSpec((rows, 128), lambda i, pos: (0, i)), ANY],
            out_specs=pl.BlockSpec((rows, 128), lambda i, pos: (0, (1 - pos[0]) * per + first + i))),
        out_shape=jax.ShapeDtypeStruct(out.shape, out.dtype),
        input_output_aliases={2: 0},
        cost_estimate=pl.CostEstimate(flops=1000 * rows * tile, bytes_accessed=8 * rows * tile, transcendentals=0),
    )(pos, recv, out)


def kmat_kernel(from_gram, two_over_h, src_ref, proj_ref, kern_ref, zb_ref, mass_ref, *scratch):
    if from_gram:
        tb, sib_out = None, None
    else:
        tb, sib_out, load_sem = scratch[-3:]
    (gbuf, sib_in, r_x1, r_y1, r_x2, r_y2, sq_parts, sq, z_in, z_all, kbuf,
     sib_send, sib_recv, rs_send, rs_recv, sq_send, sq_recv, z_send, z_recv, zb_send, zb_recv,
     k_send, k_recv, loc_sem) = scratch[:24]
    n_rows = kern_ref.shape[0]
    n_blk = n_rows // BLK
    ens, part, feat = lax.axis_index("ens"), lax.axis_index("part"), lax.axis_index("feat")
    x, core = feat // 2, lax.rem(feat, 2)

    def chip(rel):
        return lax.rem(part + rel // 2, 2), lax.rem(x + rel % 2, 2)

    def block(rel, flip):
        cy, cx = chip(rel)
        return cy * 4 + cx * 2 + lax.rem(core + flip, 2)

    def device(rel, flip):
        cy, cx = chip(rel)
        return (ens, cy, cx * 2 + lax.rem(core + flip, 2))

    me = block(0, 0)
    sibling, dev_x, dev_y = device(0, 1), device(1, 0), device(2, 0)
    others = [(rel, flip) for rel in (3, 1, 2, 0) for flip in (0, 1) if (rel, flip) != (0, 0)]

    def rcopy(src, dst, ssem, rsem, dev):
        return pltpu.make_async_remote_copy(src_ref=src, dst_ref=dst, send_sem=ssem, recv_sem=rsem,
                                            device_id=dev, device_id_type=MESH)

    barrier = pltpu.get_barrier_semaphore()
    for rel, flip in others:
        pl.semaphore_signal(barrier, inc=1, device_id=device(rel, flip), device_id_type=MESH)

    def load(b):
        rs = pl.ds(b * BLK, BLK)
        return pltpu.make_async_copy(src_ref.at[rs, :], tb.at[rs, :], load_sem.at[b])

    def own_gram(rel):
        return pltpu.make_async_copy(src_ref.at[block(rel, 0)], gbuf.at[rel], loc_sem.at[rel])

    if from_gram:
        for rel in (3, 2, 1, 0):
            own_gram(rel).start()
    else:
        for b in range(n_blk):
            load(b).start()
    pl.semaphore_wait(barrier, len(others))

    def z_cols(b):
        return proj_ref.at[:, pl.ds(pl.multiple_of(b * BLK, BLK), BLK)]

    def z_copy(i):
        rel, flip = others[i]
        return rcopy(z_cols(block(rel, flip)), z_in.at[me], z_send.at[i], z_recv.at[me], device(rel, flip))

    for i in range(len(others)):
        z_copy(i).start()
    z_own = pltpu.make_async_copy(z_cols(me), z_in.at[me], z_recv.at[me])
    z_own.start()

    def sib_copy(rel):
        src = src_ref.at[block(rel, 1)] if from_gram else sib_out.at[rel]
        return rcopy(src, sib_in.at[rel], sib_send.at[rel], sib_recv.at[rel], sibling)

    lo, hi = 0, 1
    rs_copies = {
        "d_lo": rcopy(gbuf.at[3, lo], r_x1.at[0], rs_send.at[0], rs_recv.at[0], dev_x),
        "d_hi": rcopy(gbuf.at[3, hi], r_y1.at[0], rs_send.at[1], rs_recv.at[1], dev_y),
        "y_hi": rcopy(gbuf.at[2, hi], r_y1.at[1], rs_send.at[2], rs_recv.at[2], dev_y),
        "x_lo": rcopy(gbuf.at[1, lo], r_x1.at[1], rs_send.at[3], rs_recv.at[3], dev_x),
        "y_lo": rcopy(gbuf.at[2, lo], r_y2, rs_send.at[4], rs_recv.at[4], dev_y),
        "x_hi": rcopy(gbuf.at[1, hi], r_x2, rs_send.at[5], rs_recv.at[5], dev_x),
    }
    eye = (lax.broadcasted_iota(jnp.int32, (HALF, HALF), 0) == lax.broadcasted_iota(jnp.int32, (HALF, HALF), 1)).astype(F32)

    def merge(rel):
        sib_copy(rel).wait_recv()
        gbuf[rel] += sib_in[rel]

    def first_sends(rel):
        for name in {3: ("d_lo", "d_hi"), 2: ("y_hi",), 1: ("x_lo",), 0: ()}[rel]:
            rs_copies[name].start()

    if from_gram:
        for rel in (3, 2, 1, 0):
            sib_copy(rel).start()
        for rel in (3, 2, 1, 0):
            own_gram(rel).wait()
            merge(rel)
            first_sends(rel)
    else:
        def bands_of(b, dst):
            rows = tb[pl.ds(pl.multiple_of(b * BLK, BLK), BLK), :]
            for k in range(REACH):
                j = lax.rem(b + k, n_blk)
                val = lax.dot_general(
                    rows, tb[pl.ds(pl.multiple_of(j * BLK, BLK), BLK), :], NT, preferred_element_type=F32)
                for h, col, piece in band_parts(k, val):
                    dst[h, :, col:col + piece.shape[1]] = piece

        for b in range(n_blk):
            load(b).wait()

        @pl.loop(0, 4)
        def _(i):
            rel = 3 - i
            cy, cx = lax.rem(part + rel // 2, 2), lax.rem(x + lax.rem(rel, 2), 2)
            base = cy * 4 + cx * 2
            bands_of(base + 1 - core, sib_out.at[rel])
            rcopy(sib_out.at[rel], sib_in.at[rel], sib_send.at[rel], sib_recv.at[rel], sibling).start()
            bands_of(base + core, gbuf.at[rel])
            rcopy(sib_out.at[rel], sib_in.at[rel], sib_send.at[rel], sib_recv.at[rel], sibling).wait_recv()
            gbuf[rel] += sib_in[rel]
            for r in (3, 2, 1):
                @pl.when(rel == r)
                def _():
                    first_sends(r)

    for rel in range(4):
        cy, cx = chip(rel)
        for h in range(2):
            sq_parts[me, cy * 2 + cx, :, h * HALF:(h + 1) * HALF] = jnp.sum(gbuf[rel, h, :, :HALF] * eye, axis=0, keepdims=True)

    def sq_copy(i):
        rel, flip = others[i]
        return rcopy(sq_parts.at[me], sq_parts.at[me], sq_send.at[i], sq_recv.at[me], device(rel, flip))

    def recv_from(buf, sem, rel, flip):
        b = block(rel, flip)
        return rcopy(buf.at[b], buf.at[b], sq_send.at[0], sem.at[b], sibling)

    for i in range(len(others)):
        sq_copy(i).start()

    rs_copies["d_lo"].wait_recv()
    gbuf[2, 0] += r_x1[0]
    rs_copies["y_lo"].start()
    rs_copies["d_hi"].wait_recv()
    gbuf[1, 1] += r_y1[0]
    rs_copies["x_hi"].start()

    z_own.wait()
    for rel, flip in others:
        recv_from(z_in, z_recv, rel, flip).wait_recv()
    z_sum = z_in[0]
    for b in range(1, n_blk):
        z_sum = z_sum + z_in[b]
    z_all[me] = z_sum.astype(BF16)

    def zb_copy(i):
        rel, flip = others[i]
        return rcopy(z_all.at[me], z_all.at[me], zb_send.at[i], zb_recv.at[me], device(rel, flip))

    for i in range(len(others)):
        zb_copy(i).start()
    for rel, flip in others:
        recv_from(sq_parts, sq_recv, rel, flip).wait_recv()
    for c in range(2):
        for q in range(4):
            s = sq_parts[c, q] + sq_parts[2 + c, q] + sq_parts[4 + c, q] + sq_parts[6 + c, q]
            b = 2 * q + c
            sq[:, b * BLK:(b + 1) * BLK] = s
            if b < REACH - 1:
                sq[:, n_rows + b * BLK:n_rows + (b + 1) * BLK] = s

    def kernel_of(h, gram):
        row = sq[:, pl.ds(pl.multiple_of((2 * me + h) * HALF, HALF), WIDE)]
        col = jnp.sum(eye * row[:, :HALF], axis=1, keepdims=True)
        return jnp.exp(-jnp.maximum(col + row - 2.0 * gram, 0.0) * (0.5 * two_over_h)).astype(BF16)

    slots = iter(range(14))
    sent = []

    def send_band(idx, dev):
        s = next(slots)
        cp = rcopy(kbuf.at[idx], kbuf.at[idx], k_send.at[s], k_recv.at[idx], dev)
        cp.start()
        sent.append(cp)

    def wait_band(idx):
        rcopy(kbuf.at[idx], kbuf.at[idx], k_send.at[0], k_recv.at[idx], sibling).wait_recv()

    def spread(b, h):
        idx = 2 * b + h
        row0 = pl.multiple_of(idx * HALF, HALF)
        for k in range(REACH * 2 - 1):
            col0 = pl.multiple_of(lax.rem(idx + k, 2 * n_blk) * HALF, HALF)
            tile = kbuf[idx, :, k * HALF:(k + 1) * HALF]
            kern_ref[pl.ds(row0, HALF), pl.ds(col0, HALF)] = tile
            if 0 < k < REACH * 2 - 2:
                kern_ref[pl.ds(col0, HALF), pl.ds(row0, HALF)] = tile.T

    rs_copies["x_lo"].wait_recv()
    rs_copies["y_lo"].wait_recv()
    kbuf[2 * me] = kernel_of(0, gbuf[0, 0] + (r_x1[1] + r_y2[...]))
    for dev in (dev_y, sibling):
        send_band(2 * me, dev)
    rs_copies["y_hi"].wait_recv()
    rs_copies["x_hi"].wait_recv()
    kbuf[2 * me + 1] = kernel_of(1, gbuf[0, 1] + (r_y1[1] + r_x2[...]))
    for dev in (dev_x, sibling):
        send_band(2 * me + 1, dev)
    send_band(2 * me, dev_x)
    send_band(2 * me + 1, dev_y)
    spread(me, 0)
    spread(me, 1)
    sib = block(0, 1)
    for h in range(2):
        wait_band(2 * sib + h)
        spread(sib, h)
    bx, by, bd = block(1, 0), block(2, 0), block(3, 0)
    wait_band(2 * by)
    send_band(2 * by, dev_x)
    send_band(2 * by, sibling)
    wait_band(2 * bx + 1)
    send_band(2 * bx + 1, dev_y)
    send_band(2 * bx + 1, sibling)
    spread(by, 0)
    spread(bx, 1)
    for b, h in ((bx, 0), (by, 1), (bd, 0), (bd, 1)):
        wait_band(2 * b + h)
        send_band(2 * b + h, sibling)
        spread(b, h)
    for rel, h in ((2, 0), (1, 1), (1, 0), (2, 1), (3, 0), (3, 1)):
        b = block(rel, 1)
        wait_band(2 * b + h)
        spread(b, h)
    for rel, flip in others:
        recv_from(z_all, zb_recv, rel, flip).wait_recv()
    for b in range(n_blk):
        rs = slice(b * BLK, (b + 1) * BLK)
        zb_ref[rs, :] = z_all[b].astype(F32).T.astype(BF16)
        mass_ref[rs, :] = jnp.sum(kern_ref[rs, :].astype(F32), axis=1, keepdims=True)
    for rel in range(4):
        sib_copy(rel).wait_send()
    for cp in rs_copies.values():
        cp.wait_send()
    for i in range(len(others)):
        z_copy(i).wait_send()
        sq_copy(i).wait_send()
        zb_copy(i).wait_send()
    for cp in sent:
        cp.wait_send()


def kernel_matrix(src, proj, two_over_h, collective_id, from_gram):
    rank, n_rows = proj.shape
    n_blk = n_rows // BLK
    dma = lambda *n: pltpu.SemaphoreType.DMA(n)
    scratch = [
        pltpu.VMEM((4, 2, HALF, WIDE), F32), pltpu.VMEM((4, 2, HALF, WIDE), F32),
        pltpu.VMEM((2, HALF, WIDE), F32), pltpu.VMEM((2, HALF, WIDE), F32),
        pltpu.VMEM((HALF, WIDE), F32), pltpu.VMEM((HALF, WIDE), F32),
        pltpu.VMEM((8, 4, 1, BLK), F32), pltpu.VMEM((1, n_rows + (REACH - 1) * BLK), F32),
        pltpu.VMEM((n_blk, rank, BLK), F32), pltpu.VMEM((n_blk, rank, BLK), BF16),
        pltpu.VMEM((2 * n_blk, HALF, WIDE), BF16),
        dma(4), dma(4), dma(6), dma(6), dma(7), dma(8), dma(7), dma(8), dma(7), dma(8), dma(14), dma(16), dma(4)]
    if not from_gram:
        scratch += [pltpu.VMEM(src.shape, BF16), pltpu.VMEM((4, 2, HALF, WIDE), F32), dma(n_blk)]
    return pl.pallas_call(
        functools.partial(kmat_kernel, from_gram, two_over_h),
        out_shape=(jax.ShapeDtypeStruct((n_rows, n_rows), BF16), jax.ShapeDtypeStruct((n_rows, rank), BF16),
                   jax.ShapeDtypeStruct((n_rows, 1), F32)),
        in_specs=[ANY, VMEM], out_specs=(VMEM, VMEM, VMEM), scratch_shapes=scratch,
        compiler_params=pltpu.CompilerParams(collective_id=collective_id, has_side_effects=True, vmem_limit_bytes=VMEM_LIMIT),
    )(src, proj)


def solution(mesh):
    part_size = mesh.shape["part"]
    feat_size = mesh.shape["feat"]

    def local_steps(theta, prec_loc, mean_loc, factor_loc):
        rows, feat_loc = theta.shape
        n_total = rows * part_size
        feat_total = feat_loc * feat_size
        width = feat_loc // part_size
        kern_width = 2.0 * feat_total / math.log(n_total)
        step_size = 0.15 * n_total * feat_total / math.log(n_total)
        consts = (1.0 / n_total, 2.0 / kern_width, step_size)
        part = lax.axis_index("part")
        pos = part.astype(jnp.int32).reshape(1)
        mean = lax.dynamic_slice_in_dim(mean_loc, part * width, width).reshape(1, width)
        prec = lax.dynamic_slice_in_dim(prec_loc, part * width, width).reshape(1, width)
        fact_t = lax.dynamic_slice_in_dim(factor_loc, part * width, width, axis=0).T
        chunks = [(0, BLK)] + [(at, 2 * BLK) for at in range(2 * BLK, width, 2 * BLK)] + [(BLK, BLK)]
        assert chunks[-2][0] + 2 * BLK == width

        cur, gram, proj = exchange(theta, mean, fact_t, 7)
        src = gram
        for step in range(NUM_STEPS):
            kern, zb, mass = kernel_matrix(src, proj, consts[1], 1 + step, step == 0)
            if step < NUM_STEPS - 1:
                cur, src, proj = update(consts, cur, kern, mass, zb, mean, prec, fact_t, BLK)
        out = None
        received = []
        for start, tile in chunks:
            out, send = last_update(consts, pos, cur, kern, mass, zb, mean, prec, fact_t, out, start, tile)
            received.append(lax.ppermute(send, "part", [(0, 1), (1, 0)]))
        for (start, tile), recv in zip(chunks, received):
            out = place(pos, recv, out, start)
        return out

    row_spec = P(("ens", "part"), "feat")
    vec_spec = P(("ens", "feat"))
    fac_spec = P(("ens", "feat"), None)
    return jax.shard_map(local_steps, mesh=mesh, in_specs=(row_spec, vec_spec, vec_spec, fac_spec), out_specs=row_spec, check_vma=False)
```

```python
import functools
import math
import jax
import jax.numpy as jnp
from jax import lax
from jax.experimental import pallas as pl
from jax.experimental.pallas import tpu as pltpu
from jax.sharding import PartitionSpec as P

BLK = 256
HALF = BLK // 2
REACH = 5
WIDE = 9 * HALF
MESH = pl.DeviceIdType.MESH
F32 = jnp.float32
BF16 = jnp.bfloat16
ANY = pl.BlockSpec(memory_space=pl.ANY)
VMEM = pl.BlockSpec(memory_space=pltpu.VMEM)
VMEM_LIMIT = 63 * 1024 * 1024
NT = (((1,), (1,)), ((), ()))


def band_parts(k, val):
    top, low = val[:HALF], val[HALF:]
    if k == 0:
        return (0, 0, top), (1, 0, low[:, HALF:])
    if k == REACH - 1:
        top = top[:, :HALF]
    return (0, k * BLK, top), (1, k * BLK - HALF, low)


def exchange_kernel(n_chunk, theta_ref, mean_ref, fact_ref, col_ref, gram_ref, proj_ref,
                    buf, tb, send_sem, recv_sem, own_sem, put_sem, other_sem):
    part = lax.axis_index("part")
    other = 1 - part
    feat = lax.axis_index("feat")
    peer = (lax.axis_index("ens"), other, feat)
    rows, width = theta_ref.shape[0], col_ref.shape[1]
    n_rows = col_ref.shape[0]
    cw = width // n_chunk
    n_blk = n_rows // BLK
    barrier = pltpu.get_barrier_semaphore()
    pl.semaphore_signal(barrier, inc=1, device_id=peer, device_id_type=MESH)
    pl.semaphore_wait(barrier, 1)
    own_rows = pl.ds(pl.multiple_of(part * rows, BLK), rows)
    other_rows = pl.ds(pl.multiple_of(other * rows, BLK), rows)

    def remote(c):
        return pltpu.make_async_remote_copy(
            src_ref=theta_ref.at[:, pl.ds(pl.multiple_of(other * width + c * cw, 128), cw)],
            dst_ref=col_ref.at[own_rows, pl.ds(pl.multiple_of(c * cw, 128), cw)],
            send_sem=send_sem.at[c], recv_sem=recv_sem.at[c], device_id=peer, device_id_type=MESH)

    def fetch_own(c):
        return pltpu.make_async_copy(
            theta_ref.at[:, pl.ds(pl.multiple_of(part * width + c * cw, 128), cw)],
            buf.at[own_rows, :], own_sem)

    def put_own(c):
        return pltpu.make_async_copy(
            buf.at[own_rows, :], col_ref.at[own_rows, pl.ds(pl.multiple_of(c * cw, 128), cw)], put_sem)

    def fetch_other(c):
        return pltpu.make_async_copy(
            col_ref.at[other_rows, pl.ds(pl.multiple_of(c * cw, 128), cw)], buf.at[other_rows, :], other_sem)

    @pl.loop(0, n_chunk)
    def _(c):
        remote(c).start()

    gram_ref[...] = jnp.zeros_like(gram_ref)
    proj_ref[...] = jnp.zeros_like(proj_ref)

    @pl.loop(0, n_chunk)
    def _(c):
        fetch_own(c).start()
        fetch_own(c).wait()
        put_own(c).start()
        remote(c).wait_recv()
        fetch_other(c).start()
        fetch_other(c).wait()
        cols = pl.ds(pl.multiple_of(c * cw, 128), cw)
        fact = fact_ref[:, cols]
        mean = mean_ref[:, cols]

        @pl.loop(0, n_blk)
        def _(b):
            rs = pl.ds(pl.multiple_of(b * BLK, BLK), BLK)
            th = buf[rs, :]
            tb[rs, :] = th.astype(BF16)
            proj_ref[:, rs] += lax.dot_general(fact, (th - mean).astype(BF16), NT, preferred_element_type=F32)

        for b in range(n_blk):
            rows_b = tb[b * BLK:(b + 1) * BLK, :]
            for k in range(REACH):
                j = (b + k) % n_blk
                val = lax.dot_general(rows_b, tb[j * BLK:(j + 1) * BLK, :], NT, preferred_element_type=F32)
                for h, col, piece in band_parts(k, val):
                    gram_ref[b, h, :, col:col + piece.shape[1]] += piece
        put_own(c).wait()

    @pl.loop(0, n_chunk)
    def _(c):
        remote(c).wait_send()


def exchange(theta, mean, fact_t, n_chunk):
    rows, feat = theta.shape
    width = feat // 2
    n_rows = rows * 2
    rank = fact_t.shape[0]
    return pl.pallas_call(
        functools.partial(exchange_kernel, n_chunk),
        out_shape=(jax.ShapeDtypeStruct((n_rows, width), F32),
                   jax.ShapeDtypeStruct((n_rows // BLK, 2, HALF, WIDE), F32),
                   jax.ShapeDtypeStruct((rank, n_rows), F32)),
        in_specs=[ANY, VMEM, VMEM], out_specs=(ANY, VMEM, VMEM),
        scratch_shapes=[
            pltpu.VMEM((n_rows, width // n_chunk), F32),
            pltpu.VMEM((n_rows, width // n_chunk), BF16),
            pltpu.SemaphoreType.DMA((n_chunk,)), pltpu.SemaphoreType.DMA((n_chunk,)),
            pltpu.SemaphoreType.DMA, pltpu.SemaphoreType.DMA, pltpu.SemaphoreType.DMA],
        compiler_params=pltpu.CompilerParams(collective_id=0, has_side_effects=True, vmem_limit_bytes=VMEM_LIMIT),
        name="exchange",
    )(theta, mean, fact_t)


def build_rhs(theta_ref, mean, prec, fact, zb_ref, rhs, rs):
    tile = theta_ref.shape[1]
    th = theta_ref[rs, :]
    low = jnp.dot(zb_ref[rs, :], fact, preferred_element_type=F32)
    rhs[rs, :tile] = (-((th - mean) * prec + low)).astype(BF16)
    rhs[rs, tile:] = th.astype(BF16)


def stepped(theta_ref, acc, mass_ref, rs, inv_n, two_over_h, step_size):
    tile = theta_ref.shape[1]
    th = theta_ref[rs, :]
    pull = mass_ref[rs, :] * th.astype(BF16).astype(F32) - acc[:, tile:]
    return th + step_size * ((acc[:, :tile] + two_over_h * pull) * inv_n)


def update_kernel(consts, theta_ref, next_ref, kern_ref, mass_ref, zb_ref, mean_ref, prec_ref, fact_ref,
                  mean_n, prec_n, fact_n, *rest):
    out_ref, tb_ref, proj_ref, rhs = rest[-4:]
    n_rows = theta_ref.shape[0]
    big = n_rows // 2
    slot = lax.rem(pl.program_id(0), 2)

    @pl.when(pl.program_id(0) == 0)
    def _():
        proj_ref[...] = rest[0][...] if len(rest) > 4 else jnp.zeros_like(proj_ref)

        @pl.loop(0, n_rows // BLK)
        def _(b):
            build_rhs(theta_ref, mean_ref[...], prec_ref[...], fact_ref[...], zb_ref, rhs.at[0],
                      pl.ds(pl.multiple_of(b * BLK, BLK), BLK))

    @pl.loop(0, 2)
    def _(b):
        rs = pl.ds(pl.multiple_of(b * big, big), big)
        acc = jnp.dot(kern_ref[rs, :], rhs[slot], preferred_element_type=F32)
        build_rhs(next_ref, mean_n[...], prec_n[...], fact_n[...], zb_ref, rhs.at[1 - slot], rs)
        new = stepped(theta_ref, acc, mass_ref, rs, *consts)
        out_ref[rs, :] = new
        tb_ref[rs, :] = new.astype(BF16)
        proj_ref[:, rs] += lax.dot_general(fact_ref[...], (new - mean_ref[...]).astype(BF16), NT, preferred_element_type=F32)


def update(consts, theta, kern, mass, zb, mean, prec, fact_t, tile, start, stop, own_out, before=None):
    n_rows, width = theta.shape
    rank = fact_t.shape[0]
    first, steps = start // tile, (stop - start) // tile
    col = lambda r: pl.BlockSpec((r, tile), lambda i: (0, first + i))
    nxt = lambda r: pl.BlockSpec((r, tile), lambda i: (0, first + jnp.minimum(i + 1, steps - 1)))
    in_specs = [col(n_rows), nxt(n_rows), VMEM, VMEM, VMEM, col(1), col(1), col(rank), nxt(1), nxt(1), nxt(rank)]
    args = [theta, theta, kern, mass, zb, mean, prec, fact_t, mean, prec, fact_t]
    alias = {}
    if before is not None:
        in_specs += [VMEM, ANY]
        args += [before[1], before[0]]
        alias = {12: 1}
    return pl.pallas_call(
        functools.partial(update_kernel, consts),
        grid=(steps,),
        out_shape=(jax.ShapeDtypeStruct((n_rows, stop - start if own_out else width), F32),
                   jax.ShapeDtypeStruct((n_rows, width), BF16),
                   jax.ShapeDtypeStruct((rank, n_rows), F32)),
        in_specs=in_specs,
        out_specs=(pl.BlockSpec((n_rows, tile), lambda i: (0, i)) if own_out else col(n_rows), col(n_rows), VMEM),
        scratch_shapes=[pltpu.VMEM((2, n_rows, 2 * tile), BF16)],
        input_output_aliases=alias,
        compiler_params=pltpu.CompilerParams(vmem_limit_bytes=VMEM_LIMIT),
        cost_estimate=pl.CostEstimate(flops=4 * n_rows * n_rows * (stop - start), bytes_accessed=10 * n_rows * (stop - start), transcendentals=0),
    )(*args)


def last_kernel(consts, pos_ref, theta_ref, kern_ref, mass_ref, zb_ref, mean_ref, prec_ref, fact_ref, *rest):
    out_ref, send_ref, rhs = rest[-3:]
    rows = out_ref.shape[0]
    n_blk = theta_ref.shape[0] // BLK
    part = pos_ref[0]
    fact, mean, prec = fact_ref[...], mean_ref[...], prec_ref[...]

    @pl.loop(0, n_blk)
    def _(b):
        build_rhs(theta_ref, mean, prec, fact, zb_ref, rhs, pl.ds(pl.multiple_of(b * BLK, BLK), BLK))

    for dst, which in ((send_ref, 1 - part), (out_ref, part)):
        @pl.loop(0, rows // BLK)
        def _(b):
            rs = pl.ds(pl.multiple_of(which * rows + b * BLK, BLK), BLK)
            acc = jnp.dot(kern_ref[rs, :], rhs[...], preferred_element_type=F32)
            dst[pl.ds(pl.multiple_of(b * BLK, BLK), BLK), :] = stepped(theta_ref, acc, mass_ref, rs, *consts)


def last_update(consts, pos, theta, kern, mass, zb, mean, prec, fact_t, out, start, tile):
    n_rows, width = theta.shape
    chunk = start // tile
    rank = fact_t.shape[0]
    rows, feat = n_rows // 2, width * 2
    per = width // tile
    col = lambda r: pl.BlockSpec((r, tile), lambda i, pos: (0, chunk))
    in_specs = [col(n_rows), VMEM, VMEM, VMEM, col(1), col(1), col(rank)]
    args = [theta, kern, mass, zb, mean, prec, fact_t]
    alias = {}
    if out is not None:
        in_specs.append(ANY)
        args.append(out)
        alias = {8: 0}
    return pl.pallas_call(
        functools.partial(last_kernel, consts),
        grid_spec=pltpu.PrefetchScalarGridSpec(
            num_scalar_prefetch=1, grid=(1,), in_specs=in_specs,
            out_specs=(pl.BlockSpec((rows, tile), lambda i, pos: (0, pos[0] * per + chunk)),
                       pl.BlockSpec((rows, tile), lambda i, pos: (0, 0))),
            scratch_shapes=[pltpu.VMEM((n_rows, 2 * tile), BF16)]),
        out_shape=(jax.ShapeDtypeStruct((rows, feat), F32), jax.ShapeDtypeStruct((rows, tile), F32)),
        input_output_aliases=alias,
        compiler_params=pltpu.CompilerParams(vmem_limit_bytes=VMEM_LIMIT),
        cost_estimate=pl.CostEstimate(flops=4 * n_rows * n_rows * tile, bytes_accessed=10 * n_rows * tile, transcendentals=0),
    )(pos, *args)


def own_kernel(consts, pos_ref, theta_ref, kern_ref, mass_ref, zb_ref, mean_ref, prec_ref, fact_ref, base_ref, out_ref, rhs):
    rows = out_ref.shape[0]
    fact, mean, prec = fact_ref[...], mean_ref[...], prec_ref[...]

    @pl.loop(0, theta_ref.shape[0] // BLK)
    def _(b):
        build_rhs(theta_ref, mean, prec, fact, zb_ref, rhs, pl.ds(pl.multiple_of(b * BLK, BLK), BLK))

    @pl.loop(0, rows // BLK)
    def _(b):
        rs = pl.ds(pl.multiple_of(pos_ref[0] * rows + b * BLK, BLK), BLK)
        acc = jnp.dot(kern_ref[rs, :], rhs[...], preferred_element_type=F32)
        out_ref[pl.ds(pl.multiple_of(b * BLK, BLK), BLK), :] = stepped(theta_ref, acc, mass_ref, rs, *consts)


def own_update(consts, pos, theta, kern, mass, zb, mean, prec, fact_t, out, foreign):
    n_rows, cols = theta.shape
    rank = fact_t.shape[0]
    rows, feat = out.shape
    per = feat // (2 * BLK)
    col = lambda r: pl.BlockSpec((r, BLK), lambda i, pos: (0, i))
    where = (lambda i, pos: (0, (1 - pos[0]) * per + i)) if foreign else (lambda i, pos: (0, pos[0] * per + i))
    return pl.pallas_call(
        functools.partial(own_kernel, consts),
        grid_spec=pltpu.PrefetchScalarGridSpec(
            num_scalar_prefetch=1, grid=(cols // BLK,),
            in_specs=[col(n_rows), VMEM, VMEM, VMEM, col(1), col(1), col(rank), ANY],
            out_specs=pl.BlockSpec((rows, BLK), where),
            scratch_shapes=[pltpu.VMEM((n_rows, 2 * BLK), BF16)]),
        out_shape=jax.ShapeDtypeStruct(out.shape, F32),
        input_output_aliases={8: 0},
        compiler_params=pltpu.CompilerParams(vmem_limit_bytes=VMEM_LIMIT),
        cost_estimate=pl.CostEstimate(flops=4 * rows * n_rows * cols, bytes_accessed=10 * n_rows * cols, transcendentals=0),
        name="own_foreign" if foreign else "own_shared",
    )(pos, theta, kern, mass, zb, mean, prec, fact_t, out)


def place_kernel(pos_ref, recv_ref, base_ref, out_ref):
    out_ref[...] = recv_ref[...]


def place(pos, recv, out, start):
    rows, tile = recv.shape
    per = out.shape[1] // 256
    sub = tile // 128
    first = start // 128
    return pl.pallas_call(
        place_kernel,
        grid_spec=pltpu.PrefetchScalarGridSpec(
            num_scalar_prefetch=1, grid=(sub,), in_specs=[pl.BlockSpec((rows, 128), lambda i, pos: (0, i)), ANY],
            out_specs=pl.BlockSpec((rows, 128), lambda i, pos: (0, (1 - pos[0]) * per + first + i))),
        out_shape=jax.ShapeDtypeStruct(out.shape, out.dtype),
        input_output_aliases={2: 0},
        cost_estimate=pl.CostEstimate(flops=1000 * rows * tile, bytes_accessed=8 * rows * tile, transcendentals=0),
    )(pos, recv, out)


def kmat_kernel(from_gram, two_over_h, src_ref, proj_ref, kern_ref, zb_ref, mass_ref, *scratch):
    if from_gram:
        tb, sib_out = None, None
    else:
        tb, sib_out, load_sem = scratch[-3:]
    (gbuf, sib_in, r_x1, r_y1, r_x2, r_y2, sq_parts, sq, z_in, z_all, kbuf,
     sib_send, sib_recv, rs_send, rs_recv, sq_send, sq_recv, z_send, z_recv, zb_send, zb_recv,
     k_send, k_recv, loc_sem) = scratch[:24]
    n_rows = kern_ref.shape[0]
    n_blk = n_rows // BLK
    ens, part, feat = lax.axis_index("ens"), lax.axis_index("part"), lax.axis_index("feat")
    x, core = feat // 2, lax.rem(feat, 2)

    def chip(rel):
        return lax.rem(part + rel // 2, 2), lax.rem(x + rel % 2, 2)

    def block(rel, flip):
        cy, cx = chip(rel)
        return cy * 4 + cx * 2 + lax.rem(core + flip, 2)

    def device(rel, flip):
        cy, cx = chip(rel)
        return (ens, cy, cx * 2 + lax.rem(core + flip, 2))

    me = block(0, 0)
    sibling, dev_x, dev_y = device(0, 1), device(1, 0), device(2, 0)
    others = [(rel, flip) for rel in (3, 1, 2, 0) for flip in (0, 1) if (rel, flip) != (0, 0)]

    def rcopy(src, dst, ssem, rsem, dev):
        return pltpu.make_async_remote_copy(src_ref=src, dst_ref=dst, send_sem=ssem, recv_sem=rsem,
                                            device_id=dev, device_id_type=MESH)

    barrier = pltpu.get_barrier_semaphore()
    for rel, flip in others:
        pl.semaphore_signal(barrier, inc=1, device_id=device(rel, flip), device_id_type=MESH)

    def load(b):
        rs = pl.ds(b * BLK, BLK)
        return pltpu.make_async_copy(src_ref.at[rs, :], tb.at[rs, :], load_sem.at[b])

    def own_gram(rel):
        return pltpu.make_async_copy(src_ref.at[block(rel, 0)], gbuf.at[rel], loc_sem.at[rel])

    if from_gram:
        for rel in (3, 2, 1, 0):
            own_gram(rel).start()
    else:
        for b in range(n_blk):
            load(b).start()
    pl.semaphore_wait(barrier, len(others))

    def z_cols(b):
        return proj_ref.at[:, pl.ds(pl.multiple_of(b * BLK, BLK), BLK)]

    def z_copy(i):
        rel, flip = others[i]
        return rcopy(z_cols(block(rel, flip)), z_in.at[me], z_send.at[i], z_recv.at[me], device(rel, flip))

    for i in range(len(others)):
        z_copy(i).start()
    z_own = pltpu.make_async_copy(z_cols(me), z_in.at[me], z_recv.at[me])
    z_own.start()

    def sib_copy(rel):
        src = src_ref.at[block(rel, 1)] if from_gram else sib_out.at[rel]
        return rcopy(src, sib_in.at[rel], sib_send.at[rel], sib_recv.at[rel], sibling)

    lo, hi = 0, 1
    rs_copies = {
        "d_lo": rcopy(gbuf.at[3, lo], r_x1.at[0], rs_send.at[0], rs_recv.at[0], dev_x),
        "d_hi": rcopy(gbuf.at[3, hi], r_y1.at[0], rs_send.at[1], rs_recv.at[1], dev_y),
        "y_hi": rcopy(gbuf.at[2, hi], r_y1.at[1], rs_send.at[2], rs_recv.at[2], dev_y),
        "x_lo": rcopy(gbuf.at[1, lo], r_x1.at[1], rs_send.at[3], rs_recv.at[3], dev_x),
        "y_lo": rcopy(gbuf.at[2, lo], r_y2, rs_send.at[4], rs_recv.at[4], dev_y),
        "x_hi": rcopy(gbuf.at[1, hi], r_x2, rs_send.at[5], rs_recv.at[5], dev_x),
    }
    eye = (lax.broadcasted_iota(jnp.int32, (HALF, HALF), 0) == lax.broadcasted_iota(jnp.int32, (HALF, HALF), 1)).astype(F32)

    def merge(rel):
        sib_copy(rel).wait_recv()
        gbuf[rel] += sib_in[rel]

    def first_sends(rel):
        for name in {3: ("d_lo", "d_hi"), 2: ("y_hi",), 1: ("x_lo",), 0: ()}[rel]:
            rs_copies[name].start()

    if from_gram:
        for rel in (3, 2, 1, 0):
            sib_copy(rel).start()
        for rel in (3, 2, 1, 0):
            own_gram(rel).wait()
            merge(rel)
            first_sends(rel)
    else:
        def bands_of(b, dst):
            rows = tb[pl.ds(pl.multiple_of(b * BLK, BLK), BLK), :]
            for k in range(REACH):
                j = lax.rem(b + k, n_blk)
                val = lax.dot_general(
                    rows, tb[pl.ds(pl.multiple_of(j * BLK, BLK), BLK), :], NT, preferred_element_type=F32)
                for h, col, piece in band_parts(k, val):
                    dst[h, :, col:col + piece.shape[1]] = piece

        for b in range(n_blk):
            load(b).wait()

        @pl.loop(0, 4)
        def _(i):
            rel = 3 - i
            cy, cx = lax.rem(part + rel // 2, 2), lax.rem(x + lax.rem(rel, 2), 2)
            base = cy * 4 + cx * 2
            bands_of(base + 1 - core, sib_out.at[rel])
            rcopy(sib_out.at[rel], sib_in.at[rel], sib_send.at[rel], sib_recv.at[rel], sibling).start()
            bands_of(base + core, gbuf.at[rel])
            rcopy(sib_out.at[rel], sib_in.at[rel], sib_send.at[rel], sib_recv.at[rel], sibling).wait_recv()
            gbuf[rel] += sib_in[rel]
            for r in (3, 2, 1):
                @pl.when(rel == r)
                def _():
                    first_sends(r)

    for rel in range(4):
        cy, cx = chip(rel)
        for h in range(2):
            sq_parts[me, cy * 2 + cx, :, h * HALF:(h + 1) * HALF] = jnp.sum(gbuf[rel, h, :, :HALF] * eye, axis=0, keepdims=True)

    def sq_copy(i):
        rel, flip = others[i]
        return rcopy(sq_parts.at[me], sq_parts.at[me], sq_send.at[i], sq_recv.at[me], device(rel, flip))

    def recv_from(buf, sem, rel, flip):
        b = block(rel, flip)
        return rcopy(buf.at[b], buf.at[b], sq_send.at[0], sem.at[b], sibling)

    for i in range(len(others)):
        sq_copy(i).start()

    rs_copies["d_lo"].wait_recv()
    gbuf[2, 0] += r_x1[0]
    rs_copies["y_lo"].start()
    rs_copies["d_hi"].wait_recv()
    gbuf[1, 1] += r_y1[0]
    rs_copies["x_hi"].start()

    z_own.wait()
    for rel, flip in others:
        recv_from(z_in, z_recv, rel, flip).wait_recv()
    z_sum = z_in[0]
    for b in range(1, n_blk):
        z_sum = z_sum + z_in[b]
    z_all[me] = z_sum.astype(BF16)

    def zb_copy(i):
        rel, flip = others[i]
        return rcopy(z_all.at[me], z_all.at[me], zb_send.at[i], zb_recv.at[me], device(rel, flip))

    for i in range(len(others)):
        zb_copy(i).start()
    for rel, flip in others:
        recv_from(sq_parts, sq_recv, rel, flip).wait_recv()
    for c in range(2):
        for q in range(4):
            s = sq_parts[c, q] + sq_parts[2 + c, q] + sq_parts[4 + c, q] + sq_parts[6 + c, q]
            b = 2 * q + c
            sq[:, b * BLK:(b + 1) * BLK] = s
            if b < REACH - 1:
                sq[:, n_rows + b * BLK:n_rows + (b + 1) * BLK] = s

    def kernel_of(h, gram):
        row = sq[:, pl.ds(pl.multiple_of((2 * me + h) * HALF, HALF), WIDE)]
        col = jnp.sum(eye * row[:, :HALF], axis=1, keepdims=True)
        return jnp.exp(-jnp.maximum(col + row - 2.0 * gram, 0.0) * (0.5 * two_over_h)).astype(BF16)

    slots = iter(range(14))
    sent = []

    def send_band(idx, dev):
        s = next(slots)
        cp = rcopy(kbuf.at[idx], kbuf.at[idx], k_send.at[s], k_recv.at[idx], dev)
        cp.start()
        sent.append(cp)

    def wait_band(idx):
        rcopy(kbuf.at[idx], kbuf.at[idx], k_send.at[0], k_recv.at[idx], sibling).wait_recv()

    def spread(b, h):
        idx = 2 * b + h
        row0 = pl.multiple_of(idx * HALF, HALF)
        for k in range(REACH * 2 - 1):
            col0 = pl.multiple_of(lax.rem(idx + k, 2 * n_blk) * HALF, HALF)
            tile = kbuf[idx, :, k * HALF:(k + 1) * HALF]
            kern_ref[pl.ds(row0, HALF), pl.ds(col0, HALF)] = tile
            if 0 < k < REACH * 2 - 2:
                kern_ref[pl.ds(col0, HALF), pl.ds(row0, HALF)] = tile.T

    rs_copies["x_lo"].wait_recv()
    rs_copies["y_lo"].wait_recv()
    kbuf[2 * me] = kernel_of(0, gbuf[0, 0] + (r_x1[1] + r_y2[...]))
    for dev in (dev_y, sibling):
        send_band(2 * me, dev)
    rs_copies["y_hi"].wait_recv()
    rs_copies["x_hi"].wait_recv()
    kbuf[2 * me + 1] = kernel_of(1, gbuf[0, 1] + (r_y1[1] + r_x2[...]))
    for dev in (dev_x, sibling):
        send_band(2 * me + 1, dev)
    send_band(2 * me, dev_x)
    send_band(2 * me + 1, dev_y)
    spread(me, 0)
    spread(me, 1)
    sib = block(0, 1)
    for h in range(2):
        wait_band(2 * sib + h)
        spread(sib, h)
    bx, by, bd = block(1, 0), block(2, 0), block(3, 0)
    wait_band(2 * by)
    send_band(2 * by, dev_x)
    send_band(2 * by, sibling)
    wait_band(2 * bx + 1)
    send_band(2 * bx + 1, dev_y)
    send_band(2 * bx + 1, sibling)
    spread(by, 0)
    spread(bx, 1)
    for b, h in ((bx, 0), (by, 1), (bd, 0), (bd, 1)):
        wait_band(2 * b + h)
        send_band(2 * b + h, sibling)
        spread(b, h)
    for rel, h in ((2, 0), (1, 1), (1, 0), (2, 1), (3, 0), (3, 1)):
        b = block(rel, 1)
        wait_band(2 * b + h)
        spread(b, h)
    for rel, flip in others:
        recv_from(z_all, zb_recv, rel, flip).wait_recv()
    for b in range(n_blk):
        rs = slice(b * BLK, (b + 1) * BLK)
        zb_ref[rs, :] = z_all[b].astype(F32).T.astype(BF16)
        mass_ref[rs, :] = jnp.sum(kern_ref[rs, :].astype(F32), axis=1, keepdims=True)
    for rel in range(4):
        sib_copy(rel).wait_send()
    for cp in rs_copies.values():
        cp.wait_send()
    for i in range(len(others)):
        z_copy(i).wait_send()
        sq_copy(i).wait_send()
        zb_copy(i).wait_send()
    for cp in sent:
        cp.wait_send()


def kernel_matrix(src, proj, two_over_h, collective_id, from_gram):
    rank, n_rows = proj.shape
    n_blk = n_rows // BLK
    dma = lambda *n: pltpu.SemaphoreType.DMA(n)
    scratch = [
        pltpu.VMEM((4, 2, HALF, WIDE), F32), pltpu.VMEM((4, 2, HALF, WIDE), F32),
        pltpu.VMEM((2, HALF, WIDE), F32), pltpu.VMEM((2, HALF, WIDE), F32),
        pltpu.VMEM((HALF, WIDE), F32), pltpu.VMEM((HALF, WIDE), F32),
        pltpu.VMEM((8, 4, 1, BLK), F32), pltpu.VMEM((1, n_rows + (REACH - 1) * BLK), F32),
        pltpu.VMEM((n_blk, rank, BLK), F32), pltpu.VMEM((n_blk, rank, BLK), BF16),
        pltpu.VMEM((2 * n_blk, HALF, WIDE), BF16),
        dma(4), dma(4), dma(6), dma(6), dma(7), dma(8), dma(7), dma(8), dma(7), dma(8), dma(14), dma(16), dma(4)]
    if not from_gram:
        scratch += [pltpu.VMEM(src.shape, BF16), pltpu.VMEM((4, 2, HALF, WIDE), F32), dma(n_blk)]
    return pl.pallas_call(
        functools.partial(kmat_kernel, from_gram, two_over_h),
        out_shape=(jax.ShapeDtypeStruct((n_rows, n_rows), BF16), jax.ShapeDtypeStruct((n_rows, rank), BF16),
                   jax.ShapeDtypeStruct((n_rows, 1), F32)),
        in_specs=[ANY, VMEM], out_specs=(VMEM, VMEM, VMEM), scratch_shapes=scratch,
        compiler_params=pltpu.CompilerParams(collective_id=collective_id, has_side_effects=True, vmem_limit_bytes=VMEM_LIMIT),
    )(src, proj)


def solution(mesh):
    part_size = mesh.shape["part"]
    feat_size = mesh.shape["feat"]

    def local_steps(theta, prec_loc, mean_loc, factor_loc):
        rows, feat_loc = theta.shape
        n_total = rows * part_size
        feat_total = feat_loc * feat_size
        width = feat_loc // part_size
        kern_width = 2.0 * feat_total / math.log(n_total)
        step_size = 0.15 * n_total * feat_total / math.log(n_total)
        consts = (1.0 / n_total, 2.0 / kern_width, step_size)
        part = lax.axis_index("part")
        pos = part.astype(jnp.int32).reshape(1)
        mean = lax.dynamic_slice_in_dim(mean_loc, part * width, width).reshape(1, width)
        prec = lax.dynamic_slice_in_dim(prec_loc, part * width, width).reshape(1, width)
        fact_t = lax.dynamic_slice_in_dim(factor_loc, part * width, width, axis=0).T
        shared = 2 * BLK
        chunks = [(shared, HALF)] + [(at, 2 * BLK) for at in range(2 * shared, width, 2 * BLK)] + [(shared + BLK, BLK), (shared + HALF, HALF)]
        swap = [(0, 1), (1, 0)]
        mean_f = lax.dynamic_slice_in_dim(mean_loc, (1 - part) * width, shared).reshape(1, shared)
        prec_f = lax.dynamic_slice_in_dim(prec_loc, (1 - part) * width, shared).reshape(1, shared)
        fact_f = lax.dynamic_slice_in_dim(factor_loc, (1 - part) * width, shared, axis=0).T

        cur, gram, proj = exchange(theta, mean, fact_t, 7)
        params = (mean, prec, fact_t)
        kern, zb, mass = kernel_matrix(gram, proj, consts[1], 1, True)
        cur, tb, proj = update(consts, cur, kern, mass, zb, *params, BLK, 0, width, False)
        kern, zb, mass = kernel_matrix(tb, proj, consts[1], 2, False)
        both, tb, proj = update(consts, cur, kern, mass, zb, *params, BLK, 0, shared, True)
        foreign = lax.ppermute(both, "part", swap)
        cur, tb, proj = update(consts, cur, kern, mass, zb, *params, BLK, shared, width, False, (tb, proj))
        kern, zb, mass = kernel_matrix(tb, proj, consts[1], 3, False)
        out = None
        received = []
        for start, tile in chunks:
            out, send = last_update(consts, pos, cur, kern, mass, zb, *params, out, start, tile)
            received.append(lax.ppermute(send, "part", swap))
        out = own_update(consts, pos, both, kern, mass, zb, *params, out, False)
        out = own_update(consts, pos, foreign, kern, mass, zb, mean_f, prec_f, fact_f, out, True)
        for (start, tile), recv in zip(chunks, received):
            out = place(pos, recv, out, start)
        return out

    row_spec = P(("ens", "part"), "feat")
    vec_spec = P(("ens", "feat"))
    fac_spec = P(("ens", "feat"), None)
    return jax.shard_map(local_steps, mesh=mesh, in_specs=(row_spec, vec_spec, vec_spec, fac_spec), out_specs=row_spec, check_vma=False)
```

```python
import functools
import math
import jax
import jax.numpy as jnp
from jax import lax
from jax.experimental import pallas as pl
from jax.experimental.pallas import tpu as pltpu
from jax.sharding import PartitionSpec as P

BLK = 256
HALF = BLK // 2
REACH = 5
WIDE = 9 * HALF
MESH = pl.DeviceIdType.MESH
F32 = jnp.float32
BF16 = jnp.bfloat16
ANY = pl.BlockSpec(memory_space=pl.ANY)
VMEM = pl.BlockSpec(memory_space=pltpu.VMEM)
VMEM_LIMIT = 63 * 1024 * 1024
NT = (((1,), (1,)), ((), ()))


def band_parts(k, val):
    top, low = val[:HALF], val[HALF:]
    if k == 0:
        return (0, 0, top), (1, 0, low[:, HALF:])
    if k == REACH - 1:
        top = top[:, :HALF]
    return (0, k * BLK, top), (1, k * BLK - HALF, low)


def exchange_kernel(n_early, n_late, theta_ref, mean_ref, fact_ref, col_ref, gram_ref, proj_ref,
                    buf, tb, away, away_b, late_b, send_sem, recv_sem, lsend_sem, lrecv_sem, own_sem, put_sem, other_sem):
    part = lax.axis_index("part")
    other = 1 - part
    peer = (lax.axis_index("ens"), other, lax.axis_index("feat"))
    rows, width = theta_ref.shape[0], col_ref.shape[1]
    n_rows = col_ref.shape[0]
    cw = width // (n_early + n_late)
    n_blk = n_rows // BLK
    barrier = pltpu.get_barrier_semaphore()
    pl.semaphore_signal(barrier, inc=1, device_id=peer, device_id_type=MESH)
    pl.semaphore_wait(barrier, 1)
    own_rows = pl.ds(pl.multiple_of(part * rows, BLK), rows)
    other_rows = pl.ds(pl.multiple_of(other * rows, BLK), rows)

    def chunk(half, c):
        return pl.ds(pl.multiple_of(half * width + c * cw, 128), cw)

    def remote(c):
        return pltpu.make_async_remote_copy(
            src_ref=theta_ref.at[:, chunk(other, c)], dst_ref=col_ref.at[own_rows, chunk(0, c)],
            send_sem=send_sem.at[c], recv_sem=recv_sem.at[c], device_id=peer, device_id_type=MESH)

    def remote_late(c):
        return pltpu.make_async_remote_copy(
            src_ref=away_b.at[c], dst_ref=late_b.at[c],
            send_sem=lsend_sem.at[c], recv_sem=lrecv_sem.at[c], device_id=peer, device_id_type=MESH)

    def fetch_own(c):
        return pltpu.make_async_copy(theta_ref.at[:, chunk(part, c)], buf.at[own_rows, :], own_sem)

    def put_own(c):
        return pltpu.make_async_copy(buf.at[own_rows, :], col_ref.at[own_rows, chunk(0, c)], put_sem)

    def fetch_other(c):
        return pltpu.make_async_copy(col_ref.at[other_rows, chunk(0, c)], buf.at[other_rows, :], other_sem)

    def project(src, row0, half, c, dst_row0):
        x = src[pl.ds(pl.multiple_of(row0, BLK), BLK), :] - mean_ref[:, chunk(half, c)]
        proj_ref[:, pl.ds(pl.multiple_of(dst_row0, BLK), BLK)] += lax.dot_general(
            fact_ref[:, chunk(half, c)], x.astype(BF16), NT, preferred_element_type=F32)

    def add_gram():
        for b in range(n_blk):
            rows_b = tb[b * BLK:(b + 1) * BLK, :]
            for k in range(REACH):
                j = (b + k) % n_blk
                val = lax.dot_general(rows_b, tb[j * BLK:(j + 1) * BLK, :], NT, preferred_element_type=F32)
                for h, col, piece in band_parts(k, val):
                    gram_ref[b, h, :, col:col + piece.shape[1]] += piece

    @pl.loop(0, n_early)
    def _(c):
        remote(c).start()

    gram_ref[...] = jnp.zeros_like(gram_ref)
    proj_ref[...] = jnp.zeros_like(proj_ref)

    @pl.loop(0, n_late)
    def _(c):
        fetch = pltpu.make_async_copy(theta_ref.at[:, chunk(other, n_early + c)], away, other_sem)
        fetch.start()
        fetch.wait()

        @pl.loop(0, rows // BLK)
        def _(b):
            rs = pl.ds(pl.multiple_of(b * BLK, BLK), BLK)
            away_b[c, rs, :] = away[rs, :].astype(BF16)
            project(away, b * BLK, other, n_early + c, part * rows + b * BLK)

    @pl.loop(0, n_late)
    def _(c):
        remote_late(c).start()

    @pl.loop(0, n_early + n_late)
    def _(c):
        fetch_own(c).start()
        fetch_own(c).wait()
        put_own(c).start()

        @pl.loop(0, rows // BLK)
        def _(b):
            row0 = part * rows + b * BLK
            rs = pl.ds(pl.multiple_of(row0, BLK), BLK)
            tb[rs, :] = buf[rs, :].astype(BF16)
            project(buf, row0, part, c, row0)

        @pl.when(c < n_early)
        def _():
            remote(c).wait_recv()
            fetch_other(c).start()
            fetch_other(c).wait()

            @pl.loop(0, rows // BLK)
            def _(b):
                row0 = other * rows + b * BLK
                rs = pl.ds(pl.multiple_of(row0, BLK), BLK)
                tb[rs, :] = buf[rs, :].astype(BF16)
                project(buf, row0, part, c, row0)

        @pl.when(c >= n_early)
        def _():
            remote_late(c - n_early).wait_recv()
            tb[other_rows, :] = late_b[c - n_early]

        add_gram()
        put_own(c).wait()

    @pl.loop(0, n_early)
    def _(c):
        remote(c).wait_send()

    @pl.loop(0, n_late)
    def _(c):
        remote_late(c).wait_send()


def exchange(theta, mean, fact_t, n_early, n_late):
    rows, feat = theta.shape
    width = feat // 2
    n_rows = rows * 2
    cw = width // (n_early + n_late)
    dma = lambda *n: pltpu.SemaphoreType.DMA(n)
    return pl.pallas_call(
        functools.partial(exchange_kernel, n_early, n_late),
        out_shape=(jax.ShapeDtypeStruct((n_rows, width), F32),
                   jax.ShapeDtypeStruct((n_rows // BLK, 2, HALF, WIDE), F32),
                   jax.ShapeDtypeStruct((fact_t.shape[0], n_rows), F32)),
        in_specs=[ANY, VMEM, VMEM], out_specs=(ANY, VMEM, VMEM),
        scratch_shapes=[
            pltpu.VMEM((n_rows, cw), F32), pltpu.VMEM((n_rows, cw), BF16), pltpu.VMEM((rows, cw), F32),
            pltpu.VMEM((n_late, rows, cw), BF16), pltpu.VMEM((n_late, rows, cw), BF16),
            dma(n_early), dma(n_early), dma(n_late), dma(n_late),
            pltpu.SemaphoreType.DMA, pltpu.SemaphoreType.DMA, pltpu.SemaphoreType.DMA],
        compiler_params=pltpu.CompilerParams(collective_id=0, has_side_effects=True, vmem_limit_bytes=VMEM_LIMIT),
        name="exchange",
    )(theta, mean, fact_t)


def columns(half, start, tile, refs):
    cols = pl.ds(pl.multiple_of(half * (refs[0].shape[1] // 2) + start, 128), tile)
    return tuple(ref[:, cols] for ref in refs)


def build_rhs(theta_ref, mean, prec, fact, zb_ref, rhs, rs):
    tile = theta_ref.shape[1]
    th = theta_ref[rs, :]
    low = jnp.dot(zb_ref[rs, :], fact, preferred_element_type=F32)
    rhs[rs, :tile] = (-((th - mean) * prec + low)).astype(BF16)
    rhs[rs, tile:] = th.astype(BF16)


def stepped(theta_ref, acc, mass_ref, rs, inv_n, two_over_h, step_size):
    tile = theta_ref.shape[1]
    th = theta_ref[rs, :]
    pull = mass_ref[rs, :] * th.astype(BF16).astype(F32) - acc[:, tile:]
    return th + step_size * ((acc[:, :tile] + two_over_h * pull) * inv_n)


def update_kernel(consts, first, theta_ref, next_ref, kern_hbm, mass_ref, zb_ref, mean_ref, prec_ref, fact_ref, *rest):
    out_ref, tb_ref, proj_ref, rhs, kern_ref, kern_sem = rest[-6:]
    n_rows, tile = theta_ref.shape
    big = n_rows // 2
    i = pl.program_id(0)
    slot = lax.rem(i, 2)
    part = lax.axis_index("part")
    refs = (mean_ref, prec_ref, fact_ref)

    @pl.when(i == 0)
    def _():
        kern_copy = pltpu.make_async_copy(kern_hbm, kern_ref, kern_sem)
        kern_copy.start()
        proj_ref[...] = rest[0][...] if len(rest) > 6 else jnp.zeros_like(proj_ref)
        now = columns(part, first * tile, tile, refs)

        @pl.loop(0, n_rows // BLK)
        def _(b):
            build_rhs(theta_ref, *now, zb_ref, rhs.at[0], pl.ds(pl.multiple_of(b * BLK, BLK), BLK))

        kern_copy.wait()

    mean, _, fact = columns(part, (first + i) * tile, tile, refs)
    after = columns(part, (first + jnp.minimum(i + 1, pl.num_programs(0) - 1)) * tile, tile, refs)

    @pl.loop(0, 2)
    def _(b):
        rs = pl.ds(pl.multiple_of(b * big, big), big)
        acc = jnp.dot(kern_ref[rs, :], rhs[slot], preferred_element_type=F32)
        build_rhs(next_ref, *after, zb_ref, rhs.at[1 - slot], rs)
        new = stepped(theta_ref, acc, mass_ref, rs, *consts)
        out_ref[rs, :] = new
        tb_ref[rs, :] = new.astype(BF16)
        proj_ref[:, rs] += lax.dot_general(fact, (new - mean).astype(BF16), NT, preferred_element_type=F32)


def update(consts, theta, kern, mass, zb, mean, prec, fact_t, tile, start, stop, own_out, before=None):
    n_rows, width = theta.shape
    rank = fact_t.shape[0]
    first, steps = start // tile, (stop - start) // tile
    col = lambda r: pl.BlockSpec((r, tile), lambda i: (0, first + i))
    nxt = lambda r: pl.BlockSpec((r, tile), lambda i: (0, first + jnp.minimum(i + 1, steps - 1)))
    in_specs = [col(n_rows), nxt(n_rows), ANY, VMEM, VMEM, VMEM, VMEM, VMEM]
    args = [theta, theta, kern, mass, zb, mean, prec, fact_t]
    alias = {}
    if before is not None:
        in_specs += [VMEM, ANY]
        args += [before[1], before[0]]
        alias = {9: 1}
        if len(before) > 2:
            in_specs.append(ANY)
            args.append(before[2])
            alias[10] = 0
    return pl.pallas_call(
        functools.partial(update_kernel, consts, first),
        grid=(steps,),
        out_shape=(jax.ShapeDtypeStruct((n_rows, stop - start if own_out else width), F32),
                   jax.ShapeDtypeStruct((n_rows, width), BF16),
                   jax.ShapeDtypeStruct((rank, n_rows), F32)),
        in_specs=in_specs,
        out_specs=(pl.BlockSpec((n_rows, tile), lambda i: (0, i)) if own_out else col(n_rows), col(n_rows), VMEM),
        scratch_shapes=[pltpu.VMEM((2, n_rows, 2 * tile), BF16), pltpu.VMEM(kern.shape, BF16), pltpu.SemaphoreType.DMA],
        input_output_aliases=alias,
        compiler_params=pltpu.CompilerParams(vmem_limit_bytes=VMEM_LIMIT),
        cost_estimate=pl.CostEstimate(flops=4 * n_rows * n_rows * (stop - start), bytes_accessed=10 * n_rows * (stop - start), transcendentals=0),
    )(*args)


def last_kernel(consts, start, pos_ref, theta_ref, kern_hbm, mass_ref, zb_ref, mean_ref, prec_ref, fact_ref, *rest):
    out_ref, send_ref, rhs, kern_ref, kern_sem = rest[-5:]
    kern_copy = pltpu.make_async_copy(kern_hbm, kern_ref, kern_sem)
    kern_copy.start()
    rows = out_ref.shape[0]
    n_blk = theta_ref.shape[0] // BLK
    part = pos_ref[0]
    now = columns(part, start, theta_ref.shape[1], (mean_ref, prec_ref, fact_ref))

    @pl.loop(0, n_blk)
    def _(b):
        build_rhs(theta_ref, *now, zb_ref, rhs, pl.ds(pl.multiple_of(b * BLK, BLK), BLK))

    kern_copy.wait()
    for dst, which in ((send_ref, 1 - part), (out_ref, part)):
        @pl.loop(0, rows // BLK)
        def _(b):
            rs = pl.ds(pl.multiple_of(which * rows + b * BLK, BLK), BLK)
            acc = jnp.dot(kern_ref[rs, :], rhs[...], preferred_element_type=F32)
            dst[pl.ds(pl.multiple_of(b * BLK, BLK), BLK), :] = stepped(theta_ref, acc, mass_ref, rs, *consts)


def last_update(consts, pos, theta, kern, mass, zb, mean, prec, fact_t, out, start, tile):
    n_rows, width = theta.shape
    chunk = start // tile
    rows, feat = n_rows // 2, width * 2
    per = width // tile
    col = lambda r: pl.BlockSpec((r, tile), lambda i, pos: (0, chunk))
    in_specs = [col(n_rows), ANY, VMEM, VMEM, VMEM, VMEM, VMEM]
    args = [theta, kern, mass, zb, mean, prec, fact_t]
    alias = {}
    if out is not None:
        in_specs.append(ANY)
        args.append(out)
        alias = {8: 0}
    return pl.pallas_call(
        functools.partial(last_kernel, consts, start),
        grid_spec=pltpu.PrefetchScalarGridSpec(
            num_scalar_prefetch=1, grid=(1,), in_specs=in_specs,
            out_specs=(pl.BlockSpec((rows, tile), lambda i, pos: (0, pos[0] * per + chunk)),
                       pl.BlockSpec((rows, tile), lambda i, pos: (0, 0))),
            scratch_shapes=[pltpu.VMEM((n_rows, 2 * tile), BF16), pltpu.VMEM(kern.shape, BF16), pltpu.SemaphoreType.DMA]),
        out_shape=(jax.ShapeDtypeStruct((rows, feat), F32), jax.ShapeDtypeStruct((rows, tile), F32)),
        input_output_aliases=alias,
        compiler_params=pltpu.CompilerParams(vmem_limit_bytes=VMEM_LIMIT),
        cost_estimate=pl.CostEstimate(flops=4 * n_rows * n_rows * tile, bytes_accessed=10 * n_rows * tile, transcendentals=0),
    )(pos, *args)


def own_kernel(consts, foreign, pos_ref, theta_ref, kern_ref, mass_ref, zb_ref, mean_ref, prec_ref, fact_ref, base_ref, out_ref, rhs):
    rows = out_ref.shape[0]
    half = 1 - pos_ref[0] if foreign else pos_ref[0]
    now = columns(half, pl.program_id(0) * BLK, BLK, (mean_ref, prec_ref, fact_ref))

    @pl.loop(0, theta_ref.shape[0] // BLK)
    def _(b):
        build_rhs(theta_ref, *now, zb_ref, rhs, pl.ds(pl.multiple_of(b * BLK, BLK), BLK))

    @pl.loop(0, rows // BLK)
    def _(b):
        rs = pl.ds(pl.multiple_of(pos_ref[0] * rows + b * BLK, BLK), BLK)
        acc = jnp.dot(kern_ref[rs, :], rhs[...], preferred_element_type=F32)
        out_ref[pl.ds(pl.multiple_of(b * BLK, BLK), BLK), :] = stepped(theta_ref, acc, mass_ref, rs, *consts)


def own_update(consts, pos, theta, kern, mass, zb, mean, prec, fact_t, out, foreign):
    n_rows, cols = theta.shape
    rows, feat = out.shape
    per = feat // (2 * BLK)
    col = lambda r: pl.BlockSpec((r, BLK), lambda i, pos: (0, i))
    where = (lambda i, pos: (0, (1 - pos[0]) * per + i)) if foreign else (lambda i, pos: (0, pos[0] * per + i))
    return pl.pallas_call(
        functools.partial(own_kernel, consts, foreign),
        grid_spec=pltpu.PrefetchScalarGridSpec(
            num_scalar_prefetch=1, grid=(cols // BLK,),
            in_specs=[col(n_rows), VMEM, VMEM, VMEM, VMEM, VMEM, VMEM, ANY],
            out_specs=pl.BlockSpec((rows, BLK), where),
            scratch_shapes=[pltpu.VMEM((n_rows, 2 * BLK), BF16)]),
        out_shape=jax.ShapeDtypeStruct(out.shape, F32),
        input_output_aliases={8: 0},
        compiler_params=pltpu.CompilerParams(vmem_limit_bytes=VMEM_LIMIT),
        cost_estimate=pl.CostEstimate(flops=4 * rows * n_rows * cols, bytes_accessed=10 * n_rows * cols, transcendentals=0),
        name="own_foreign" if foreign else "own_shared",
    )(pos, theta, kern, mass, zb, mean, prec, fact_t, out)


def place_kernel(pos_ref, recv_ref, base_ref, out_ref):
    out_ref[...] = recv_ref[...]


def place(pos, recv, out, start):
    rows, tile = recv.shape
    per = out.shape[1] // 256
    sub = tile // 128
    first = start // 128
    return pl.pallas_call(
        place_kernel,
        grid_spec=pltpu.PrefetchScalarGridSpec(
            num_scalar_prefetch=1, grid=(sub,), in_specs=[pl.BlockSpec((rows, 128), lambda i, pos: (0, i)), ANY],
            out_specs=pl.BlockSpec((rows, 128), lambda i, pos: (0, (1 - pos[0]) * per + first + i))),
        out_shape=jax.ShapeDtypeStruct(out.shape, out.dtype),
        input_output_aliases={2: 0},
        cost_estimate=pl.CostEstimate(flops=1000 * rows * tile, bytes_accessed=8 * rows * tile, transcendentals=0),
    )(pos, recv, out)


def place_rows(pos, recv, cur, start):
    rows, cols = recv.shape
    return pl.pallas_call(
        place_kernel,
        grid_spec=pltpu.PrefetchScalarGridSpec(
            num_scalar_prefetch=1, grid=(cols // BLK,), in_specs=[pl.BlockSpec((rows, BLK), lambda i, pos: (0, i)), ANY],
            out_specs=pl.BlockSpec((rows, BLK), lambda i, pos: (1 - pos[0], start // BLK + i))),
        out_shape=jax.ShapeDtypeStruct(cur.shape, cur.dtype),
        input_output_aliases={2: 0},
        name="place_rows",
    )(pos, recv, cur)


def kmat_kernel(from_gram, two_over_h, src_ref, proj_ref, kern_ref, zb_ref, mass_ref, *scratch):
    if from_gram:
        tb, sib_out = None, None
    else:
        tb, sib_out, load_sem = scratch[-3:]
    (gbuf, sib_in, r_x1, r_y1, r_x2, r_y2, sq_parts, sq, z_in, z_all, kbuf,
     sib_send, sib_recv, rs_send, rs_recv, sq_send, sq_recv, z_send, z_recv, zb_send, zb_recv,
     k_send, k_recv, loc_sem) = scratch[:24]
    n_rows = kern_ref.shape[0]
    n_blk = n_rows // BLK
    ens, part, feat = lax.axis_index("ens"), lax.axis_index("part"), lax.axis_index("feat")
    x, core = feat // 2, lax.rem(feat, 2)

    def chip(rel):
        return lax.rem(part + rel // 2, 2), lax.rem(x + rel % 2, 2)

    def block(rel, flip):
        cy, cx = chip(rel)
        return cy * 4 + cx * 2 + lax.rem(core + flip, 2)

    def device(rel, flip):
        cy, cx = chip(rel)
        return (ens, cy, cx * 2 + lax.rem(core + flip, 2))

    me = block(0, 0)
    sibling, dev_x, dev_y = device(0, 1), device(1, 0), device(2, 0)
    others = [(rel, flip) for rel in (3, 1, 2, 0) for flip in (0, 1) if (rel, flip) != (0, 0)]

    def rcopy(src, dst, ssem, rsem, dev):
        return pltpu.make_async_remote_copy(src_ref=src, dst_ref=dst, send_sem=ssem, recv_sem=rsem,
                                            device_id=dev, device_id_type=MESH)

    barrier = pltpu.get_barrier_semaphore()
    for rel, flip in others:
        pl.semaphore_signal(barrier, inc=1, device_id=device(rel, flip), device_id_type=MESH)

    def load(b):
        rs = pl.ds(b * BLK, BLK)
        return pltpu.make_async_copy(src_ref.at[rs, :], tb.at[rs, :], load_sem.at[b])

    def own_gram(rel):
        return pltpu.make_async_copy(src_ref.at[block(rel, 0)], gbuf.at[rel], loc_sem.at[rel])

    if from_gram:
        for rel in (3, 2, 1, 0):
            own_gram(rel).start()
    else:
        for b in range(n_blk):
            load(b).start()
    pl.semaphore_wait(barrier, len(others))

    def z_cols(b):
        return proj_ref.at[:, pl.ds(pl.multiple_of(b * BLK, BLK), BLK)]

    def z_copy(i):
        rel, flip = others[i]
        return rcopy(z_cols(block(rel, flip)), z_in.at[me], z_send.at[i], z_recv.at[me], device(rel, flip))

    for i in range(len(others)):
        z_copy(i).start()
    z_own = pltpu.make_async_copy(z_cols(me), z_in.at[me], z_recv.at[me])
    z_own.start()

    def sib_copy(rel):
        src = src_ref.at[block(rel, 1)] if from_gram else sib_out.at[rel]
        return rcopy(src, sib_in.at[rel], sib_send.at[rel], sib_recv.at[rel], sibling)

    lo, hi = 0, 1
    rs_copies = {
        "d_lo": rcopy(gbuf.at[3, lo], r_x1.at[0], rs_send.at[0], rs_recv.at[0], dev_x),
        "d_hi": rcopy(gbuf.at[3, hi], r_y1.at[0], rs_send.at[1], rs_recv.at[1], dev_y),
        "y_hi": rcopy(gbuf.at[2, hi], r_y1.at[1], rs_send.at[2], rs_recv.at[2], dev_y),
        "x_lo": rcopy(gbuf.at[1, lo], r_x1.at[1], rs_send.at[3], rs_recv.at[3], dev_x),
        "y_lo": rcopy(gbuf.at[2, lo], r_y2, rs_send.at[4], rs_recv.at[4], dev_y),
        "x_hi": rcopy(gbuf.at[1, hi], r_x2, rs_send.at[5], rs_recv.at[5], dev_x),
    }
    eye = (lax.broadcasted_iota(jnp.int32, (HALF, HALF), 0) == lax.broadcasted_iota(jnp.int32, (HALF, HALF), 1)).astype(F32)

    def merge(rel):
        sib_copy(rel).wait_recv()
        gbuf[rel] += sib_in[rel]

    def first_sends(rel):
        for name in {3: ("d_lo", "d_hi"), 2: ("y_hi",), 1: ("x_lo",), 0: ()}[rel]:
            rs_copies[name].start()

    if from_gram:
        for rel in (3, 2, 1, 0):
            sib_copy(rel).start()
        for rel in (3, 2, 1, 0):
            own_gram(rel).wait()
            merge(rel)
            first_sends(rel)
    else:
        def bands_of(b, dst):
            rows = tb[pl.ds(pl.multiple_of(b * BLK, BLK), BLK), :]
            for k in range(REACH):
                j = lax.rem(b + k, n_blk)
                val = lax.dot_general(
                    rows, tb[pl.ds(pl.multiple_of(j * BLK, BLK), BLK), :], NT, preferred_element_type=F32)
                for h, col, piece in band_parts(k, val):
                    dst[h, :, col:col + piece.shape[1]] = piece

        for b in range(n_blk):
            load(b).wait()

        @pl.loop(0, 4)
        def _(i):
            rel = 3 - i
            cy, cx = lax.rem(part + rel // 2, 2), lax.rem(x + lax.rem(rel, 2), 2)
            base = cy * 4 + cx * 2
            bands_of(base + 1 - core, sib_out.at[rel])
            rcopy(sib_out.at[rel], sib_in.at[rel], sib_send.at[rel], sib_recv.at[rel], sibling).start()
            bands_of(base + core, gbuf.at[rel])
            rcopy(sib_out.at[rel], sib_in.at[rel], sib_send.at[rel], sib_recv.at[rel], sibling).wait_recv()
            gbuf[rel] += sib_in[rel]
            for r in (3, 2, 1):
                @pl.when(rel == r)
                def _():
                    first_sends(r)

    for rel in range(4):
        cy, cx = chip(rel)
        for h in range(2):
            sq_parts[me, cy * 2 + cx, :, h * HALF:(h + 1) * HALF] = jnp.sum(gbuf[rel, h, :, :HALF] * eye, axis=0, keepdims=True)

    def sq_copy(i):
        rel, flip = others[i]
        return rcopy(sq_parts.at[me], sq_parts.at[me], sq_send.at[i], sq_recv.at[me], device(rel, flip))

    def recv_from(buf, sem, rel, flip):
        b = block(rel, flip)
        return rcopy(buf.at[b], buf.at[b], sq_send.at[0], sem.at[b], sibling)

    for i in range(len(others)):
        sq_copy(i).start()

    rs_copies["d_lo"].wait_recv()
    gbuf[2, 0] += r_x1[0]
    rs_copies["y_lo"].start()
    rs_copies["d_hi"].wait_recv()
    gbuf[1, 1] += r_y1[0]
    rs_copies["x_hi"].start()

    z_own.wait()
    for rel, flip in others:
        recv_from(z_in, z_recv, rel, flip).wait_recv()
    z_sum = z_in[0]
    for b in range(1, n_blk):
        z_sum = z_sum + z_in[b]
    z_all[me] = z_sum.astype(BF16)

    def zb_copy(i):
        rel, flip = others[i]
        return rcopy(z_all.at[me], z_all.at[me], zb_send.at[i], zb_recv.at[me], device(rel, flip))

    for i in range(len(others)):
        zb_copy(i).start()
    for rel, flip in others:
        recv_from(sq_parts, sq_recv, rel, flip).wait_recv()
    for c in range(2):
        for q in range(4):
            s = sq_parts[c, q] + sq_parts[2 + c, q] + sq_parts[4 + c, q] + sq_parts[6 + c, q]
            b = 2 * q + c
            sq[:, b * BLK:(b + 1) * BLK] = s
            if b < REACH - 1:
                sq[:, n_rows + b * BLK:n_rows + (b + 1) * BLK] = s

    def kernel_of(h, gram):
        row = sq[:, pl.ds(pl.multiple_of((2 * me + h) * HALF, HALF), WIDE)]
        col = jnp.sum(eye * row[:, :HALF], axis=1, keepdims=True)
        return jnp.exp(-jnp.maximum(col + row - 2.0 * gram, 0.0) * (0.5 * two_over_h)).astype(BF16)

    slots = iter(range(14))
    sent = []

    def send_band(idx, dev):
        s = next(slots)
        cp = rcopy(kbuf.at[idx], kbuf.at[idx], k_send.at[s], k_recv.at[idx], dev)
        cp.start()
        sent.append(cp)

    def wait_band(idx):
        rcopy(kbuf.at[idx], kbuf.at[idx], k_send.at[0], k_recv.at[idx], sibling).wait_recv()

    def spread(b, h):
        idx = 2 * b + h
        row0 = pl.multiple_of(idx * HALF, HALF)
        for k in range(REACH * 2 - 1):
            col0 = pl.multiple_of(lax.rem(idx + k, 2 * n_blk) * HALF, HALF)
            tile = kbuf[idx, :, k * HALF:(k + 1) * HALF]
            kern_ref[pl.ds(row0, HALF), pl.ds(col0, HALF)] = tile
            if 0 < k < REACH * 2 - 2:
                kern_ref[pl.ds(col0, HALF), pl.ds(row0, HALF)] = tile.T

    rs_copies["x_lo"].wait_recv()
    rs_copies["y_lo"].wait_recv()
    kbuf[2 * me] = kernel_of(0, gbuf[0, 0] + (r_x1[1] + r_y2[...]))
    for dev in (dev_y, sibling):
        send_band(2 * me, dev)
    rs_copies["y_hi"].wait_recv()
    rs_copies["x_hi"].wait_recv()
    kbuf[2 * me + 1] = kernel_of(1, gbuf[0, 1] + (r_y1[1] + r_x2[...]))
    for dev in (dev_x, sibling):
        send_band(2 * me + 1, dev)
    send_band(2 * me, dev_x)
    send_band(2 * me + 1, dev_y)
    spread(me, 0)
    spread(me, 1)
    sib = block(0, 1)
    for h in range(2):
        wait_band(2 * sib + h)
        spread(sib, h)
    bx, by, bd = block(1, 0), block(2, 0), block(3, 0)
    wait_band(2 * by)
    send_band(2 * by, dev_x)
    send_band(2 * by, sibling)
    wait_band(2 * bx + 1)
    send_band(2 * bx + 1, dev_y)
    send_band(2 * bx + 1, sibling)
    spread(by, 0)
    spread(bx, 1)
    for b, h in ((bx, 0), (by, 1), (bd, 0), (bd, 1)):
        wait_band(2 * b + h)
        send_band(2 * b + h, sibling)
        spread(b, h)
    for rel, h in ((2, 0), (1, 1), (1, 0), (2, 1), (3, 0), (3, 1)):
        b = block(rel, 1)
        wait_band(2 * b + h)
        spread(b, h)
    for rel, flip in others:
        recv_from(z_all, zb_recv, rel, flip).wait_recv()
    for b in range(n_blk):
        rs = slice(b * BLK, (b + 1) * BLK)
        zb_ref[rs, :] = z_all[b].astype(F32).T.astype(BF16)
        mass_ref[rs, :] = jnp.sum(kern_ref[rs, :].astype(F32), axis=1, keepdims=True)
    for rel in range(4):
        sib_copy(rel).wait_send()
    for cp in rs_copies.values():
        cp.wait_send()
    for i in range(len(others)):
        z_copy(i).wait_send()
        sq_copy(i).wait_send()
        zb_copy(i).wait_send()
    for cp in sent:
        cp.wait_send()


def kernel_matrix(src, proj, two_over_h, collective_id, from_gram):
    rank, n_rows = proj.shape
    n_blk = n_rows // BLK
    dma = lambda *n: pltpu.SemaphoreType.DMA(n)
    scratch = [
        pltpu.VMEM((4, 2, HALF, WIDE), F32), pltpu.VMEM((4, 2, HALF, WIDE), F32),
        pltpu.VMEM((2, HALF, WIDE), F32), pltpu.VMEM((2, HALF, WIDE), F32),
        pltpu.VMEM((HALF, WIDE), F32), pltpu.VMEM((HALF, WIDE), F32),
        pltpu.VMEM((8, 4, 1, BLK), F32), pltpu.VMEM((1, n_rows + (REACH - 1) * BLK), F32),
        pltpu.VMEM((n_blk, rank, BLK), F32), pltpu.VMEM((n_blk, rank, BLK), BF16),
        pltpu.VMEM((2 * n_blk, HALF, WIDE), BF16),
        dma(4), dma(4), dma(6), dma(6), dma(7), dma(8), dma(7), dma(8), dma(7), dma(8), dma(14), dma(16), dma(4)]
    if not from_gram:
        scratch += [pltpu.VMEM(src.shape, BF16), pltpu.VMEM((4, 2, HALF, WIDE), F32), dma(n_blk)]
    return pl.pallas_call(
        functools.partial(kmat_kernel, from_gram, two_over_h),
        out_shape=(jax.ShapeDtypeStruct((n_rows, n_rows), BF16), jax.ShapeDtypeStruct((n_rows, rank), BF16),
                   jax.ShapeDtypeStruct((n_rows, 1), F32)),
        in_specs=[ANY, VMEM], out_specs=(VMEM, VMEM, VMEM), scratch_shapes=scratch,
        compiler_params=pltpu.CompilerParams(collective_id=collective_id, has_side_effects=True, vmem_limit_bytes=VMEM_LIMIT),
    )(src, proj)


def solution(mesh):
    part_size = mesh.shape["part"]
    feat_size = mesh.shape["feat"]

    def local_steps(theta, prec_loc, mean_loc, factor_loc):
        rows, feat_loc = theta.shape
        n_total = rows * part_size
        feat_total = feat_loc * feat_size
        width = feat_loc // part_size
        kern_width = 2.0 * feat_total / math.log(n_total)
        step_size = 0.15 * n_total * feat_total / math.log(n_total)
        consts = (1.0 / n_total, 2.0 / kern_width, step_size)
        part = lax.axis_index("part")
        pos = part.astype(jnp.int32).reshape(1)
        params = (mean_loc.reshape(1, feat_loc), prec_loc.reshape(1, feat_loc), factor_loc.T)
        shared = 2 * BLK
        chunks = [(shared, HALF)] + [(at, 2 * BLK) for at in range(2 * shared, width, 2 * BLK)] + [(shared + BLK, BLK), (shared + HALF, HALF)]
        swap = [(0, 1), (1, 0)]
        late = 3 * BLK
        early = width - late
        late_rows = lax.dynamic_slice_in_dim(theta, (1 - part) * width + early, late, axis=1)

        cur, gram, proj = exchange(theta, params[0], params[2], early // BLK, late // BLK)
        kern, zb, mass = kernel_matrix(gram, proj, consts[1], 1, True)
        late_rows, mass = lax.optimization_barrier((late_rows, mass))
        recv = lax.ppermute(late_rows, "part", swap)
        new, tb, proj = update(consts, cur, kern, mass, zb, *params, BLK, 0, early, False)
        cur = place_rows(pos, recv, cur, early)
        cur, tb, proj = update(consts, cur, kern, mass, zb, *params, BLK, early, width, False, (tb, proj, new))
        kern, zb, mass = kernel_matrix(tb, proj, consts[1], 2, False)
        both, tb, proj = update(consts, cur, kern, mass, zb, *params, BLK, 0, shared, True)
        foreign = lax.ppermute(both, "part", swap)
        cur, tb, proj = update(consts, cur, kern, mass, zb, *params, BLK, shared, width, False, (tb, proj))
        kern, zb, mass = kernel_matrix(tb, proj, consts[1], 3, False)
        out = None
        received = []
        for start, tile in chunks:
            out, send = last_update(consts, pos, cur, kern, mass, zb, *params, out, start, tile)
            received.append(lax.ppermute(send, "part", swap))
        out = own_update(consts, pos, both, kern, mass, zb, *params, out, False)
        out = own_update(consts, pos, foreign, kern, mass, zb, *params, out, True)
        for (start, tile), recv in zip(chunks, received):
            out = place(pos, recv, out, start)
        return out

    row_spec = P(("ens", "part"), "feat")
    vec_spec = P(("ens", "feat"))
    fac_spec = P(("ens", "feat"), None)
    return jax.shard_map(local_steps, mesh=mesh, in_specs=(row_spec, vec_spec, vec_spec, fac_spec), out_specs=row_spec, check_vma=False)
```

```python
import functools
import math
import jax
import jax.numpy as jnp
from jax import lax
from jax.experimental import pallas as pl
from jax.experimental.pallas import tpu as pltpu
from jax.sharding import PartitionSpec as P

BLK = 256
HALF = BLK // 2
REACH = 5
WIDE = 9 * HALF
MESH = pl.DeviceIdType.MESH
F32 = jnp.float32
BF16 = jnp.bfloat16
ANY = pl.BlockSpec(memory_space=pl.ANY)
VMEM = pl.BlockSpec(memory_space=pltpu.VMEM)
VMEM_LIMIT = 63 * 1024 * 1024
NT = (((1,), (1,)), ((), ()))


def band_parts(k, val):
    top, low = val[:HALF], val[HALF:]
    if k == 0:
        return (0, 0, top), (1, 0, low[:, HALF:])
    if k == REACH - 1:
        top = top[:, :HALF]
    return (0, k * BLK, top), (1, k * BLK - HALF, low)


def exchange_kernel(n_early, n_late, theta_ref, mean_ref, fact_ref, col_ref, late_own_ref, late_away_ref, gram_ref, proj_ref,
                    buf, tb, away, away_b, late_b, send_sem, recv_sem, lsend_sem, lrecv_sem, own_sem, put_sem, other_sem):
    part = lax.axis_index("part")
    other = 1 - part
    peer = (lax.axis_index("ens"), other, lax.axis_index("feat"))
    rows, width = theta_ref.shape[0], theta_ref.shape[1] // 2
    n_rows = col_ref.shape[0]
    cw = width // (n_early + n_late)
    n_blk = n_rows // BLK
    barrier = pltpu.get_barrier_semaphore()
    pl.semaphore_signal(barrier, inc=1, device_id=peer, device_id_type=MESH)
    pl.semaphore_wait(barrier, 1)
    own_rows = pl.ds(pl.multiple_of(part * rows, BLK), rows)
    other_rows = pl.ds(pl.multiple_of(other * rows, BLK), rows)

    def chunk(half, c):
        return pl.ds(pl.multiple_of(half * width + c * cw, 128), cw)

    def remote(c):
        return pltpu.make_async_remote_copy(
            src_ref=theta_ref.at[:, chunk(other, c)], dst_ref=col_ref.at[own_rows, chunk(0, c)],
            send_sem=send_sem.at[c], recv_sem=recv_sem.at[c], device_id=peer, device_id_type=MESH)

    def remote_late(c):
        return pltpu.make_async_remote_copy(
            src_ref=away_b.at[c], dst_ref=late_b.at[c],
            send_sem=lsend_sem.at[c], recv_sem=lrecv_sem.at[c], device_id=peer, device_id_type=MESH)

    def fetch_own(c):
        return pltpu.make_async_copy(theta_ref.at[:, chunk(part, c)], buf.at[own_rows, :], own_sem)

    def put_own(c):
        return pltpu.make_async_copy(buf.at[own_rows, :], col_ref.at[own_rows, chunk(0, c)], put_sem)

    def put_late(c):
        return pltpu.make_async_copy(buf.at[own_rows, :], late_own_ref.at[:, chunk(0, c - n_early)], put_sem)

    def fetch_other(c):
        return pltpu.make_async_copy(col_ref.at[other_rows, chunk(0, c)], buf.at[other_rows, :], other_sem)

    def project(src, row0, half, c, dst_row0):
        x = src[pl.ds(pl.multiple_of(row0, BLK), BLK), :] - mean_ref[:, chunk(half, c)]
        proj_ref[:, pl.ds(pl.multiple_of(dst_row0, BLK), BLK)] += lax.dot_general(
            fact_ref[:, chunk(half, c)], x.astype(BF16), NT, preferred_element_type=F32)

    def add_gram():
        for b in range(n_blk):
            rows_b = tb[b * BLK:(b + 1) * BLK, :]
            for k in range(REACH):
                j = (b + k) % n_blk
                val = lax.dot_general(rows_b, tb[j * BLK:(j + 1) * BLK, :], NT, preferred_element_type=F32)
                for h, col, piece in band_parts(k, val):
                    gram_ref[b, h, :, col:col + piece.shape[1]] += piece

    @pl.loop(0, n_early)
    def _(c):
        remote(c).start()

    gram_ref[...] = jnp.zeros_like(gram_ref)
    proj_ref[...] = jnp.zeros_like(proj_ref)

    @pl.loop(0, n_late)
    def _(c):
        fetch = pltpu.make_async_copy(theta_ref.at[:, chunk(other, n_early + c)], away, other_sem)
        fetch.start()
        fetch.wait()
        keep = pltpu.make_async_copy(away, late_away_ref.at[:, chunk(0, c)], own_sem)
        keep.start()

        @pl.loop(0, rows // BLK)
        def _(b):
            rs = pl.ds(pl.multiple_of(b * BLK, BLK), BLK)
            away_b[c, rs, :] = away[rs, :].astype(BF16)
            project(away, b * BLK, other, n_early + c, part * rows + b * BLK)

        keep.wait()

    @pl.loop(0, n_late)
    def _(c):
        remote_late(c).start()

    @pl.loop(0, n_early + n_late)
    def _(c):
        fetch_own(c).start()
        fetch_own(c).wait()

        @pl.when(c < n_early)
        def _():
            put_own(c).start()

        @pl.when(c >= n_early)
        def _():
            put_late(c).start()

        @pl.loop(0, rows // BLK)
        def _(b):
            row0 = part * rows + b * BLK
            rs = pl.ds(pl.multiple_of(row0, BLK), BLK)
            tb[rs, :] = buf[rs, :].astype(BF16)
            project(buf, row0, part, c, row0)

        @pl.when(c < n_early)
        def _():
            remote(c).wait_recv()
            fetch_other(c).start()
            fetch_other(c).wait()

            @pl.loop(0, rows // BLK)
            def _(b):
                row0 = other * rows + b * BLK
                rs = pl.ds(pl.multiple_of(row0, BLK), BLK)
                tb[rs, :] = buf[rs, :].astype(BF16)
                project(buf, row0, part, c, row0)

        @pl.when(c >= n_early)
        def _():
            remote_late(c - n_early).wait_recv()
            tb[other_rows, :] = late_b[c - n_early]

        add_gram()

        @pl.when(c < n_early)
        def _():
            put_own(c).wait()

        @pl.when(c >= n_early)
        def _():
            put_late(c).wait()

    @pl.loop(0, n_early)
    def _(c):
        remote(c).wait_send()

    @pl.loop(0, n_late)
    def _(c):
        remote_late(c).wait_send()


def exchange(theta, mean, fact_t, n_early, n_late):
    rows, feat = theta.shape
    width = feat // 2
    n_rows = rows * 2
    cw = width // (n_early + n_late)
    dma = lambda *n: pltpu.SemaphoreType.DMA(n)
    return pl.pallas_call(
        functools.partial(exchange_kernel, n_early, n_late),
        out_shape=(jax.ShapeDtypeStruct((n_rows, n_early * cw), F32),
                   jax.ShapeDtypeStruct((rows, n_late * cw), F32),
                   jax.ShapeDtypeStruct((rows, n_late * cw), F32),
                   jax.ShapeDtypeStruct((n_rows // BLK, 2, HALF, WIDE), F32),
                   jax.ShapeDtypeStruct((fact_t.shape[0], n_rows), F32)),
        in_specs=[ANY, VMEM, VMEM], out_specs=(ANY, ANY, ANY, VMEM, VMEM),
        scratch_shapes=[
            pltpu.VMEM((n_rows, cw), F32), pltpu.VMEM((n_rows, cw), BF16), pltpu.VMEM((rows, cw), F32),
            pltpu.VMEM((n_late, rows, cw), BF16), pltpu.VMEM((n_late, rows, cw), BF16),
            dma(n_early), dma(n_early), dma(n_late), dma(n_late),
            pltpu.SemaphoreType.DMA, pltpu.SemaphoreType.DMA, pltpu.SemaphoreType.DMA],
        compiler_params=pltpu.CompilerParams(collective_id=0, has_side_effects=True, vmem_limit_bytes=VMEM_LIMIT),
        name="exchange",
    )(theta, mean, fact_t)


def columns(half, start, tile, refs):
    cols = pl.ds(pl.multiple_of(half * (refs[0].shape[1] // 2) + start, 128), tile)
    return tuple(ref[:, cols] for ref in refs)


def build_rhs(th, mean, prec, fact, zb_ref, rhs, rs):
    tile = th.shape[1]
    low = jnp.dot(zb_ref[rs, :], fact, preferred_element_type=F32)
    rhs[rs, :tile] = (-((th - mean) * prec + low)).astype(BF16)
    rhs[rs, tile:] = th.astype(BF16)


def stepped(th, acc, mass_ref, rs, inv_n, two_over_h, step_size):
    tile = th.shape[1]
    pull = mass_ref[rs, :] * th.astype(BF16).astype(F32) - acc[:, tile:]
    return th + step_size * ((acc[:, :tile] + two_over_h * pull) * inv_n)


def update_kernel(consts, first, split, has_before, *refs):
    n_in = 2 * (2 if split else 1)
    kern_hbm, mass_ref, zb_ref = refs[n_in:n_in + 3]
    params = refs[n_in + 3:n_in + 6]
    out_ref, tb_ref, proj_ref, rhs, kern_ref, kern_sem = refs[-6:]
    tile = out_ref.shape[1]
    big = out_ref.shape[0] // 2
    i = pl.program_id(0)
    slot = lax.rem(i, 2)
    part = lax.axis_index("part")

    def span(at, size):
        return pl.ds(pl.multiple_of(at, BLK), size)

    @pl.when(i == 0)
    def _():
        kern_copy = pltpu.make_async_copy(kern_hbm, kern_ref, kern_sem)
        kern_copy.start()
        proj_ref[...] = refs[n_in + 6][...] if has_before else jnp.zeros_like(proj_ref)
        now = columns(part, first * tile, tile, params)
        if split:
            for ref, half in ((refs[0], part), (refs[2], 1 - part)):
                build_rhs(ref[...], *now, zb_ref, rhs.at[0], span(half * big, big))
        else:
            @pl.loop(0, 2)
            def _(b):
                rs = span(b * big, big)
                build_rhs(refs[0][rs, :], *now, zb_ref, rhs.at[0], rs)
        kern_copy.wait()

    mean, _, fact = columns(part, (first + i) * tile, tile, params)
    after = columns(part, (first + jnp.minimum(i + 1, pl.num_programs(0) - 1)) * tile, tile, params)

    def half_step(ref, next_ref, src, rs):
        acc = jnp.dot(kern_ref[rs, :], rhs[slot], preferred_element_type=F32)
        build_rhs(next_ref[src, :], *after, zb_ref, rhs.at[1 - slot], rs)
        new = stepped(ref[src, :], acc, mass_ref, rs, *consts)
        out_ref[rs, :] = new
        tb_ref[rs, :] = new.astype(BF16)
        proj_ref[:, rs] += lax.dot_general(fact, (new - mean).astype(BF16), NT, preferred_element_type=F32)

    if split:
        for at, half in ((0, part), (2, 1 - part)):
            half_step(refs[at], refs[at + 1], slice(None), span(half * big, big))
    else:
        @pl.loop(0, 2)
        def _(b):
            rs = span(b * big, big)
            half_step(refs[0], refs[1], rs, rs)


def update(consts, theta, kern, mass, zb, params, width, start, stop, own_out, before=None):
    split = isinstance(theta, tuple)
    n_rows = kern.shape[0]
    rank = params[2].shape[0]
    first, steps = start // BLK, (stop - start) // BLK
    base = 0 if split else first
    held = n_rows // 2 if split else n_rows
    in_specs, args = [], []
    for arr in theta if split else (theta,):
        in_specs += [pl.BlockSpec((held, BLK), lambda i: (0, base + i)),
                     pl.BlockSpec((held, BLK), lambda i: (0, base + jnp.minimum(i + 1, steps - 1)))]
        args += [arr, arr]
    in_specs += [ANY] + [VMEM] * 5
    args += [kern, mass, zb, *params]
    alias = {}
    if before is not None:
        in_specs += [VMEM, ANY]
        args += [before[1], before[0]]
        alias = {len(args) - 1: 1}
        if len(before) > 2:
            in_specs.append(ANY)
            args.append(before[2])
            alias[len(args) - 1] = 0
    col = pl.BlockSpec((n_rows, BLK), lambda i: (0, first + i))
    return pl.pallas_call(
        functools.partial(update_kernel, consts, first, split, before is not None),
        grid=(steps,),
        out_shape=(jax.ShapeDtypeStruct((n_rows, stop - start if own_out else width), F32),
                   jax.ShapeDtypeStruct((n_rows, width), BF16),
                   jax.ShapeDtypeStruct((rank, n_rows), F32)),
        in_specs=in_specs,
        out_specs=(pl.BlockSpec((n_rows, BLK), lambda i: (0, i)) if own_out else col, col, VMEM),
        scratch_shapes=[pltpu.VMEM((2, n_rows, 2 * BLK), BF16), pltpu.VMEM(kern.shape, BF16), pltpu.SemaphoreType.DMA],
        input_output_aliases=alias,
        compiler_params=pltpu.CompilerParams(vmem_limit_bytes=VMEM_LIMIT),
        cost_estimate=pl.CostEstimate(flops=4 * n_rows * n_rows * (stop - start), bytes_accessed=10 * n_rows * (stop - start), transcendentals=0),
    )(*args)


def last_kernel(consts, start, pos_ref, theta_ref, kern_hbm, mass_ref, zb_ref, mean_ref, prec_ref, fact_ref, *rest):
    out_ref, send_ref, rhs, kern_ref, kern_sem = rest[-5:]
    kern_copy = pltpu.make_async_copy(kern_hbm, kern_ref, kern_sem)
    kern_copy.start()
    rows = out_ref.shape[0]
    part = pos_ref[0]
    now = columns(part, start, theta_ref.shape[1], (mean_ref, prec_ref, fact_ref))

    @pl.loop(0, 2)
    def _(b):
        rs = pl.ds(pl.multiple_of(b * rows, BLK), rows)
        build_rhs(theta_ref[rs, :], *now, zb_ref, rhs, rs)

    kern_copy.wait()
    for dst, which in ((send_ref, 1 - part), (out_ref, part)):
        @pl.loop(0, rows // BLK)
        def _(b):
            rs = pl.ds(pl.multiple_of(which * rows + b * BLK, BLK), BLK)
            acc = jnp.dot(kern_ref[rs, :], rhs[...], preferred_element_type=F32)
            dst[pl.ds(pl.multiple_of(b * BLK, BLK), BLK), :] = stepped(theta_ref[rs, :], acc, mass_ref, rs, *consts)


def last_update(consts, pos, theta, kern, mass, zb, mean, prec, fact_t, out, start, tile):
    n_rows, width = theta.shape
    chunk = start // tile
    rows, feat = n_rows // 2, width * 2
    per = width // tile
    col = lambda r: pl.BlockSpec((r, tile), lambda i, pos: (0, chunk))
    in_specs = [col(n_rows), ANY, VMEM, VMEM, VMEM, VMEM, VMEM]
    args = [theta, kern, mass, zb, mean, prec, fact_t]
    alias = {}
    if out is not None:
        in_specs.append(ANY)
        args.append(out)
        alias = {8: 0}
    return pl.pallas_call(
        functools.partial(last_kernel, consts, start),
        grid_spec=pltpu.PrefetchScalarGridSpec(
            num_scalar_prefetch=1, grid=(1,), in_specs=in_specs,
            out_specs=(pl.BlockSpec((rows, tile), lambda i, pos: (0, pos[0] * per + chunk)),
                       pl.BlockSpec((rows, tile), lambda i, pos: (0, 0))),
            scratch_shapes=[pltpu.VMEM((n_rows, 2 * tile), BF16), pltpu.VMEM(kern.shape, BF16), pltpu.SemaphoreType.DMA]),
        out_shape=(jax.ShapeDtypeStruct((rows, feat), F32), jax.ShapeDtypeStruct((rows, tile), F32)),
        input_output_aliases=alias,
        compiler_params=pltpu.CompilerParams(vmem_limit_bytes=VMEM_LIMIT),
        cost_estimate=pl.CostEstimate(flops=4 * n_rows * n_rows * tile, bytes_accessed=10 * n_rows * tile, transcendentals=0),
    )(pos, *args)


def own_kernel(consts, foreign, pos_ref, theta_ref, kern_ref, mass_ref, zb_ref, mean_ref, prec_ref, fact_ref, base_ref, out_ref, rhs):
    rows = out_ref.shape[0]
    half = 1 - pos_ref[0] if foreign else pos_ref[0]
    now = columns(half, pl.program_id(0) * BLK, BLK, (mean_ref, prec_ref, fact_ref))

    @pl.loop(0, theta_ref.shape[0] // BLK)
    def _(b):
        rs = pl.ds(pl.multiple_of(b * BLK, BLK), BLK)
        build_rhs(theta_ref[rs, :], *now, zb_ref, rhs, rs)

    @pl.loop(0, rows // BLK)
    def _(b):
        rs = pl.ds(pl.multiple_of(pos_ref[0] * rows + b * BLK, BLK), BLK)
        acc = jnp.dot(kern_ref[rs, :], rhs[...], preferred_element_type=F32)
        out_ref[pl.ds(pl.multiple_of(b * BLK, BLK), BLK), :] = stepped(theta_ref[rs, :], acc, mass_ref, rs, *consts)


def own_update(consts, pos, theta, kern, mass, zb, mean, prec, fact_t, out, foreign):
    n_rows, cols = theta.shape
    rows, feat = out.shape
    per = feat // (2 * BLK)
    col = lambda r: pl.BlockSpec((r, BLK), lambda i, pos: (0, i))
    where = (lambda i, pos: (0, (1 - pos[0]) * per + i)) if foreign else (lambda i, pos: (0, pos[0] * per + i))
    return pl.pallas_call(
        functools.partial(own_kernel, consts, foreign),
        grid_spec=pltpu.PrefetchScalarGridSpec(
            num_scalar_prefetch=1, grid=(cols // BLK,),
            in_specs=[col(n_rows), VMEM, VMEM, VMEM, VMEM, VMEM, VMEM, ANY],
            out_specs=pl.BlockSpec((rows, BLK), where),
            scratch_shapes=[pltpu.VMEM((n_rows, 2 * BLK), BF16)]),
        out_shape=jax.ShapeDtypeStruct(out.shape, F32),
        input_output_aliases={8: 0},
        compiler_params=pltpu.CompilerParams(vmem_limit_bytes=VMEM_LIMIT),
        cost_estimate=pl.CostEstimate(flops=4 * rows * n_rows * cols, bytes_accessed=10 * n_rows * cols, transcendentals=0),
        name="own_foreign" if foreign else "own_shared",
    )(pos, theta, kern, mass, zb, mean, prec, fact_t, out)


def place_kernel(pos_ref, recv_ref, base_ref, out_ref):
    out_ref[...] = recv_ref[...]


def place(pos, recv, out, start):
    rows, tile = recv.shape
    per = out.shape[1] // 256
    sub = tile // 128
    first = start // 128
    return pl.pallas_call(
        place_kernel,
        grid_spec=pltpu.PrefetchScalarGridSpec(
            num_scalar_prefetch=1, grid=(sub,), in_specs=[pl.BlockSpec((rows, 128), lambda i, pos: (0, i)), ANY],
            out_specs=pl.BlockSpec((rows, 128), lambda i, pos: (0, (1 - pos[0]) * per + first + i))),
        out_shape=jax.ShapeDtypeStruct(out.shape, out.dtype),
        input_output_aliases={2: 0},
        cost_estimate=pl.CostEstimate(flops=1000 * rows * tile, bytes_accessed=8 * rows * tile, transcendentals=0),
    )(pos, recv, out)


def kmat_kernel(from_gram, two_over_h, src_ref, proj_ref, kern_ref, zb_ref, mass_ref, *scratch):
    if from_gram:
        tb, sib_out = None, None
    else:
        tb, sib_out, load_sem = scratch[-3:]
    (gbuf, sib_in, r_x1, r_y1, r_x2, r_y2, sq_parts, sq, z_in, z_all, kbuf,
     sib_send, sib_recv, rs_send, rs_recv, sq_send, sq_recv, z_send, z_recv, zb_send, zb_recv,
     k_send, k_recv, loc_sem) = scratch[:24]
    n_rows = kern_ref.shape[0]
    n_blk = n_rows // BLK
    ens, part, feat = lax.axis_index("ens"), lax.axis_index("part"), lax.axis_index("feat")
    x, core = feat // 2, lax.rem(feat, 2)

    def chip(rel):
        return lax.rem(part + rel // 2, 2), lax.rem(x + rel % 2, 2)

    def block(rel, flip):
        cy, cx = chip(rel)
        return cy * 4 + cx * 2 + lax.rem(core + flip, 2)

    def device(rel, flip):
        cy, cx = chip(rel)
        return (ens, cy, cx * 2 + lax.rem(core + flip, 2))

    me = block(0, 0)
    sibling, dev_x, dev_y = device(0, 1), device(1, 0), device(2, 0)
    others = [(rel, flip) for rel in (3, 1, 2, 0) for flip in (0, 1) if (rel, flip) != (0, 0)]

    def rcopy(src, dst, ssem, rsem, dev):
        return pltpu.make_async_remote_copy(src_ref=src, dst_ref=dst, send_sem=ssem, recv_sem=rsem,
                                            device_id=dev, device_id_type=MESH)

    barrier = pltpu.get_barrier_semaphore()
    for rel, flip in others:
        pl.semaphore_signal(barrier, inc=1, device_id=device(rel, flip), device_id_type=MESH)

    def load(b):
        rs = pl.ds(b * BLK, BLK)
        return pltpu.make_async_copy(src_ref.at[rs, :], tb.at[rs, :], load_sem.at[b])

    def own_gram(rel):
        return pltpu.make_async_copy(src_ref.at[block(rel, 0)], gbuf.at[rel], loc_sem.at[rel])

    if from_gram:
        for rel in (3, 2, 1, 0):
            own_gram(rel).start()
    else:
        for b in range(n_blk):
            load(b).start()
    pl.semaphore_wait(barrier, len(others))

    def z_cols(b):
        return proj_ref.at[:, pl.ds(pl.multiple_of(b * BLK, BLK), BLK)]

    def z_copy(i):
        rel, flip = others[i]
        return rcopy(z_cols(block(rel, flip)), z_in.at[me], z_send.at[i], z_recv.at[me], device(rel, flip))

    for i in range(len(others)):
        z_copy(i).start()
    z_own = pltpu.make_async_copy(z_cols(me), z_in.at[me], z_recv.at[me])
    z_own.start()

    def sib_copy(rel):
        src = src_ref.at[block(rel, 1)] if from_gram else sib_out.at[rel]
        return rcopy(src, sib_in.at[rel], sib_send.at[rel], sib_recv.at[rel], sibling)

    lo, hi = 0, 1
    rs_copies = {
        "d_lo": rcopy(gbuf.at[3, lo], r_x1.at[0], rs_send.at[0], rs_recv.at[0], dev_x),
        "d_hi": rcopy(gbuf.at[3, hi], r_y1.at[0], rs_send.at[1], rs_recv.at[1], dev_y),
        "y_hi": rcopy(gbuf.at[2, hi], r_y1.at[1], rs_send.at[2], rs_recv.at[2], dev_y),
        "x_lo": rcopy(gbuf.at[1, lo], r_x1.at[1], rs_send.at[3], rs_recv.at[3], dev_x),
        "y_lo": rcopy(gbuf.at[2, lo], r_y2, rs_send.at[4], rs_recv.at[4], dev_y),
        "x_hi": rcopy(gbuf.at[1, hi], r_x2, rs_send.at[5], rs_recv.at[5], dev_x),
    }
    eye = (lax.broadcasted_iota(jnp.int32, (HALF, HALF), 0) == lax.broadcasted_iota(jnp.int32, (HALF, HALF), 1)).astype(F32)

    def merge(rel):
        sib_copy(rel).wait_recv()
        gbuf[rel] += sib_in[rel]

    def first_sends(rel):
        for name in {3: ("d_lo", "d_hi"), 2: ("y_hi",), 1: ("x_lo",), 0: ()}[rel]:
            rs_copies[name].start()

    if from_gram:
        for rel in (3, 2, 1, 0):
            sib_copy(rel).start()
        for rel in (3, 2, 1, 0):
            own_gram(rel).wait()
            merge(rel)
            first_sends(rel)
    else:
        def bands_of(b, dst):
            rows = tb[pl.ds(pl.multiple_of(b * BLK, BLK), BLK), :]
            for k in range(REACH):
                j = lax.rem(b + k, n_blk)
                val = lax.dot_general(
                    rows, tb[pl.ds(pl.multiple_of(j * BLK, BLK), BLK), :], NT, preferred_element_type=F32)
                for h, col, piece in band_parts(k, val):
                    dst[h, :, col:col + piece.shape[1]] = piece

        for b in range(n_blk):
            load(b).wait()

        @pl.loop(0, 4)
        def _(i):
            rel = 3 - i
            cy, cx = lax.rem(part + rel // 2, 2), lax.rem(x + lax.rem(rel, 2), 2)
            base = cy * 4 + cx * 2
            bands_of(base + 1 - core, sib_out.at[rel])
            rcopy(sib_out.at[rel], sib_in.at[rel], sib_send.at[rel], sib_recv.at[rel], sibling).start()
            bands_of(base + core, gbuf.at[rel])
            rcopy(sib_out.at[rel], sib_in.at[rel], sib_send.at[rel], sib_recv.at[rel], sibling).wait_recv()
            gbuf[rel] += sib_in[rel]
            for r in (3, 2, 1):
                @pl.when(rel == r)
                def _():
                    first_sends(r)

    for rel in range(4):
        cy, cx = chip(rel)
        for h in range(2):
            sq_parts[me, cy * 2 + cx, :, h * HALF:(h + 1) * HALF] = jnp.sum(gbuf[rel, h, :, :HALF] * eye, axis=0, keepdims=True)

    def sq_copy(i):
        rel, flip = others[i]
        return rcopy(sq_parts.at[me], sq_parts.at[me], sq_send.at[i], sq_recv.at[me], device(rel, flip))

    def recv_from(buf, sem, rel, flip):
        b = block(rel, flip)
        return rcopy(buf.at[b], buf.at[b], sq_send.at[0], sem.at[b], sibling)

    for i in range(len(others)):
        sq_copy(i).start()

    rs_copies["d_lo"].wait_recv()
    gbuf[2, 0] += r_x1[0]
    rs_copies["y_lo"].start()
    rs_copies["d_hi"].wait_recv()
    gbuf[1, 1] += r_y1[0]
    rs_copies["x_hi"].start()

    z_own.wait()
    for rel, flip in others:
        recv_from(z_in, z_recv, rel, flip).wait_recv()
    z_sum = z_in[0]
    for b in range(1, n_blk):
        z_sum = z_sum + z_in[b]
    z_all[me] = z_sum.astype(BF16)

    def zb_copy(i):
        rel, flip = others[i]
        return rcopy(z_all.at[me], z_all.at[me], zb_send.at[i], zb_recv.at[me], device(rel, flip))

    for i in range(len(others)):
        zb_copy(i).start()
    for rel, flip in others:
        recv_from(sq_parts, sq_recv, rel, flip).wait_recv()
    for c in range(2):
        for q in range(4):
            s = sq_parts[c, q] + sq_parts[2 + c, q] + sq_parts[4 + c, q] + sq_parts[6 + c, q]
            b = 2 * q + c
            sq[:, b * BLK:(b + 1) * BLK] = s
            if b < REACH - 1:
                sq[:, n_rows + b * BLK:n_rows + (b + 1) * BLK] = s

    def kernel_of(h, gram):
        row = sq[:, pl.ds(pl.multiple_of((2 * me + h) * HALF, HALF), WIDE)]
        col = jnp.sum(eye * row[:, :HALF], axis=1, keepdims=True)
        return jnp.exp(-jnp.maximum(col + row - 2.0 * gram, 0.0) * (0.5 * two_over_h)).astype(BF16)

    slots = iter(range(14))
    sent = []

    def send_band(idx, dev):
        s = next(slots)
        cp = rcopy(kbuf.at[idx], kbuf.at[idx], k_send.at[s], k_recv.at[idx], dev)
        cp.start()
        sent.append(cp)

    def wait_band(idx):
        rcopy(kbuf.at[idx], kbuf.at[idx], k_send.at[0], k_recv.at[idx], sibling).wait_recv()

    def spread(b, h):
        idx = 2 * b + h
        row0 = pl.multiple_of(idx * HALF, HALF)
        for k in range(REACH * 2 - 1):
            col0 = pl.multiple_of(lax.rem(idx + k, 2 * n_blk) * HALF, HALF)
            tile = kbuf[idx, :, k * HALF:(k + 1) * HALF]
            kern_ref[pl.ds(row0, HALF), pl.ds(col0, HALF)] = tile
            if 0 < k < REACH * 2 - 2:
                kern_ref[pl.ds(col0, HALF), pl.ds(row0, HALF)] = tile.T

    rs_copies["x_lo"].wait_recv()
    rs_copies["y_lo"].wait_recv()
    kbuf[2 * me] = kernel_of(0, gbuf[0, 0] + (r_x1[1] + r_y2[...]))
    for dev in (dev_y, sibling):
        send_band(2 * me, dev)
    rs_copies["y_hi"].wait_recv()
    rs_copies["x_hi"].wait_recv()
    kbuf[2 * me + 1] = kernel_of(1, gbuf[0, 1] + (r_y1[1] + r_x2[...]))
    for dev in (dev_x, sibling):
        send_band(2 * me + 1, dev)
    send_band(2 * me, dev_x)
    send_band(2 * me + 1, dev_y)
    spread(me, 0)
    spread(me, 1)
    sib = block(0, 1)
    for h in range(2):
        wait_band(2 * sib + h)
        spread(sib, h)
    bx, by, bd = block(1, 0), block(2, 0), block(3, 0)
    wait_band(2 * by)
    send_band(2 * by, dev_x)
    send_band(2 * by, sibling)
    wait_band(2 * bx + 1)
    send_band(2 * bx + 1, dev_y)
    send_band(2 * bx + 1, sibling)
    spread(by, 0)
    spread(bx, 1)
    for b, h in ((bx, 0), (by, 1), (bd, 0), (bd, 1)):
        wait_band(2 * b + h)
        send_band(2 * b + h, sibling)
        spread(b, h)
    for rel, h in ((2, 0), (1, 1), (1, 0), (2, 1), (3, 0), (3, 1)):
        b = block(rel, 1)
        wait_band(2 * b + h)
        spread(b, h)
    for rel, flip in others:
        recv_from(z_all, zb_recv, rel, flip).wait_recv()
    for b in range(n_blk):
        rs = slice(b * BLK, (b + 1) * BLK)
        zb_ref[rs, :] = z_all[b].astype(F32).T.astype(BF16)
        mass_ref[rs, :] = jnp.sum(kern_ref[rs, :].astype(F32), axis=1, keepdims=True)
    for rel in range(4):
        sib_copy(rel).wait_send()
    for cp in rs_copies.values():
        cp.wait_send()
    for i in range(len(others)):
        z_copy(i).wait_send()
        sq_copy(i).wait_send()
        zb_copy(i).wait_send()
    for cp in sent:
        cp.wait_send()


def kernel_matrix(src, proj, two_over_h, collective_id, from_gram):
    rank, n_rows = proj.shape
    n_blk = n_rows // BLK
    dma = lambda *n: pltpu.SemaphoreType.DMA(n)
    scratch = [
        pltpu.VMEM((4, 2, HALF, WIDE), F32), pltpu.VMEM((4, 2, HALF, WIDE), F32),
        pltpu.VMEM((2, HALF, WIDE), F32), pltpu.VMEM((2, HALF, WIDE), F32),
        pltpu.VMEM((HALF, WIDE), F32), pltpu.VMEM((HALF, WIDE), F32),
        pltpu.VMEM((8, 4, 1, BLK), F32), pltpu.VMEM((1, n_rows + (REACH - 1) * BLK), F32),
        pltpu.VMEM((n_blk, rank, BLK), F32), pltpu.VMEM((n_blk, rank, BLK), BF16),
        pltpu.VMEM((2 * n_blk, HALF, WIDE), BF16),
        dma(4), dma(4), dma(6), dma(6), dma(7), dma(8), dma(7), dma(8), dma(7), dma(8), dma(14), dma(16), dma(4)]
    if not from_gram:
        scratch += [pltpu.VMEM(src.shape, BF16), pltpu.VMEM((4, 2, HALF, WIDE), F32), dma(n_blk)]
    return pl.pallas_call(
        functools.partial(kmat_kernel, from_gram, two_over_h),
        out_shape=(jax.ShapeDtypeStruct((n_rows, n_rows), BF16), jax.ShapeDtypeStruct((n_rows, rank), BF16),
                   jax.ShapeDtypeStruct((n_rows, 1), F32)),
        in_specs=[ANY, VMEM], out_specs=(VMEM, VMEM, VMEM), scratch_shapes=scratch,
        compiler_params=pltpu.CompilerParams(collective_id=collective_id, has_side_effects=True, vmem_limit_bytes=VMEM_LIMIT),
    )(src, proj)


def solution(mesh):
    part_size = mesh.shape["part"]
    feat_size = mesh.shape["feat"]

    def local_steps(theta, prec_loc, mean_loc, factor_loc):
        rows, feat_loc = theta.shape
        n_total = rows * part_size
        feat_total = feat_loc * feat_size
        width = feat_loc // part_size
        kern_width = 2.0 * feat_total / math.log(n_total)
        step_size = 0.15 * n_total * feat_total / math.log(n_total)
        consts = (1.0 / n_total, 2.0 / kern_width, step_size)
        part = lax.axis_index("part")
        pos = part.astype(jnp.int32).reshape(1)
        params = (mean_loc.reshape(1, feat_loc), prec_loc.reshape(1, feat_loc), factor_loc.T)
        shared = 2 * BLK
        chunks = [(shared, HALF)] + [(at, 2 * BLK) for at in range(2 * shared, width, 2 * BLK)] + [(shared + BLK, BLK), (shared + HALF, HALF)]
        swap = [(0, 1), (1, 0)]
        late = 3 * BLK
        early = width - late

        cur, late_own, late_away, gram, proj = exchange(theta, params[0], params[2], early // BLK, late // BLK)
        kern, zb, mass = kernel_matrix(gram, proj, consts[1], 1, True)
        late_away, mass = lax.optimization_barrier((late_away, mass))
        recv = lax.ppermute(late_away, "part", swap)
        new, tb, proj = update(consts, cur, kern, mass, zb, params, width, 0, early, False)
        cur, tb, proj = update(consts, (late_own, recv), kern, mass, zb, params, width, early, width, False, (tb, proj, new))
        kern, zb, mass = kernel_matrix(tb, proj, consts[1], 2, False)
        both, tb, proj = update(consts, cur, kern, mass, zb, params, width, 0, shared, True)
        foreign = lax.ppermute(both, "part", swap)
        cur, tb, proj = update(consts, cur, kern, mass, zb, params, width, shared, width, False, (tb, proj))
        kern, zb, mass = kernel_matrix(tb, proj, consts[1], 3, False)
        out = None
        received = []
        for start, tile in chunks:
            out, send = last_update(consts, pos, cur, kern, mass, zb, *params, out, start, tile)
            received.append(lax.ppermute(send, "part", swap))
        out = own_update(consts, pos, both, kern, mass, zb, *params, out, False)
        out = own_update(consts, pos, foreign, kern, mass, zb, *params, out, True)
        for (start, tile), recv in zip(chunks, received):
            out = place(pos, recv, out, start)
        return out

    row_spec = P(("ens", "part"), "feat")
    vec_spec = P(("ens", "feat"))
    fac_spec = P(("ens", "feat"), None)
    return jax.shard_map(local_steps, mesh=mesh, in_specs=(row_spec, vec_spec, vec_spec, fac_spec), out_specs=row_spec, check_vma=False)
```

```python
import functools
import math
import jax
import jax.numpy as jnp
from jax import lax
from jax.experimental import pallas as pl
from jax.experimental.pallas import tpu as pltpu
from jax.sharding import PartitionSpec as P

BLK = 256
HALF = BLK // 2
WIDE = 8 * HALF
TALL = HALF + 8
MESH = pl.DeviceIdType.MESH
F32 = jnp.float32
BF16 = jnp.bfloat16
ANY = pl.BlockSpec(memory_space=pl.ANY)
VMEM = pl.BlockSpec(memory_space=pltpu.VMEM)
VMEM_LIMIT = 63 * 1024 * 1024
NT = (((1,), (1,)), ((), ()))


def fold(tile):
    return jnp.concatenate([tile[8 * g:8 * g + 8] for g in range(8)], axis=1)


def unfold(rows):
    return jnp.concatenate([rows[:, HALF * g:HALF * (g + 1)] for g in range(8)], axis=0)


def band_pieces(rows_at, b, n_blk):
    def dot(left, right):
        return lax.dot_general(left, right, NT, preferred_element_type=F32)

    def wrap(j):
        return j % n_blk if isinstance(j, int) else lax.rem(j, n_blk)

    main = slice(0, HALF)
    both = rows_at(b * BLK, BLK)
    for k in range(4):
        val = dot(both, rows_at(wrap(b + k) * BLK, BLK))
        yield 0, main, slice(k * BLK, (k + 1) * BLK), val[:HALF]
        if k == 0:
            yield 1, main, slice(0, HALF), val[HALF:, HALF:]
        else:
            yield 1, main, slice(k * BLK - HALF, k * BLK + HALF), val[HALF:]
    yield 1, main, slice(WIDE - HALF, WIDE), dot(rows_at(b * BLK + HALF, HALF), rows_at(wrap(b + 4) * BLK, HALF))
    far = dot(rows_at(b * HALF, HALF), rows_at((b + n_blk) * HALF, HALF))
    for h in range(2):
        yield h, slice(HALF, TALL), slice(0, WIDE), fold(far[h * (HALF // 2):(h + 1) * (HALF // 2)])


def exchange_kernel(n_early, n_late, theta_ref, mean_ref, fact_ref, col_ref, late_own_ref, late_away_ref, gram_ref, proj_ref,
                    buf, tb, away, away_b, late_b, send_sem, recv_sem, lsend_sem, lrecv_sem, own_sem, put_sem, other_sem):
    part = lax.axis_index("part")
    other = 1 - part
    peer = (lax.axis_index("ens"), other, lax.axis_index("feat"))
    rows, width = theta_ref.shape[0], theta_ref.shape[1] // 2
    n_rows = col_ref.shape[0]
    cw = width // (n_early + n_late)
    n_blk = n_rows // BLK
    barrier = pltpu.get_barrier_semaphore()
    pl.semaphore_signal(barrier, inc=1, device_id=peer, device_id_type=MESH)
    pl.semaphore_wait(barrier, 1)
    own_rows = pl.ds(pl.multiple_of(part * rows, BLK), rows)
    other_rows = pl.ds(pl.multiple_of(other * rows, BLK), rows)

    def chunk(half, c):
        return pl.ds(pl.multiple_of(half * width + c * cw, 128), cw)

    def remote(c):
        return pltpu.make_async_remote_copy(
            src_ref=theta_ref.at[:, chunk(other, c)], dst_ref=col_ref.at[own_rows, chunk(0, c)],
            send_sem=send_sem.at[c], recv_sem=recv_sem.at[c], device_id=peer, device_id_type=MESH)

    def remote_late(c):
        return pltpu.make_async_remote_copy(
            src_ref=away_b.at[c], dst_ref=late_b.at[c],
            send_sem=lsend_sem.at[c], recv_sem=lrecv_sem.at[c], device_id=peer, device_id_type=MESH)

    def fetch_own(c):
        return pltpu.make_async_copy(theta_ref.at[:, chunk(part, c)], buf.at[own_rows, :], own_sem)

    def put_own(c):
        return pltpu.make_async_copy(buf.at[own_rows, :], col_ref.at[own_rows, chunk(0, c)], put_sem)

    def put_late(c):
        return pltpu.make_async_copy(buf.at[own_rows, :], late_own_ref.at[:, chunk(0, c - n_early)], put_sem)

    def fetch_other(c):
        return pltpu.make_async_copy(col_ref.at[other_rows, chunk(0, c)], buf.at[other_rows, :], other_sem)

    def project(src, row0, half, c, dst_row0):
        x = src[pl.ds(pl.multiple_of(row0, BLK), BLK), :] - mean_ref[:, chunk(half, c)]
        proj_ref[:, pl.ds(pl.multiple_of(dst_row0, BLK), BLK)] += lax.dot_general(
            fact_ref[:, chunk(half, c)], x.astype(BF16), NT, preferred_element_type=F32)

    def add_gram():
        for b in range(n_blk):
            for h, rows_, cols_, piece in band_pieces(lambda at, n: tb[at:at + n, :], b, n_blk):
                gram_ref[b, h, rows_, cols_] += piece

    @pl.loop(0, n_early)
    def _(c):
        remote(c).start()

    gram_ref[...] = jnp.zeros_like(gram_ref)
    proj_ref[...] = jnp.zeros_like(proj_ref)

    @pl.loop(0, n_late)
    def _(c):
        fetch = pltpu.make_async_copy(theta_ref.at[:, chunk(other, n_early + c)], away, other_sem)
        fetch.start()
        fetch.wait()
        keep = pltpu.make_async_copy(away, late_away_ref.at[:, chunk(0, c)], own_sem)
        keep.start()

        @pl.loop(0, rows // BLK)
        def _(b):
            rs = pl.ds(pl.multiple_of(b * BLK, BLK), BLK)
            away_b[c, rs, :] = away[rs, :].astype(BF16)
            project(away, b * BLK, other, n_early + c, part * rows + b * BLK)

        keep.wait()

    @pl.loop(0, n_late)
    def _(c):
        remote_late(c).start()

    @pl.loop(0, n_early + n_late)
    def _(c):
        fetch_own(c).start()
        fetch_own(c).wait()

        @pl.when(c < n_early)
        def _():
            put_own(c).start()

        @pl.when(c >= n_early)
        def _():
            put_late(c).start()

        @pl.loop(0, rows // BLK)
        def _(b):
            row0 = part * rows + b * BLK
            rs = pl.ds(pl.multiple_of(row0, BLK), BLK)
            tb[rs, :] = buf[rs, :].astype(BF16)
            project(buf, row0, part, c, row0)

        @pl.when(c < n_early)
        def _():
            remote(c).wait_recv()
            fetch_other(c).start()
            fetch_other(c).wait()

            @pl.loop(0, rows // BLK)
            def _(b):
                row0 = other * rows + b * BLK
                rs = pl.ds(pl.multiple_of(row0, BLK), BLK)
                tb[rs, :] = buf[rs, :].astype(BF16)
                project(buf, row0, part, c, row0)

        @pl.when(c >= n_early)
        def _():
            remote_late(c - n_early).wait_recv()
            tb[other_rows, :] = late_b[c - n_early]

        add_gram()

        @pl.when(c < n_early)
        def _():
            put_own(c).wait()

        @pl.when(c >= n_early)
        def _():
            put_late(c).wait()

    @pl.loop(0, n_early)
    def _(c):
        remote(c).wait_send()

    @pl.loop(0, n_late)
    def _(c):
        remote_late(c).wait_send()


def exchange(theta, mean, fact_t, n_early, n_late):
    rows, feat = theta.shape
    width = feat // 2
    n_rows = rows * 2
    cw = width // (n_early + n_late)
    dma = lambda *n: pltpu.SemaphoreType.DMA(n)
    return pl.pallas_call(
        functools.partial(exchange_kernel, n_early, n_late),
        out_shape=(jax.ShapeDtypeStruct((n_rows, n_early * cw), F32),
                   jax.ShapeDtypeStruct((rows, n_late * cw), F32),
                   jax.ShapeDtypeStruct((rows, n_late * cw), F32),
                   jax.ShapeDtypeStruct((n_rows // BLK, 2, TALL, WIDE), F32),
                   jax.ShapeDtypeStruct((fact_t.shape[0], n_rows), F32)),
        in_specs=[ANY, VMEM, VMEM], out_specs=(ANY, ANY, ANY, VMEM, VMEM),
        scratch_shapes=[
            pltpu.VMEM((n_rows, cw), F32), pltpu.VMEM((n_rows, cw), BF16), pltpu.VMEM((rows, cw), F32),
            pltpu.VMEM((n_late, rows, cw), BF16), pltpu.VMEM((n_late, rows, cw), BF16),
            dma(n_early), dma(n_early), dma(n_late), dma(n_late),
            pltpu.SemaphoreType.DMA, pltpu.SemaphoreType.DMA, pltpu.SemaphoreType.DMA],
        compiler_params=pltpu.CompilerParams(collective_id=0, has_side_effects=True, vmem_limit_bytes=VMEM_LIMIT),
        name="exchange",
    )(theta, mean, fact_t)


def columns(half, start, tile, refs):
    cols = pl.ds(pl.multiple_of(half * (refs[0].shape[1] // 2) + start, 128), tile)
    return tuple(ref[:, cols] for ref in refs)


def build_rhs(th, mean, prec, fact, zb_ref, rhs, rs):
    tile = th.shape[1]
    low = jnp.dot(zb_ref[rs, :], fact, preferred_element_type=F32)
    rhs[rs, :tile] = (-((th - mean) * prec + low)).astype(BF16)
    rhs[rs, tile:] = th.astype(BF16)


def stepped(th, acc, mass_ref, rs, inv_n, two_over_h, step_size):
    tile = th.shape[1]
    pull = mass_ref[rs, :] * th.astype(BF16).astype(F32) - acc[:, tile:]
    return th + step_size * ((acc[:, :tile] + two_over_h * pull) * inv_n)


def update_kernel(consts, first, split, has_before, *refs):
    n_in = 2 * (2 if split else 1)
    kern_hbm, mass_ref, zb_ref = refs[n_in:n_in + 3]
    params = refs[n_in + 3:n_in + 6]
    out_ref, tb_ref, proj_ref, rhs, kern_ref, kern_sem = refs[-6:]
    tile = out_ref.shape[1]
    big = out_ref.shape[0] // 2
    i = pl.program_id(0)
    slot = lax.rem(i, 2)
    part = lax.axis_index("part")

    def span(at, size):
        return pl.ds(pl.multiple_of(at, BLK), size)

    def order(h):
        return lax.rem(part + h, 2) if split else h

    def fetch(half):
        return pltpu.make_async_copy(kern_hbm.at[span(half * big, big), :], kern_ref.at[span(half * big, big), :], kern_sem.at[half])

    @pl.when(i == 0)
    def _():
        for h in range(2):
            fetch(order(h)).start()
        proj_ref[...] = refs[n_in + 6][...] if has_before else jnp.zeros_like(proj_ref)
        now = columns(part, first * tile, tile, params)
        if split:
            for ref, half in ((refs[0], part), (refs[2], 1 - part)):
                build_rhs(ref[...], *now, zb_ref, rhs.at[0], span(half * big, big))
        else:
            @pl.loop(0, 2)
            def _(b):
                rs = span(b * big, big)
                build_rhs(refs[0][rs, :], *now, zb_ref, rhs.at[0], rs)

    mean, _, fact = columns(part, (first + i) * tile, tile, params)
    after = columns(part, (first + jnp.minimum(i + 1, pl.num_programs(0) - 1)) * tile, tile, params)

    def half_step(ref, next_ref, src, half):
        rs = span(half * big, big)

        @pl.when(i == 0)
        def _():
            fetch(half).wait()

        acc = jnp.dot(kern_ref[rs, :], rhs[slot], preferred_element_type=F32)
        build_rhs(next_ref[src, :], *after, zb_ref, rhs.at[1 - slot], rs)
        new = stepped(ref[src, :], acc, mass_ref, rs, *consts)
        out_ref[rs, :] = new
        tb_ref[rs, :] = new.astype(BF16)
        proj_ref[:, rs] += lax.dot_general(fact, (new - mean).astype(BF16), NT, preferred_element_type=F32)

    if split:
        for at, half in ((0, part), (2, 1 - part)):
            half_step(refs[at], refs[at + 1], slice(None), half)
    else:
        @pl.loop(0, 2)
        def _(b):
            half_step(refs[0], refs[1], span(b * big, big), b)


def update(consts, theta, kern, mass, zb, params, width, start, stop, own_out, before=None):
    split = isinstance(theta, tuple)
    n_rows = kern.shape[0]
    rank = params[2].shape[0]
    first, steps = start // BLK, (stop - start) // BLK
    base = 0 if split else first
    held = n_rows // 2 if split else n_rows
    in_specs, args = [], []
    for arr in theta if split else (theta,):
        in_specs += [pl.BlockSpec((held, BLK), lambda i: (0, base + i)),
                     pl.BlockSpec((held, BLK), lambda i: (0, base + jnp.minimum(i + 1, steps - 1)))]
        args += [arr, arr]
    in_specs += [ANY] + [VMEM] * 5
    args += [kern, mass, zb, *params]
    alias = {}
    if before is not None:
        in_specs += [VMEM, ANY]
        args += [before[1], before[0]]
        alias = {len(args) - 1: 1}
        if len(before) > 2:
            in_specs.append(ANY)
            args.append(before[2])
            alias[len(args) - 1] = 0
    col = pl.BlockSpec((n_rows, BLK), lambda i: (0, first + i))
    return pl.pallas_call(
        functools.partial(update_kernel, consts, first, split, before is not None),
        grid=(steps,),
        out_shape=(jax.ShapeDtypeStruct((n_rows, stop - start if own_out else width), F32),
                   jax.ShapeDtypeStruct((n_rows, width), BF16),
                   jax.ShapeDtypeStruct((rank, n_rows), F32)),
        in_specs=in_specs,
        out_specs=(pl.BlockSpec((n_rows, BLK), lambda i: (0, i)) if own_out else col, col, VMEM),
        scratch_shapes=[pltpu.VMEM((2, n_rows, 2 * BLK), BF16), pltpu.VMEM(kern.shape, BF16), pltpu.SemaphoreType.DMA((2,))],
        input_output_aliases=alias,
        compiler_params=pltpu.CompilerParams(vmem_limit_bytes=VMEM_LIMIT),
        cost_estimate=pl.CostEstimate(flops=4 * n_rows * n_rows * (stop - start), bytes_accessed=10 * n_rows * (stop - start), transcendentals=0),
    )(*args)


def last_kernel(consts, start, pos_ref, theta_ref, kern_hbm, mass_ref, zb_ref, mean_ref, prec_ref, fact_ref, *rest):
    out_ref, send_ref, rhs, kern_ref, kern_sem = rest[-5:]
    kern_copy = pltpu.make_async_copy(kern_hbm, kern_ref, kern_sem)
    kern_copy.start()
    rows = out_ref.shape[0]
    part = pos_ref[0]
    now = columns(part, start, theta_ref.shape[1], (mean_ref, prec_ref, fact_ref))

    @pl.loop(0, 2)
    def _(b):
        rs = pl.ds(pl.multiple_of(b * rows, BLK), rows)
        build_rhs(theta_ref[rs, :], *now, zb_ref, rhs, rs)

    kern_copy.wait()
    size = BLK if theta_ref.shape[1] < BLK else HALF
    each = rows // size

    @pl.loop(0, 2 * each)
    def _(b):
        mine = b // each
        at = pl.multiple_of(lax.rem(b, each) * size, size)
        rs = pl.ds(pl.multiple_of(lax.rem(1 - part + mine, 2) * rows + at, size), size)
        acc = jnp.dot(kern_ref[rs, :], rhs[...], preferred_element_type=F32)
        new = stepped(theta_ref[rs, :], acc, mass_ref, rs, *consts)

        @pl.when(mine == 0)
        def _():
            send_ref[pl.ds(at, size), :] = new

        @pl.when(mine == 1)
        def _():
            out_ref[pl.ds(at, size), :] = new


def last_update(consts, pos, theta, kern, mass, zb, mean, prec, fact_t, out, start, tile):
    n_rows, width = theta.shape
    chunk = start // tile
    rows, feat = n_rows // 2, width * 2
    per = width // tile
    col = lambda r: pl.BlockSpec((r, tile), lambda i, pos: (0, chunk))
    in_specs = [col(n_rows), ANY, VMEM, VMEM, VMEM, VMEM, VMEM]
    args = [theta, kern, mass, zb, mean, prec, fact_t]
    alias = {}
    if out is not None:
        in_specs.append(ANY)
        args.append(out)
        alias = {8: 0}
    return pl.pallas_call(
        functools.partial(last_kernel, consts, start),
        grid_spec=pltpu.PrefetchScalarGridSpec(
            num_scalar_prefetch=1, grid=(1,), in_specs=in_specs,
            out_specs=(pl.BlockSpec((rows, tile), lambda i, pos: (0, pos[0] * per + chunk)),
                       pl.BlockSpec((rows, tile), lambda i, pos: (0, 0))),
            scratch_shapes=[pltpu.VMEM((n_rows, 2 * tile), BF16), pltpu.VMEM(kern.shape, BF16), pltpu.SemaphoreType.DMA]),
        out_shape=(jax.ShapeDtypeStruct((rows, feat), F32), jax.ShapeDtypeStruct((rows, tile), F32)),
        input_output_aliases=alias,
        compiler_params=pltpu.CompilerParams(vmem_limit_bytes=VMEM_LIMIT),
        cost_estimate=pl.CostEstimate(flops=4 * n_rows * n_rows * tile, bytes_accessed=10 * n_rows * tile, transcendentals=0),
    )(pos, *args)


def own_kernel(consts, foreign, pos_ref, theta_ref, kern_ref, mass_ref, zb_ref, mean_ref, prec_ref, fact_ref, base_ref, out_ref, rhs):
    rows = out_ref.shape[0]
    half = 1 - pos_ref[0] if foreign else pos_ref[0]
    now = columns(half, pl.program_id(0) * BLK, BLK, (mean_ref, prec_ref, fact_ref))

    @pl.loop(0, theta_ref.shape[0] // BLK)
    def _(b):
        rs = pl.ds(pl.multiple_of(b * BLK, BLK), BLK)
        build_rhs(theta_ref[rs, :], *now, zb_ref, rhs, rs)

    @pl.loop(0, rows // BLK)
    def _(b):
        rs = pl.ds(pl.multiple_of(pos_ref[0] * rows + b * BLK, BLK), BLK)
        acc = jnp.dot(kern_ref[rs, :], rhs[...], preferred_element_type=F32)
        out_ref[pl.ds(pl.multiple_of(b * BLK, BLK), BLK), :] = stepped(theta_ref[rs, :], acc, mass_ref, rs, *consts)


def own_update(consts, pos, theta, kern, mass, zb, mean, prec, fact_t, out, foreign):
    n_rows, cols = theta.shape
    rows, feat = out.shape
    per = feat // (2 * BLK)
    col = lambda r: pl.BlockSpec((r, BLK), lambda i, pos: (0, i))
    where = (lambda i, pos: (0, (1 - pos[0]) * per + i)) if foreign else (lambda i, pos: (0, pos[0] * per + i))
    return pl.pallas_call(
        functools.partial(own_kernel, consts, foreign),
        grid_spec=pltpu.PrefetchScalarGridSpec(
            num_scalar_prefetch=1, grid=(cols // BLK,),
            in_specs=[col(n_rows), VMEM, VMEM, VMEM, VMEM, VMEM, VMEM, ANY],
            out_specs=pl.BlockSpec((rows, BLK), where),
            scratch_shapes=[pltpu.VMEM((n_rows, 2 * BLK), BF16)]),
        out_shape=jax.ShapeDtypeStruct(out.shape, F32),
        input_output_aliases={8: 0},
        compiler_params=pltpu.CompilerParams(vmem_limit_bytes=VMEM_LIMIT),
        cost_estimate=pl.CostEstimate(flops=4 * rows * n_rows * cols, bytes_accessed=10 * n_rows * cols, transcendentals=0),
        name="own_foreign" if foreign else "own_shared",
    )(pos, theta, kern, mass, zb, mean, prec, fact_t, out)


def place_kernel(pos_ref, recv_ref, base_ref, out_ref):
    out_ref[...] = recv_ref[...]


def place(pos, recv, out, start):
    rows, tile = recv.shape
    per = out.shape[1] // 256
    sub = tile // 128
    first = start // 128
    return pl.pallas_call(
        place_kernel,
        grid_spec=pltpu.PrefetchScalarGridSpec(
            num_scalar_prefetch=1, grid=(sub,), in_specs=[pl.BlockSpec((rows, 128), lambda i, pos: (0, i)), ANY],
            out_specs=pl.BlockSpec((rows, 128), lambda i, pos: (0, (1 - pos[0]) * per + first + i))),
        out_shape=jax.ShapeDtypeStruct(out.shape, out.dtype),
        input_output_aliases={2: 0},
        cost_estimate=pl.CostEstimate(flops=1000 * rows * tile, bytes_accessed=8 * rows * tile, transcendentals=0),
    )(pos, recv, out)


def kmat_kernel(from_gram, two_over_h, src_ref, proj_ref, kern_out, zb_ref, mass_ref, *scratch):
    if not from_gram:
        tb, load_sem = scratch[-2:]
    (gbuf, sib_in, r_x1, r_y1, r_x2, r_y2, sq_parts, sq, z_in, z_all, kbuf,
     sib_send, sib_recv, rs_send, rs_recv, sq_send, sq_recv, z_send, z_recv, zb_send, zb_recv,
     k_send, k_recv, loc_sem, kern_ref, kern_sem) = scratch[:26]
    n_rows = kern_ref.shape[0]
    n_blk = n_rows // BLK
    ens, part, feat = lax.axis_index("ens"), lax.axis_index("part"), lax.axis_index("feat")
    x, core = feat // 2, lax.rem(feat, 2)

    def chip(rel):
        return lax.rem(part + rel // 2, 2), lax.rem(x + rel % 2, 2)

    def block(rel, flip):
        cy, cx = chip(rel)
        return cy * 4 + cx * 2 + lax.rem(core + flip, 2)

    def device(rel, flip):
        cy, cx = chip(rel)
        return (ens, cy, cx * 2 + lax.rem(core + flip, 2))

    me = block(0, 0)
    sibling, dev_x, dev_y = device(0, 1), device(1, 0), device(2, 0)
    others = [(rel, flip) for rel in (3, 1, 2, 0) for flip in (0, 1) if (rel, flip) != (0, 0)]

    def rcopy(src, dst, ssem, rsem, dev):
        return pltpu.make_async_remote_copy(src_ref=src, dst_ref=dst, send_sem=ssem, recv_sem=rsem,
                                            device_id=dev, device_id_type=MESH)

    barrier = pltpu.get_barrier_semaphore()
    for rel, flip in others:
        pl.semaphore_signal(barrier, inc=1, device_id=device(rel, flip), device_id_type=MESH)

    def load(b):
        rs = pl.ds(b * BLK, BLK)
        return pltpu.make_async_copy(src_ref.at[rs, :], tb.at[rs, :], load_sem.at[b])

    def own_gram(rel):
        return pltpu.make_async_copy(src_ref.at[block(rel, 0)], gbuf.at[rel], loc_sem.at[rel])

    if from_gram:
        for rel in (3, 2, 1, 0):
            own_gram(rel).start()
    else:
        for b in range(n_blk):
            load(b).start()
    pl.semaphore_wait(barrier, len(others))

    def z_cols(b):
        return proj_ref.at[:, pl.ds(pl.multiple_of(b * BLK, BLK), BLK)]

    def z_copy(i):
        rel, flip = others[i]
        return rcopy(z_cols(block(rel, flip)), z_in.at[me], z_send.at[i], z_recv.at[me], device(rel, flip))

    for i in range(len(others)):
        z_copy(i).start()
    z_own = pltpu.make_async_copy(z_cols(me), z_in.at[me], z_recv.at[me])
    z_own.start()

    def sib_copy(rel):
        src = src_ref.at[block(rel, 1)] if from_gram else gbuf.at[4 + rel]
        return rcopy(src, sib_in.at[rel], sib_send.at[rel], sib_recv.at[rel], sibling)

    lo, hi = 0, 1
    rs_copies = {
        "d_lo": rcopy(gbuf.at[3, lo], r_x1.at[0], rs_send.at[0], rs_recv.at[0], dev_x),
        "d_hi": rcopy(gbuf.at[3, hi], r_y1.at[0], rs_send.at[1], rs_recv.at[1], dev_y),
        "y_hi": rcopy(gbuf.at[2, hi], r_y1.at[1], rs_send.at[2], rs_recv.at[2], dev_y),
        "x_lo": rcopy(gbuf.at[1, lo], r_x1.at[1], rs_send.at[3], rs_recv.at[3], dev_x),
        "y_lo": rcopy(gbuf.at[2, lo], r_y2, rs_send.at[4], rs_recv.at[4], dev_y),
        "x_hi": rcopy(gbuf.at[1, hi], r_x2, rs_send.at[5], rs_recv.at[5], dev_x),
    }
    eye = (lax.broadcasted_iota(jnp.int32, (HALF, HALF), 0) == lax.broadcasted_iota(jnp.int32, (HALF, HALF), 1)).astype(F32)

    def merge(rel):
        sib_copy(rel).wait_recv()
        gbuf[rel] += sib_in[rel]

    def first_sends(rel):
        for name in {3: ("d_lo", "d_hi"), 2: ("y_hi",), 1: ("x_lo",), 0: ()}[rel]:
            rs_copies[name].start()

    if from_gram:
        for rel in (3, 2, 1, 0):
            sib_copy(rel).start()
        for rel in (3, 2, 1, 0):
            own_gram(rel).wait()
            merge(rel)
            first_sends(rel)
    else:
        def rows_at(at, n):
            return tb[pl.ds(pl.multiple_of(at, HALF), n), :]

        for b in range(n_blk):
            load(b).wait()

        @pl.loop(0, 8)
        def _(i):
            rel, own = 3 - i // 2, lax.rem(i, 2)
            cy, cx = lax.rem(part + rel // 2, 2), lax.rem(x + lax.rem(rel, 2), 2)
            b = cy * 4 + cx * 2 + lax.rem(core + 1 - own, 2)
            dst = rel + 4 * (1 - own)
            for h, rows_, cols_, piece in band_pieces(rows_at, b, n_blk):
                gbuf[dst, h, rows_, cols_] = piece
            across = rcopy(gbuf.at[4 + rel], sib_in.at[rel], sib_send.at[rel], sib_recv.at[rel], sibling)

            @pl.when(own == 0)
            def _():
                across.start()

            @pl.when(own == 1)
            def _():
                across.wait_recv()
                gbuf[rel] += sib_in[rel]
                for r in (3, 2, 1):
                    @pl.when(rel == r)
                    def _():
                        first_sends(r)

    for rel in range(4):
        cy, cx = chip(rel)
        for h in range(2):
            sq_parts[me, cy * 2 + cx, :, h * HALF:(h + 1) * HALF] = jnp.sum(gbuf[rel, h, :HALF, :HALF] * eye, axis=0, keepdims=True)

    def sq_copy(i):
        rel, flip = others[i]
        return rcopy(sq_parts.at[me], sq_parts.at[me], sq_send.at[i], sq_recv.at[me], device(rel, flip))

    def recv_from(buf, sem, rel, flip):
        b = block(rel, flip)
        return rcopy(buf.at[b], buf.at[b], sq_send.at[0], sem.at[b], sibling)

    for i in range(len(others)):
        sq_copy(i).start()

    rs_copies["d_lo"].wait_recv()
    gbuf[2, 0] += r_x1[0]
    rs_copies["y_lo"].start()
    rs_copies["d_hi"].wait_recv()
    gbuf[1, 1] += r_y1[0]
    rs_copies["x_hi"].start()

    z_own.wait()
    for rel, flip in others:
        recv_from(z_in, z_recv, rel, flip).wait_recv()
    z_sum = z_in[0]
    for b in range(1, n_blk):
        z_sum = z_sum + z_in[b]
    z_all[me] = z_sum.astype(BF16)

    def zb_copy(i):
        rel, flip = others[i]
        return rcopy(z_all.at[me], z_all.at[me], zb_send.at[i], zb_recv.at[me], device(rel, flip))

    for i in range(len(others)):
        zb_copy(i).start()
    for rel, flip in others:
        recv_from(sq_parts, sq_recv, rel, flip).wait_recv()
    for c in range(2):
        for q in range(4):
            s = sq_parts[c, q] + sq_parts[2 + c, q] + sq_parts[4 + c, q] + sq_parts[6 + c, q]
            b = 2 * q + c
            sq[:, b * BLK:(b + 1) * BLK] = s
            if b < WIDE // BLK:
                sq[:, n_rows + b * BLK:n_rows + (b + 1) * BLK] = s

    def sq_at(at, n):
        return sq[:, pl.ds(pl.multiple_of(at * HALF, HALF), n)]

    def upright(row):
        return jnp.sum(eye * row, axis=1, keepdims=True)

    def kernel_of(gram, col, row):
        return jnp.exp(-jnp.maximum(col + row - 2.0 * gram, 0.0) * (0.5 * two_over_h))

    def make_band(h, gram):
        idx = 2 * me + h
        row = sq_at(idx, WIDE)
        kbuf[idx, :HALF, :] = kernel_of(gram[:HALF], upright(row[:, :HALF]), row).astype(BF16)
        col = upright(sq_at(me, HALF))[h * (HALF // 2):(h + 1) * (HALF // 2)]
        kbuf[idx, HALF:, :] = fold(kernel_of(unfold(gram[HALF:]), col, sq_at(me + n_blk, HALF))).astype(BF16)

    slots = iter(range(14))
    sent = []

    def send_band(idx, dev):
        s = next(slots)
        cp = rcopy(kbuf.at[idx], kbuf.at[idx], k_send.at[s], k_recv.at[idx], dev)
        cp.start()
        sent.append(cp)

    def wait_band(idx):
        rcopy(kbuf.at[idx], kbuf.at[idx], k_send.at[0], k_recv.at[idx], sibling).wait_recv()

    def spread(b, h):
        idx = 2 * b + h
        row0 = pl.multiple_of(idx * HALF, HALF)
        for k in range(WIDE // HALF):
            col0 = pl.multiple_of(lax.rem(idx + k, 2 * n_blk) * HALF, HALF)
            tile = kbuf[idx, :HALF, k * HALF:(k + 1) * HALF]
            kern_ref[pl.ds(row0, HALF), pl.ds(col0, HALF)] = tile
            if k > 0:
                kern_ref[pl.ds(col0, HALF), pl.ds(row0, HALF)] = tile.T

    rs_copies["x_lo"].wait_recv()
    rs_copies["y_lo"].wait_recv()
    make_band(0, gbuf[0, 0] + (r_x1[1] + r_y2[...]))
    for dev in (dev_y, sibling):
        send_band(2 * me, dev)
    rs_copies["y_hi"].wait_recv()
    rs_copies["x_hi"].wait_recv()
    make_band(1, gbuf[0, 1] + (r_y1[1] + r_x2[...]))
    for dev in (dev_x, sibling):
        send_band(2 * me + 1, dev)
    send_band(2 * me, dev_x)
    send_band(2 * me + 1, dev_y)
    spread(me, 0)
    spread(me, 1)
    sib = block(0, 1)
    for h in range(2):
        wait_band(2 * sib + h)
        spread(sib, h)
    bx, by, bd = block(1, 0), block(2, 0), block(3, 0)
    wait_band(2 * by)
    send_band(2 * by, dev_x)
    send_band(2 * by, sibling)
    wait_band(2 * bx + 1)
    send_band(2 * bx + 1, dev_y)
    send_band(2 * bx + 1, sibling)
    spread(by, 0)
    spread(bx, 1)
    for b, h in ((bx, 0), (by, 1), (bd, 0), (bd, 1)):
        wait_band(2 * b + h)
        send_band(2 * b + h, sibling)
        spread(b, h)
    for rel, h in ((2, 0), (1, 1), (1, 0), (2, 1), (3, 0), (3, 1)):
        b = block(rel, 1)
        wait_band(2 * b + h)
        spread(b, h)
    for rel, flip in others:
        recv_from(z_all, zb_recv, rel, flip).wait_recv()
    for b in range(n_blk):
        tile = jnp.concatenate([unfold(kbuf[2 * b + h, HALF:, :].astype(F32)) for h in range(2)], axis=0)
        near, away = slice(b * HALF, (b + 1) * HALF), slice((b + n_blk) * HALF, (b + n_blk + 1) * HALF)
        kern_ref[near, away] = tile.astype(BF16)
        kern_ref[away, near] = tile.T.astype(BF16)

    def put(b):
        rs = pl.ds(b * BLK, BLK)
        return pltpu.make_async_copy(kern_ref.at[rs, :], kern_out.at[rs, :], kern_sem.at[b])

    for b in range(n_blk):
        rs = slice(b * BLK, (b + 1) * BLK)
        zb_ref[rs, :] = z_all[b].astype(F32).T.astype(BF16)
        mass_ref[rs, :] = jnp.sum(kern_ref[rs, :].astype(F32), axis=1, keepdims=True)
        put(b).start()
    for b in range(n_blk):
        put(b).wait()
    for rel in range(4):
        sib_copy(rel).wait_send()
    for cp in rs_copies.values():
        cp.wait_send()
    for i in range(len(others)):
        z_copy(i).wait_send()
        sq_copy(i).wait_send()
        zb_copy(i).wait_send()
    for cp in sent:
        cp.wait_send()


def kernel_matrix(src, proj, two_over_h, collective_id, from_gram):
    rank, n_rows = proj.shape
    n_blk = n_rows // BLK
    dma = lambda *n: pltpu.SemaphoreType.DMA(n)
    scratch = [
        pltpu.VMEM((4 if from_gram else 8, 2, TALL, WIDE), F32), pltpu.VMEM((4, 2, TALL, WIDE), F32),
        pltpu.VMEM((2, TALL, WIDE), F32), pltpu.VMEM((2, TALL, WIDE), F32),
        pltpu.VMEM((TALL, WIDE), F32), pltpu.VMEM((TALL, WIDE), F32),
        pltpu.VMEM((8, 4, 1, BLK), F32), pltpu.VMEM((1, n_rows + WIDE), F32),
        pltpu.VMEM((n_blk, rank, BLK), F32), pltpu.VMEM((n_blk, rank, BLK), BF16),
        pltpu.VMEM((2 * n_blk, TALL, WIDE), BF16),
        dma(4), dma(4), dma(6), dma(6), dma(7), dma(8), dma(7), dma(8), dma(7), dma(8), dma(14), dma(16), dma(4),
        pltpu.VMEM((n_rows, n_rows), BF16), dma(n_blk)]
    if not from_gram:
        scratch += [pltpu.VMEM(src.shape, BF16), dma(n_blk)]
    return pl.pallas_call(
        functools.partial(kmat_kernel, from_gram, two_over_h),
        out_shape=(jax.ShapeDtypeStruct((n_rows, n_rows), BF16), jax.ShapeDtypeStruct((n_rows, rank), BF16),
                   jax.ShapeDtypeStruct((n_rows, 1), F32)),
        in_specs=[ANY, VMEM], out_specs=(ANY, VMEM, VMEM), scratch_shapes=scratch,
        compiler_params=pltpu.CompilerParams(collective_id=collective_id, has_side_effects=True, vmem_limit_bytes=VMEM_LIMIT),
    )(src, proj)


def solution(mesh):
    part_size = mesh.shape["part"]
    feat_size = mesh.shape["feat"]

    def local_steps(theta, prec_loc, mean_loc, factor_loc):
        rows, feat_loc = theta.shape
        n_total = rows * part_size
        feat_total = feat_loc * feat_size
        width = feat_loc // part_size
        kern_width = 2.0 * feat_total / math.log(n_total)
        step_size = 0.15 * n_total * feat_total / math.log(n_total)
        consts = (1.0 / n_total, 2.0 / kern_width, step_size)
        part = lax.axis_index("part")
        pos = part.astype(jnp.int32).reshape(1)
        params = (mean_loc.reshape(1, feat_loc), prec_loc.reshape(1, feat_loc), factor_loc.T)
        shared = 2 * BLK
        chunks = [(shared, HALF)] + [(at, 2 * BLK) for at in range(2 * shared, width, 2 * BLK)] + [(shared + BLK, BLK), (shared + HALF, HALF)]
        swap = [(0, 1), (1, 0)]
        late = 3 * BLK
        early = width - late

        cur, late_own, late_away, gram, proj = exchange(theta, params[0], params[2], early // BLK, late // BLK)
        kern, zb, mass = kernel_matrix(gram, proj, consts[1], 1, True)
        late_away, mass = lax.optimization_barrier((late_away, mass))
        recv = lax.ppermute(late_away, "part", swap)
        new, tb, proj = update(consts, cur, kern, mass, zb, params, width, 0, early, False)
        cur, tb, proj = update(consts, (late_own, recv), kern, mass, zb, params, width, early, width, False, (tb, proj, new))
        kern, zb, mass = kernel_matrix(tb, proj, consts[1], 2, False)
        both, tb, proj = update(consts, cur, kern, mass, zb, params, width, 0, shared, True)
        foreign = lax.ppermute(both, "part", swap)
        cur, tb, proj = update(consts, cur, kern, mass, zb, params, width, shared, width, False, (tb, proj))
        kern, zb, mass = kernel_matrix(tb, proj, consts[1], 3, False)
        out = None
        received = []
        for start, tile in chunks:
            out, send = last_update(consts, pos, cur, kern, mass, zb, *params, out, start, tile)
            received.append(lax.ppermute(send, "part", swap))
        out = own_update(consts, pos, both, kern, mass, zb, *params, out, False)
        out = own_update(consts, pos, foreign, kern, mass, zb, *params, out, True)
        for (start, tile), recv in zip(chunks, received):
            out = place(pos, recv, out, start)
        return out

    row_spec = P(("ens", "part"), "feat")
    vec_spec = P(("ens", "feat"))
    fac_spec = P(("ens", "feat"), None)
    return jax.shard_map(local_steps, mesh=mesh, in_specs=(row_spec, vec_spec, vec_spec, fac_spec), out_specs=row_spec, check_vma=False)
```

```python
import functools
import math
import jax
import jax.numpy as jnp
from jax import lax
from jax.experimental import pallas as pl
from jax.experimental.pallas import tpu as pltpu
from jax.sharding import PartitionSpec as P

BLK = 256
HALF = BLK // 2
WIDE = 8 * HALF
TALL = HALF + 8
MESH = pl.DeviceIdType.MESH
F32 = jnp.float32
BF16 = jnp.bfloat16
ANY = pl.BlockSpec(memory_space=pl.ANY)
VMEM = pl.BlockSpec(memory_space=pltpu.VMEM)
VMEM_LIMIT = 63 * 1024 * 1024
NT = (((1,), (1,)), ((), ()))


def fold(tile):
    return jnp.concatenate([tile[8 * g:8 * g + 8] for g in range(8)], axis=1)


def unfold(rows):
    return jnp.concatenate([rows[:, HALF * g:HALF * (g + 1)] for g in range(8)], axis=0)


def band_pieces(rows_at, b, n_blk):
    def dot(left, right):
        return lax.dot_general(left, right, NT, preferred_element_type=F32)

    def wrap(j):
        return j % n_blk if isinstance(j, int) else lax.rem(j, n_blk)

    main = slice(0, HALF)
    both = rows_at(b * BLK, BLK)
    for k in range(4):
        val = dot(both, rows_at(wrap(b + k) * BLK, BLK))
        yield 0, main, slice(k * BLK, (k + 1) * BLK), val[:HALF]
        if k == 0:
            yield 1, main, slice(0, HALF), val[HALF:, HALF:]
        else:
            yield 1, main, slice(k * BLK - HALF, k * BLK + HALF), val[HALF:]
    yield 1, main, slice(WIDE - HALF, WIDE), dot(rows_at(b * BLK + HALF, HALF), rows_at(wrap(b + 4) * BLK, HALF))
    far = dot(rows_at(b * HALF, HALF), rows_at((b + n_blk) * HALF, HALF))
    for h in range(2):
        yield h, slice(HALF, TALL), slice(0, WIDE), fold(far[h * (HALF // 2):(h + 1) * (HALF // 2)])


def exchange_body(n_early, n_late, theta_ref, mean_ref, fact_ref, col_ref, late_own_ref, late_away_ref, gram_ref, proj_ref,
                  buf, tb, away, away_b, late_b, send_sem, recv_sem, lsend_sem, lrecv_sem, own_sem, put_sem, other_sem):
    part = lax.axis_index("part")
    other = 1 - part
    peer = (lax.axis_index("ens"), other, lax.axis_index("feat"))
    rows, width = theta_ref.shape[0], theta_ref.shape[1] // 2
    n_rows = col_ref.shape[0]
    cw = width // (n_early + n_late)
    n_blk = n_rows // BLK
    own_rows = pl.ds(pl.multiple_of(part * rows, BLK), rows)
    other_rows = pl.ds(pl.multiple_of(other * rows, BLK), rows)

    def chunk(half, c):
        return pl.ds(pl.multiple_of(half * width + c * cw, 128), cw)

    def remote(c):
        return pltpu.make_async_remote_copy(
            src_ref=theta_ref.at[:, chunk(other, c)], dst_ref=col_ref.at[own_rows, chunk(0, c)],
            send_sem=send_sem.at[c], recv_sem=recv_sem.at[c], device_id=peer, device_id_type=MESH)

    def remote_late(c):
        return pltpu.make_async_remote_copy(
            src_ref=away_b.at[c], dst_ref=late_b.at[c],
            send_sem=lsend_sem.at[c], recv_sem=lrecv_sem.at[c], device_id=peer, device_id_type=MESH)

    def fetch_own(c):
        return pltpu.make_async_copy(theta_ref.at[:, chunk(part, c)], buf.at[own_rows, :], own_sem)

    def put_own(c):
        return pltpu.make_async_copy(buf.at[own_rows, :], col_ref.at[own_rows, chunk(0, c)], put_sem)

    def put_late(c):
        return pltpu.make_async_copy(buf.at[own_rows, :], late_own_ref.at[:, chunk(0, c - n_early)], put_sem)

    def fetch_other(c):
        return pltpu.make_async_copy(col_ref.at[other_rows, chunk(0, c)], buf.at[other_rows, :], other_sem)

    def project(src, row0, half, c, dst_row0):
        x = src[pl.ds(pl.multiple_of(row0, BLK), BLK), :] - mean_ref[:, chunk(half, c)]
        proj_ref[:, pl.ds(pl.multiple_of(dst_row0, BLK), BLK)] += lax.dot_general(
            fact_ref[:, chunk(half, c)], x.astype(BF16), NT, preferred_element_type=F32)

    def add_gram():
        for b in range(n_blk):
            for h, rows_, cols_, piece in band_pieces(lambda at, n: tb[at:at + n, :], b, n_blk):
                gram_ref[b, h, rows_, cols_] += piece

    @pl.loop(0, n_early)
    def _(c):
        remote(c).start()

    gram_ref[...] = jnp.zeros_like(gram_ref)
    proj_ref[...] = jnp.zeros_like(proj_ref)

    @pl.loop(0, n_late)
    def _(c):
        fetch = pltpu.make_async_copy(theta_ref.at[:, chunk(other, n_early + c)], away, other_sem)
        fetch.start()
        fetch.wait()
        keep = pltpu.make_async_copy(away, late_away_ref.at[:, chunk(0, c)], own_sem)
        keep.start()

        @pl.loop(0, rows // BLK)
        def _(b):
            rs = pl.ds(pl.multiple_of(b * BLK, BLK), BLK)
            away_b[c, rs, :] = away[rs, :].astype(BF16)
            project(away, b * BLK, other, n_early + c, part * rows + b * BLK)

        keep.wait()

    @pl.loop(0, n_late)
    def _(c):
        remote_late(c).start()

    @pl.loop(0, n_early + n_late)
    def _(c):
        fetch_own(c).start()
        fetch_own(c).wait()

        @pl.when(c < n_early)
        def _():
            put_own(c).start()

        @pl.when(c >= n_early)
        def _():
            put_late(c).start()

        @pl.loop(0, rows // BLK)
        def _(b):
            row0 = part * rows + b * BLK
            rs = pl.ds(pl.multiple_of(row0, BLK), BLK)
            tb[rs, :] = buf[rs, :].astype(BF16)
            project(buf, row0, part, c, row0)

        @pl.when(c < n_early)
        def _():
            remote(c).wait_recv()
            fetch_other(c).start()
            fetch_other(c).wait()

            @pl.loop(0, rows // BLK)
            def _(b):
                row0 = other * rows + b * BLK
                rs = pl.ds(pl.multiple_of(row0, BLK), BLK)
                tb[rs, :] = buf[rs, :].astype(BF16)
                project(buf, row0, part, c, row0)

        @pl.when(c >= n_early)
        def _():
            remote_late(c - n_early).wait_recv()
            tb[other_rows, :] = late_b[c - n_early]

        add_gram()

        @pl.when(c < n_early)
        def _():
            put_own(c).wait()

        @pl.when(c >= n_early)
        def _():
            put_late(c).wait()

    @pl.loop(0, n_early)
    def _(c):
        remote(c).wait_send()

    @pl.loop(0, n_late)
    def _(c):
        remote_late(c).wait_send()


def columns(half, start, tile, refs):
    cols = pl.ds(pl.multiple_of(half * (refs[0].shape[1] // 2) + start, 128), tile)
    return tuple(ref[:, cols] for ref in refs)


def build_rhs(th, mean, prec, fact, zb_ref, rhs, rs):
    tile = th.shape[1]
    low = jnp.dot(zb_ref[rs, :], fact, preferred_element_type=F32)
    rhs[rs, :tile] = (-((th - mean) * prec + low)).astype(BF16)
    rhs[rs, tile:] = th.astype(BF16)


def stepped(th, acc, mass_ref, rs, inv_n, two_over_h, step_size):
    tile = th.shape[1]
    pull = mass_ref[rs, :] * th.astype(BF16).astype(F32) - acc[:, tile:]
    return th + step_size * ((acc[:, :tile] + two_over_h * pull) * inv_n)


def update_kernel(consts, first, split, has_before, *refs):
    n_in = 2 * (2 if split else 1)
    kern_hbm, mass_ref, zb_ref = refs[n_in:n_in + 3]
    params = refs[n_in + 3:n_in + 6]
    out_ref, tb_ref, proj_ref, rhs, kern_ref, kern_sem = refs[-6:]
    tile = out_ref.shape[1]
    big = out_ref.shape[0] // 2
    i = pl.program_id(0)
    slot = lax.rem(i, 2)
    part = lax.axis_index("part")

    def span(at, size):
        return pl.ds(pl.multiple_of(at, BLK), size)

    def order(h):
        return lax.rem(part + h, 2) if split else h

    def fetch(half):
        return pltpu.make_async_copy(kern_hbm.at[span(half * big, big), :], kern_ref.at[span(half * big, big), :], kern_sem.at[half])

    @pl.when(i == 0)
    def _():
        for h in range(2):
            fetch(order(h)).start()
        proj_ref[...] = refs[n_in + 6][...] if has_before else jnp.zeros_like(proj_ref)
        now = columns(part, first * tile, tile, params)
        if split:
            for ref, half in ((refs[0], part), (refs[2], 1 - part)):
                build_rhs(ref[...], *now, zb_ref, rhs.at[0], span(half * big, big))
        else:
            @pl.loop(0, 2)
            def _(b):
                rs = span(b * big, big)
                build_rhs(refs[0][rs, :], *now, zb_ref, rhs.at[0], rs)

    mean, _, fact = columns(part, (first + i) * tile, tile, params)
    after = columns(part, (first + jnp.minimum(i + 1, pl.num_programs(0) - 1)) * tile, tile, params)

    def half_step(ref, next_ref, src, half):
        rs = span(half * big, big)

        @pl.when(i == 0)
        def _():
            fetch(half).wait()

        acc = jnp.dot(kern_ref[rs, :], rhs[slot], preferred_element_type=F32)
        build_rhs(next_ref[src, :], *after, zb_ref, rhs.at[1 - slot], rs)
        new = stepped(ref[src, :], acc, mass_ref, rs, *consts)
        out_ref[rs, :] = new
        tb_ref[rs, :] = new.astype(BF16)
        proj_ref[:, rs] += lax.dot_general(fact, (new - mean).astype(BF16), NT, preferred_element_type=F32)

    if split:
        for at, half in ((0, part), (2, 1 - part)):
            half_step(refs[at], refs[at + 1], slice(None), half)
    else:
        @pl.loop(0, 2)
        def _(b):
            half_step(refs[0], refs[1], span(b * big, big), b)


def update(consts, theta, kern, mass, zb, params, width, start, stop, own_out, before=None):
    split = isinstance(theta, tuple)
    n_rows = kern.shape[0]
    rank = params[2].shape[0]
    first, steps = start // BLK, (stop - start) // BLK
    base = 0 if split else first
    held = n_rows // 2 if split else n_rows
    in_specs, args = [], []
    for arr in theta if split else (theta,):
        in_specs += [pl.BlockSpec((held, BLK), lambda i: (0, base + i)),
                     pl.BlockSpec((held, BLK), lambda i: (0, base + jnp.minimum(i + 1, steps - 1)))]
        args += [arr, arr]
    in_specs += [ANY] + [VMEM] * 5
    args += [kern, mass, zb, *params]
    alias = {}
    if before is not None:
        in_specs += [VMEM, ANY]
        args += [before[1], before[0]]
        alias = {len(args) - 1: 1}
        if len(before) > 2:
            in_specs.append(ANY)
            args.append(before[2])
            alias[len(args) - 1] = 0
    col = pl.BlockSpec((n_rows, BLK), lambda i: (0, first + i))
    return pl.pallas_call(
        functools.partial(update_kernel, consts, first, split, before is not None),
        grid=(steps,),
        out_shape=(jax.ShapeDtypeStruct((n_rows, stop - start if own_out else width), F32),
                   jax.ShapeDtypeStruct((n_rows, width), BF16),
                   jax.ShapeDtypeStruct((rank, n_rows), F32)),
        in_specs=in_specs,
        out_specs=(pl.BlockSpec((n_rows, BLK), lambda i: (0, i)) if own_out else col, col, VMEM),
        scratch_shapes=[pltpu.VMEM((2, n_rows, 2 * BLK), BF16), pltpu.VMEM(kern.shape, BF16), pltpu.SemaphoreType.DMA((2,))],
        input_output_aliases=alias,
        compiler_params=pltpu.CompilerParams(vmem_limit_bytes=VMEM_LIMIT),
        cost_estimate=pl.CostEstimate(flops=4 * n_rows * n_rows * (stop - start), bytes_accessed=10 * n_rows * (stop - start), transcendentals=0),
    )(*args)


def last_kernel(consts, start, pos_ref, theta_ref, kern_hbm, mass_ref, zb_ref, mean_ref, prec_ref, fact_ref, *rest):
    out_ref, send_ref, rhs, kern_ref, kern_sem = rest[-5:]

    def fetch(mine):
        rs = pl.ds(pl.multiple_of(lax.rem(1 - pos_ref[0] + mine, 2) * out_ref.shape[0], BLK), out_ref.shape[0])
        return pltpu.make_async_copy(kern_hbm.at[rs, :], kern_ref.at[rs, :], kern_sem.at[mine])

    fetch(0).start()
    fetch(1).start()
    rows = out_ref.shape[0]
    part = pos_ref[0]
    now = columns(part, start, theta_ref.shape[1], (mean_ref, prec_ref, fact_ref))

    @pl.loop(0, 2)
    def _(b):
        rs = pl.ds(pl.multiple_of(b * rows, BLK), rows)
        build_rhs(theta_ref[rs, :], *now, zb_ref, rhs, rs)

    size = BLK if theta_ref.shape[1] < BLK else HALF
    each = rows // size

    @pl.loop(0, 2 * each)
    def _(b):
        mine = b // each

        @pl.when(lax.rem(b, each) == 0)
        def _():
            fetch(mine).wait()

        at = pl.multiple_of(lax.rem(b, each) * size, size)
        rs = pl.ds(pl.multiple_of(lax.rem(1 - part + mine, 2) * rows + at, size), size)
        acc = jnp.dot(kern_ref[rs, :], rhs[...], preferred_element_type=F32)
        new = stepped(theta_ref[rs, :], acc, mass_ref, rs, *consts)

        @pl.when(mine == 0)
        def _():
            send_ref[pl.ds(at, size), :] = new

        @pl.when(mine == 1)
        def _():
            out_ref[pl.ds(at, size), :] = new


def last_update(consts, pos, theta, kern, mass, zb, mean, prec, fact_t, out, start, tile):
    n_rows, width = theta.shape
    chunk = start // tile
    rows, feat = n_rows // 2, width * 2
    per = width // tile
    col = lambda r: pl.BlockSpec((r, tile), lambda i, pos: (0, chunk))
    in_specs = [col(n_rows), ANY, VMEM, VMEM, VMEM, VMEM, VMEM]
    args = [theta, kern, mass, zb, mean, prec, fact_t]
    alias = {}
    if out is not None:
        in_specs.append(ANY)
        args.append(out)
        alias = {8: 0}
    return pl.pallas_call(
        functools.partial(last_kernel, consts, start),
        grid_spec=pltpu.PrefetchScalarGridSpec(
            num_scalar_prefetch=1, grid=(1,), in_specs=in_specs,
            out_specs=(pl.BlockSpec((rows, tile), lambda i, pos: (0, pos[0] * per + chunk)),
                       pl.BlockSpec((rows, tile), lambda i, pos: (0, 0))),
            scratch_shapes=[pltpu.VMEM((n_rows, 2 * tile), BF16), pltpu.VMEM(kern.shape, BF16), pltpu.SemaphoreType.DMA((2,))]),
        out_shape=(jax.ShapeDtypeStruct((rows, feat), F32), jax.ShapeDtypeStruct((rows, tile), F32)),
        input_output_aliases=alias,
        compiler_params=pltpu.CompilerParams(vmem_limit_bytes=VMEM_LIMIT),
        cost_estimate=pl.CostEstimate(flops=4 * n_rows * n_rows * tile, bytes_accessed=10 * n_rows * tile, transcendentals=0),
    )(pos, *args)


def own_kernel(consts, foreign, pos_ref, theta_ref, kern_ref, mass_ref, zb_ref, mean_ref, prec_ref, fact_ref, base_ref, out_ref, rhs):
    rows = out_ref.shape[0]
    half = 1 - pos_ref[0] if foreign else pos_ref[0]
    now = columns(half, pl.program_id(0) * BLK, BLK, (mean_ref, prec_ref, fact_ref))

    @pl.loop(0, theta_ref.shape[0] // BLK)
    def _(b):
        rs = pl.ds(pl.multiple_of(b * BLK, BLK), BLK)
        build_rhs(theta_ref[rs, :], *now, zb_ref, rhs, rs)

    @pl.loop(0, rows // BLK)
    def _(b):
        rs = pl.ds(pl.multiple_of(pos_ref[0] * rows + b * BLK, BLK), BLK)
        acc = jnp.dot(kern_ref[rs, :], rhs[...], preferred_element_type=F32)
        out_ref[pl.ds(pl.multiple_of(b * BLK, BLK), BLK), :] = stepped(theta_ref[rs, :], acc, mass_ref, rs, *consts)


def own_update(consts, pos, theta, kern, mass, zb, mean, prec, fact_t, out, foreign):
    n_rows, cols = theta.shape
    rows, feat = out.shape
    per = feat // (2 * BLK)
    col = lambda r: pl.BlockSpec((r, BLK), lambda i, pos: (0, i))
    where = (lambda i, pos: (0, (1 - pos[0]) * per + i)) if foreign else (lambda i, pos: (0, pos[0] * per + i))
    return pl.pallas_call(
        functools.partial(own_kernel, consts, foreign),
        grid_spec=pltpu.PrefetchScalarGridSpec(
            num_scalar_prefetch=1, grid=(cols // BLK,),
            in_specs=[col(n_rows), VMEM, VMEM, VMEM, VMEM, VMEM, VMEM, ANY],
            out_specs=pl.BlockSpec((rows, BLK), where),
            scratch_shapes=[pltpu.VMEM((n_rows, 2 * BLK), BF16)]),
        out_shape=jax.ShapeDtypeStruct(out.shape, F32),
        input_output_aliases={8: 0},
        compiler_params=pltpu.CompilerParams(vmem_limit_bytes=VMEM_LIMIT),
        cost_estimate=pl.CostEstimate(flops=4 * rows * n_rows * cols, bytes_accessed=10 * n_rows * cols, transcendentals=0),
        name="own_foreign" if foreign else "own_shared",
    )(pos, theta, kern, mass, zb, mean, prec, fact_t, out)


def place_kernel(pos_ref, recv_ref, base_ref, out_ref):
    out_ref[...] = recv_ref[...]


def place(pos, recv, out, start):
    rows, tile = recv.shape
    per = out.shape[1] // 256
    sub = tile // 128
    first = start // 128
    return pl.pallas_call(
        place_kernel,
        grid_spec=pltpu.PrefetchScalarGridSpec(
            num_scalar_prefetch=1, grid=(sub,), in_specs=[pl.BlockSpec((rows, 128), lambda i, pos: (0, i)), ANY],
            out_specs=pl.BlockSpec((rows, 128), lambda i, pos: (0, (1 - pos[0]) * per + first + i))),
        out_shape=jax.ShapeDtypeStruct(out.shape, out.dtype),
        input_output_aliases={2: 0},
        cost_estimate=pl.CostEstimate(flops=1000 * rows * tile, bytes_accessed=8 * rows * tile, transcendentals=0),
    )(pos, recv, out)


def greet():
    ens, part, feat = lax.axis_index("ens"), lax.axis_index("part"), lax.axis_index("feat")
    barrier = pltpu.get_barrier_semaphore()
    for i in range(1, 8):
        there = (ens, lax.rem(part + i // 4, 2), lax.rem(feat + i % 4, 4))
        pl.semaphore_signal(barrier, inc=1, device_id=there, device_id_type=MESH)
    pl.semaphore_wait(barrier, 7)


def kmat_body(from_gram, two_over_h, src_ref, proj_ref, kern_out, zb_ref, mass_ref, *scratch):
    if not from_gram:
        tb, load_sem = scratch[-2:]
    (gbuf, sib_in, r_x1, r_y1, r_x2, r_y2, sq_parts, sq, z_in, z_all, kbuf,
     sib_send, sib_recv, rs_send, rs_recv, sq_send, sq_recv, z_send, z_recv, zb_send, zb_recv,
     k_send, k_recv, _, kern_ref, kern_sem) = scratch[:26]
    n_rows = kern_ref.shape[0]
    n_blk = n_rows // BLK
    ens, part, feat = lax.axis_index("ens"), lax.axis_index("part"), lax.axis_index("feat")
    x, core = feat // 2, lax.rem(feat, 2)

    def chip(rel):
        return lax.rem(part + rel // 2, 2), lax.rem(x + rel % 2, 2)

    def block(rel, flip):
        cy, cx = chip(rel)
        return cy * 4 + cx * 2 + lax.rem(core + flip, 2)

    def device(rel, flip):
        cy, cx = chip(rel)
        return (ens, cy, cx * 2 + lax.rem(core + flip, 2))

    me = block(0, 0)
    sibling, dev_x, dev_y = device(0, 1), device(1, 0), device(2, 0)
    others = [(rel, flip) for rel in (3, 1, 2, 0) for flip in (0, 1) if (rel, flip) != (0, 0)]

    def rcopy(src, dst, ssem, rsem, dev):
        return pltpu.make_async_remote_copy(src_ref=src, dst_ref=dst, send_sem=ssem, recv_sem=rsem,
                                            device_id=dev, device_id_type=MESH)

    def load(b):
        rs = pl.ds(b * BLK, BLK)
        return pltpu.make_async_copy(src_ref.at[rs, :], tb.at[rs, :], load_sem.at[b])

    if not from_gram:
        for b in range(n_blk):
            load(b).start()
        greet()

    def z_cols(b):
        return proj_ref.at[:, pl.ds(pl.multiple_of(b * BLK, BLK), BLK)]

    def z_copy(i):
        rel, flip = others[i]
        return rcopy(z_cols(block(rel, flip)), z_in.at[me], z_send.at[i], z_recv.at[me], device(rel, flip))

    for i in range(len(others)):
        z_copy(i).start()
    z_own = pltpu.make_async_copy(z_cols(me), z_in.at[me], z_recv.at[me])
    z_own.start()

    def sib_copy(rel):
        src = src_ref.at[block(rel, 1)] if from_gram else gbuf.at[4 + rel]
        return rcopy(src, sib_in.at[rel], sib_send.at[rel], sib_recv.at[rel], sibling)

    lo, hi = 0, 1
    rs_copies = {
        "d_lo": rcopy(gbuf.at[3, lo], r_x1.at[0], rs_send.at[0], rs_recv.at[0], dev_x),
        "d_hi": rcopy(gbuf.at[3, hi], r_y1.at[0], rs_send.at[1], rs_recv.at[1], dev_y),
        "y_hi": rcopy(gbuf.at[2, hi], r_y1.at[1], rs_send.at[2], rs_recv.at[2], dev_y),
        "x_lo": rcopy(gbuf.at[1, lo], r_x1.at[1], rs_send.at[3], rs_recv.at[3], dev_x),
        "y_lo": rcopy(gbuf.at[2, lo], r_y2, rs_send.at[4], rs_recv.at[4], dev_y),
        "x_hi": rcopy(gbuf.at[1, hi], r_x2, rs_send.at[5], rs_recv.at[5], dev_x),
    }
    eye = (lax.broadcasted_iota(jnp.int32, (HALF, HALF), 0) == lax.broadcasted_iota(jnp.int32, (HALF, HALF), 1)).astype(F32)

    def merge(rel):
        sib_copy(rel).wait_recv()
        gbuf[rel] = src_ref[block(rel, 0)] + sib_in[rel]

    def first_sends(rel):
        for name in {3: ("d_lo", "d_hi"), 2: ("y_hi",), 1: ("x_lo",), 0: ()}[rel]:
            rs_copies[name].start()

    if from_gram:
        for rel in (3, 2, 1, 0):
            sib_copy(rel).start()
        for rel in (3, 2, 1, 0):
            merge(rel)
            first_sends(rel)
    else:
        def rows_at(at, n):
            return tb[pl.ds(pl.multiple_of(at, HALF), n), :]

        for b in range(n_blk):
            load(b).wait()

        @pl.loop(0, 8)
        def _(i):
            rel, own = 3 - i // 2, lax.rem(i, 2)
            cy, cx = lax.rem(part + rel // 2, 2), lax.rem(x + lax.rem(rel, 2), 2)
            b = cy * 4 + cx * 2 + lax.rem(core + 1 - own, 2)
            dst = rel + 4 * (1 - own)
            for h, rows_, cols_, piece in band_pieces(rows_at, b, n_blk):
                gbuf[dst, h, rows_, cols_] = piece
            across = rcopy(gbuf.at[4 + rel], sib_in.at[rel], sib_send.at[rel], sib_recv.at[rel], sibling)

            @pl.when(own == 0)
            def _():
                across.start()

            @pl.when(own == 1)
            def _():
                across.wait_recv()
                gbuf[rel] += sib_in[rel]
                for r in (3, 2, 1):
                    @pl.when(rel == r)
                    def _():
                        first_sends(r)

    for rel in range(4):
        cy, cx = chip(rel)
        for h in range(2):
            sq_parts[me, cy * 2 + cx, :, h * HALF:(h + 1) * HALF] = jnp.sum(gbuf[rel, h, :HALF, :HALF] * eye, axis=0, keepdims=True)

    def sq_copy(i):
        rel, flip = others[i]
        return rcopy(sq_parts.at[me], sq_parts.at[me], sq_send.at[i], sq_recv.at[me], device(rel, flip))

    def recv_from(buf, sem, rel, flip):
        b = block(rel, flip)
        return rcopy(buf.at[b], buf.at[b], sq_send.at[0], sem.at[b], sibling)

    for i in range(len(others)):
        sq_copy(i).start()

    rs_copies["d_lo"].wait_recv()
    gbuf[2, 0] += r_x1[0]
    rs_copies["y_lo"].start()
    rs_copies["d_hi"].wait_recv()
    gbuf[1, 1] += r_y1[0]
    rs_copies["x_hi"].start()

    z_own.wait()
    for rel, flip in others:
        recv_from(z_in, z_recv, rel, flip).wait_recv()
    z_sum = z_in[0]
    for b in range(1, n_blk):
        z_sum = z_sum + z_in[b]
    z_all[me] = z_sum.astype(BF16)

    def zb_copy(i):
        rel, flip = others[i]
        return rcopy(z_all.at[me], z_all.at[me], zb_send.at[i], zb_recv.at[me], device(rel, flip))

    for i in range(len(others)):
        zb_copy(i).start()
    for rel, flip in others:
        recv_from(sq_parts, sq_recv, rel, flip).wait_recv()
    for c in range(2):
        for q in range(4):
            s = sq_parts[c, q] + sq_parts[2 + c, q] + sq_parts[4 + c, q] + sq_parts[6 + c, q]
            b = 2 * q + c
            sq[:, b * BLK:(b + 1) * BLK] = s
            if b < WIDE // BLK:
                sq[:, n_rows + b * BLK:n_rows + (b + 1) * BLK] = s

    def sq_at(at, n):
        return sq[:, pl.ds(pl.multiple_of(at * HALF, HALF), n)]

    def upright(row):
        return jnp.sum(eye * row, axis=1, keepdims=True)

    def kernel_of(gram, col, row):
        return jnp.exp(-jnp.maximum(col + row - 2.0 * gram, 0.0) * (0.5 * two_over_h))

    def make_band(h, gram):
        idx = 2 * me + h
        row = sq_at(idx, WIDE)
        kbuf[idx, :HALF, :] = kernel_of(gram[:HALF], upright(row[:, :HALF]), row).astype(BF16)
        col = upright(sq_at(me, HALF))[h * (HALF // 2):(h + 1) * (HALF // 2)]
        kbuf[idx, HALF:, :] = fold(kernel_of(unfold(gram[HALF:]), col, sq_at(me + n_blk, HALF))).astype(BF16)

    slots = iter(range(14))
    sent = []

    def send_band(idx, dev):
        s = next(slots)
        cp = rcopy(kbuf.at[idx], kbuf.at[idx], k_send.at[s], k_recv.at[idx], dev)
        cp.start()
        sent.append(cp)

    def wait_band(idx):
        rcopy(kbuf.at[idx], kbuf.at[idx], k_send.at[0], k_recv.at[idx], sibling).wait_recv()

    def spread(b, h):
        idx = 2 * b + h
        row0 = pl.multiple_of(idx * HALF, HALF)
        kern_ref[pl.ds(row0, HALF), pl.ds(row0, HALF)] = kbuf[idx, :HALF, :HALF]

        @pl.loop(1, WIDE // HALF)
        def _(k):
            col0 = pl.multiple_of(lax.rem(idx + k, 2 * n_blk) * HALF, HALF)
            tile = kbuf[idx, :HALF, pl.ds(pl.multiple_of(k * HALF, HALF), HALF)]
            kern_ref[pl.ds(row0, HALF), pl.ds(col0, HALF)] = tile
            kern_ref[pl.ds(col0, HALF), pl.ds(row0, HALF)] = tile.T

    rs_copies["x_lo"].wait_recv()
    rs_copies["y_lo"].wait_recv()
    make_band(0, gbuf[0, 0] + (r_x1[1] + r_y2[...]))
    for dev in (dev_y, sibling):
        send_band(2 * me, dev)
    rs_copies["y_hi"].wait_recv()
    rs_copies["x_hi"].wait_recv()
    make_band(1, gbuf[0, 1] + (r_y1[1] + r_x2[...]))
    for dev in (dev_x, sibling):
        send_band(2 * me + 1, dev)
    send_band(2 * me, dev_x)
    send_band(2 * me + 1, dev_y)
    spread(me, 0)
    spread(me, 1)
    sib = block(0, 1)
    for h in range(2):
        wait_band(2 * sib + h)
        spread(sib, h)
    bx, by, bd = block(1, 0), block(2, 0), block(3, 0)
    wait_band(2 * by)
    send_band(2 * by, dev_x)
    send_band(2 * by, sibling)
    wait_band(2 * bx + 1)
    send_band(2 * bx + 1, dev_y)
    send_band(2 * bx + 1, sibling)
    spread(by, 0)
    spread(bx, 1)
    for b, h in ((bx, 0), (by, 1), (bd, 0), (bd, 1)):
        wait_band(2 * b + h)
        send_band(2 * b + h, sibling)
        spread(b, h)
    for rel, h in ((2, 0), (1, 1), (1, 0), (2, 1), (3, 0), (3, 1)):
        b = block(rel, 1)
        wait_band(2 * b + h)
        spread(b, h)
    for rel, flip in others:
        recv_from(z_all, zb_recv, rel, flip).wait_recv()

    @pl.loop(0, n_blk)
    def _(b):
        tile = jnp.concatenate([unfold(kbuf[2 * b + h, HALF:, :].astype(F32)) for h in range(2)], axis=0)
        near = pl.ds(pl.multiple_of(b * HALF, HALF), HALF)
        away = pl.ds(pl.multiple_of((b + n_blk) * HALF, HALF), HALF)
        kern_ref[near, away] = tile.astype(BF16)
        kern_ref[away, near] = tile.T.astype(BF16)

    def put(b):
        rs = pl.ds(pl.multiple_of(b * BLK, BLK), BLK)
        return pltpu.make_async_copy(kern_ref.at[rs, :], kern_out.at[rs, :], kern_sem.at[b])

    @pl.loop(0, n_blk)
    def _(b):
        rs = pl.ds(pl.multiple_of(b * BLK, BLK), BLK)
        zb_ref[rs, :] = z_all[b].astype(F32).T.astype(BF16)
        mass_ref[rs, :] = jnp.sum(kern_ref[rs, :].astype(F32), axis=1, keepdims=True)
        put(b).start()

    @pl.loop(0, n_blk)
    def _(b):
        put(b).wait()

    for rel in range(4):
        sib_copy(rel).wait_send()
    for cp in rs_copies.values():
        cp.wait_send()
    for i in range(len(others)):
        z_copy(i).wait_send()
        sq_copy(i).wait_send()
        zb_copy(i).wait_send()
    for cp in sent:
        cp.wait_send()


def kmat_scratch(n_rows, rank, n_own):
    n_blk = n_rows // BLK
    dma = lambda *n: pltpu.SemaphoreType.DMA(n)
    return [
        pltpu.VMEM((n_own, 2, TALL, WIDE), F32), pltpu.VMEM((4, 2, TALL, WIDE), F32),
        pltpu.VMEM((2, TALL, WIDE), F32), pltpu.VMEM((2, TALL, WIDE), F32),
        pltpu.VMEM((TALL, WIDE), F32), pltpu.VMEM((TALL, WIDE), F32),
        pltpu.VMEM((8, 4, 1, BLK), F32), pltpu.VMEM((1, n_rows + WIDE), F32),
        pltpu.VMEM((n_blk, rank, BLK), F32), pltpu.VMEM((n_blk, rank, BLK), BF16),
        pltpu.VMEM((2 * n_blk, TALL, WIDE), BF16),
        dma(4), dma(4), dma(6), dma(6), dma(7), dma(8), dma(7), dma(8), dma(7), dma(8), dma(14), dma(16), dma(4),
        pltpu.VMEM((n_rows, n_rows), BF16), dma(n_blk)]


def kmat_shapes(n_rows, rank):
    return (jax.ShapeDtypeStruct((n_rows, n_rows), BF16), jax.ShapeDtypeStruct((n_rows, rank), BF16),
            jax.ShapeDtypeStruct((n_rows, 1), F32))


def kernel_matrix(tb, proj, two_over_h, collective_id):
    rank, n_rows = proj.shape
    return pl.pallas_call(
        functools.partial(kmat_body, False, two_over_h),
        out_shape=kmat_shapes(n_rows, rank), in_specs=[ANY, VMEM], out_specs=(ANY, VMEM, VMEM),
        scratch_shapes=kmat_scratch(n_rows, rank, 8) + [pltpu.VMEM(tb.shape, BF16), pltpu.SemaphoreType.DMA((n_rows // BLK,))],
        compiler_params=pltpu.CompilerParams(collective_id=collective_id, has_side_effects=True, vmem_limit_bytes=VMEM_LIMIT),
    )(tb, proj)


def opening_kernel(n_early, n_late, two_over_h, theta_ref, mean_ref, fact_ref, col_ref, late_own_ref, late_away_ref,
                   kern_out, zb_ref, mass_ref, gram, proj, *scratch):
    greet()
    exchange_body(n_early, n_late, theta_ref, mean_ref, fact_ref, col_ref, late_own_ref, late_away_ref, gram, proj, *scratch[:12])
    kmat_body(True, two_over_h, gram, proj, kern_out, zb_ref, mass_ref, *scratch[12:])


def opening(theta, mean, fact_t, two_over_h, n_early, n_late):
    rows, feat = theta.shape
    rank = fact_t.shape[0]
    width = feat // 2
    n_rows = rows * 2
    cw = width // (n_early + n_late)
    dma = lambda *n: pltpu.SemaphoreType.DMA(n)
    return pl.pallas_call(
        functools.partial(opening_kernel, n_early, n_late, two_over_h),
        out_shape=(jax.ShapeDtypeStruct((n_rows, n_early * cw), F32),
                   jax.ShapeDtypeStruct((rows, n_late * cw), F32),
                   jax.ShapeDtypeStruct((rows, n_late * cw), F32)) + kmat_shapes(n_rows, rank),
        in_specs=[ANY, VMEM, VMEM], out_specs=(ANY, ANY, ANY, ANY, VMEM, VMEM),
        scratch_shapes=[
            pltpu.VMEM((n_rows // BLK, 2, TALL, WIDE), F32), pltpu.VMEM((rank, n_rows), F32),
            pltpu.VMEM((n_rows, cw), F32), pltpu.VMEM((n_rows, cw), BF16), pltpu.VMEM((rows, cw), F32),
            pltpu.VMEM((n_late, rows, cw), BF16), pltpu.VMEM((n_late, rows, cw), BF16),
            dma(n_early), dma(n_early), dma(n_late), dma(n_late),
            pltpu.SemaphoreType.DMA, pltpu.SemaphoreType.DMA, pltpu.SemaphoreType.DMA] + kmat_scratch(n_rows, rank, 4),
        compiler_params=pltpu.CompilerParams(collective_id=0, has_side_effects=True, vmem_limit_bytes=VMEM_LIMIT),
        name="opening",
    )(theta, mean, fact_t)


def solution(mesh):
    part_size = mesh.shape["part"]
    feat_size = mesh.shape["feat"]

    def local_steps(theta, prec_loc, mean_loc, factor_loc):
        rows, feat_loc = theta.shape
        n_total = rows * part_size
        feat_total = feat_loc * feat_size
        width = feat_loc // part_size
        kern_width = 2.0 * feat_total / math.log(n_total)
        step_size = 0.15 * n_total * feat_total / math.log(n_total)
        consts = (1.0 / n_total, 2.0 / kern_width, step_size)
        part = lax.axis_index("part")
        pos = part.astype(jnp.int32).reshape(1)
        params = (mean_loc.reshape(1, feat_loc), prec_loc.reshape(1, feat_loc), factor_loc.T)
        shared = 2 * BLK
        chunks = [(shared, HALF)] + [(at, 2 * BLK) for at in range(2 * shared, width, 2 * BLK)] + [(shared + BLK, BLK), (shared + HALF, HALF)]
        swap = [(0, 1), (1, 0)]
        late = 3 * BLK
        early = width - late

        cur, late_own, late_away, kern, zb, mass = opening(theta, params[0], params[2], consts[1], early // BLK, late // BLK)
        recv = lax.ppermute(late_away, "part", swap)
        new, tb, proj = update(consts, cur, kern, mass, zb, params, width, 0, early, False)
        cur, tb, proj = update(consts, (late_own, recv), kern, mass, zb, params, width, early, width, False, (tb, proj, new))
        kern, zb, mass = kernel_matrix(tb, proj, consts[1], 2)
        both, tb, proj = update(consts, cur, kern, mass, zb, params, width, 0, shared, True)
        foreign = lax.ppermute(both, "part", swap)
        cur, tb, proj = update(consts, cur, kern, mass, zb, params, width, shared, width, False, (tb, proj))
        kern, zb, mass = kernel_matrix(tb, proj, consts[1], 3)
        out = None
        received = []
        for start, tile in chunks:
            out, send = last_update(consts, pos, cur, kern, mass, zb, *params, out, start, tile)
            received.append(lax.ppermute(send, "part", swap))
        out = own_update(consts, pos, both, kern, mass, zb, *params, out, False)
        out = own_update(consts, pos, foreign, kern, mass, zb, *params, out, True)
        for (start, tile), recv in zip(chunks, received):
            out = place(pos, recv, out, start)
        return out

    row_spec = P(("ens", "part"), "feat")
    vec_spec = P(("ens", "feat"))
    fac_spec = P(("ens", "feat"), None)
    return jax.shard_map(local_steps, mesh=mesh, in_specs=(row_spec, vec_spec, vec_spec, fac_spec), out_specs=row_spec, check_vma=False)
```

```python
import functools
import math
import jax
import jax.numpy as jnp
from jax import lax
from jax.experimental import pallas as pl
from jax.experimental.pallas import tpu as pltpu
from jax.sharding import PartitionSpec as P

BLK = 256
HALF = BLK // 2
WIDE = 8 * HALF
TALL = HALF + 8
MESH = pl.DeviceIdType.MESH
F32 = jnp.float32
BF16 = jnp.bfloat16
ANY = pl.BlockSpec(memory_space=pl.ANY)
VMEM = pl.BlockSpec(memory_space=pltpu.VMEM)
VMEM_LIMIT = 63 * 1024 * 1024
NT = (((1,), (1,)), ((), ()))


def fold(tile):
    return jnp.concatenate([tile[8 * g:8 * g + 8] for g in range(8)], axis=1)


def unfold(rows):
    return jnp.concatenate([rows[:, HALF * g:HALF * (g + 1)] for g in range(8)], axis=0)


def band_pieces(rows_at, b, n_blk):
    def dot(left, right):
        return lax.dot_general(left, right, NT, preferred_element_type=F32)

    def wrap(j):
        return j % n_blk if isinstance(j, int) else lax.rem(j, n_blk)

    main = slice(0, HALF)
    both = rows_at(b * BLK, BLK)
    for k in range(4):
        val = dot(both, rows_at(wrap(b + k) * BLK, BLK))
        yield 0, main, slice(k * BLK, (k + 1) * BLK), val[:HALF]
        if k == 0:
            yield 1, main, slice(0, HALF), val[HALF:, HALF:]
        else:
            yield 1, main, slice(k * BLK - HALF, k * BLK + HALF), val[HALF:]
    yield 1, main, slice(WIDE - HALF, WIDE), dot(rows_at(b * BLK + HALF, HALF), rows_at(wrap(b + 4) * BLK, HALF))
    far = dot(rows_at(b * HALF, HALF), rows_at((b + n_blk) * HALF, HALF))
    for h in range(2):
        yield h, slice(HALF, TALL), slice(0, WIDE), fold(far[h * (HALF // 2):(h + 1) * (HALF // 2)])


def exchange_body(n_early, n_late, theta_ref, mean_ref, fact_ref, col_ref, late_own_ref, late_away_ref, gram_ref, proj_ref,
                  buf, tb, away, away_b, late_b, send_sem, recv_sem, lsend_sem, lrecv_sem, own_sem, put_sem, other_sem):
    part = lax.axis_index("part")
    other = 1 - part
    peer = (lax.axis_index("ens"), other, lax.axis_index("feat"))
    rows, width = theta_ref.shape[0], theta_ref.shape[1] // 2
    n_rows = col_ref.shape[0]
    cw = width // (n_early + n_late)
    n_blk = n_rows // BLK
    own_rows = pl.ds(pl.multiple_of(part * rows, BLK), rows)
    other_rows = pl.ds(pl.multiple_of(other * rows, BLK), rows)

    def chunk(half, c):
        return pl.ds(pl.multiple_of(half * width + c * cw, 128), cw)

    def remote(c):
        return pltpu.make_async_remote_copy(
            src_ref=theta_ref.at[:, chunk(other, c)], dst_ref=col_ref.at[own_rows, chunk(0, c)],
            send_sem=send_sem.at[c], recv_sem=recv_sem.at[c], device_id=peer, device_id_type=MESH)

    def remote_late(c):
        return pltpu.make_async_remote_copy(
            src_ref=away_b.at[c], dst_ref=late_b.at[c],
            send_sem=lsend_sem.at[c], recv_sem=lrecv_sem.at[c], device_id=peer, device_id_type=MESH)

    def fetch_own(c):
        return pltpu.make_async_copy(theta_ref.at[:, chunk(part, c)], buf.at[own_rows, :], own_sem)

    def put_own(c):
        return pltpu.make_async_copy(buf.at[own_rows, :], col_ref.at[own_rows, chunk(0, c)], put_sem)

    def put_late(c):
        return pltpu.make_async_copy(buf.at[own_rows, :], late_own_ref.at[:, chunk(0, c - n_early)], put_sem)

    def fetch_other(c):
        return pltpu.make_async_copy(col_ref.at[other_rows, chunk(0, c)], buf.at[other_rows, :], other_sem)

    def project(src, row0, half, c, dst_row0):
        x = src[pl.ds(pl.multiple_of(row0, BLK), BLK), :] - mean_ref[:, chunk(half, c)]
        proj_ref[:, pl.ds(pl.multiple_of(dst_row0, BLK), BLK)] += lax.dot_general(
            fact_ref[:, chunk(half, c)], x.astype(BF16), NT, preferred_element_type=F32)

    def add_gram():
        for b in range(n_blk):
            for h, rows_, cols_, piece in band_pieces(lambda at, n: tb[at:at + n, :], b, n_blk):
                gram_ref[b, h, rows_, cols_] += piece

    @pl.loop(0, n_early)
    def _(c):
        remote(c).start()

    gram_ref[...] = jnp.zeros_like(gram_ref)
    proj_ref[...] = jnp.zeros_like(proj_ref)

    @pl.loop(0, n_late)
    def _(c):
        fetch = pltpu.make_async_copy(theta_ref.at[:, chunk(other, n_early + c)], away, other_sem)
        fetch.start()
        fetch.wait()
        keep = pltpu.make_async_copy(away, late_away_ref.at[:, chunk(0, c)], own_sem)
        keep.start()

        @pl.loop(0, rows // BLK)
        def _(b):
            rs = pl.ds(pl.multiple_of(b * BLK, BLK), BLK)
            away_b[c, rs, :] = away[rs, :].astype(BF16)
            project(away, b * BLK, other, n_early + c, part * rows + b * BLK)

        keep.wait()

    @pl.loop(0, n_late)
    def _(c):
        remote_late(c).start()

    @pl.loop(0, n_early + n_late)
    def _(c):
        fetch_own(c).start()
        fetch_own(c).wait()

        @pl.when(c < n_early)
        def _():
            put_own(c).start()

        @pl.when(c >= n_early)
        def _():
            put_late(c).start()

        @pl.loop(0, rows // BLK)
        def _(b):
            row0 = part * rows + b * BLK
            rs = pl.ds(pl.multiple_of(row0, BLK), BLK)
            tb[rs, :] = buf[rs, :].astype(BF16)
            project(buf, row0, part, c, row0)

        @pl.when(c < n_early)
        def _():
            remote(c).wait_recv()
            fetch_other(c).start()
            fetch_other(c).wait()

            @pl.loop(0, rows // BLK)
            def _(b):
                row0 = other * rows + b * BLK
                rs = pl.ds(pl.multiple_of(row0, BLK), BLK)
                tb[rs, :] = buf[rs, :].astype(BF16)
                project(buf, row0, part, c, row0)

        @pl.when(c >= n_early)
        def _():
            remote_late(c - n_early).wait_recv()
            tb[other_rows, :] = late_b[c - n_early]

        add_gram()

        @pl.when(c < n_early)
        def _():
            put_own(c).wait()

        @pl.when(c >= n_early)
        def _():
            put_late(c).wait()

    @pl.loop(0, n_early)
    def _(c):
        remote(c).wait_send()

    @pl.loop(0, n_late)
    def _(c):
        remote_late(c).wait_send()


def columns(half, start, tile, refs):
    cols = pl.ds(pl.multiple_of(half * (refs[0].shape[1] // 2) + start, 128), tile)
    return tuple(ref[:, cols] for ref in refs)


def build_rhs(th, mean, prec, fact, zb_ref, rhs, rs):
    tile = th.shape[1]
    low = jnp.dot(zb_ref[rs, :], fact, preferred_element_type=F32)
    rhs[rs, :tile] = (-((th - mean) * prec + low)).astype(BF16)
    rhs[rs, tile:] = th.astype(BF16)


def stepped(th, acc, mass_ref, rs, inv_n, two_over_h, step_size):
    tile = th.shape[1]
    pull = mass_ref[rs, :] * th.astype(BF16).astype(F32) - acc[:, tile:]
    return th + step_size * ((acc[:, :tile] + two_over_h * pull) * inv_n)


def update_kernel(consts, first, split, has_before, *refs):
    n_in = 2 * (2 if split else 1)
    kern_hbm, mass_ref, zb_ref = refs[n_in:n_in + 3]
    params = refs[n_in + 3:n_in + 6]
    out_ref, tb_ref, proj_ref, rhs, kern_ref, kern_sem = refs[-6:]
    tile = out_ref.shape[1]
    big = out_ref.shape[0] // 2
    i = pl.program_id(0)
    slot = lax.rem(i, 2)
    part = lax.axis_index("part")

    def span(at, size):
        return pl.ds(pl.multiple_of(at, BLK), size)

    def order(h):
        return lax.rem(part + h, 2) if split else h

    def fetch(half):
        return pltpu.make_async_copy(kern_hbm.at[span(half * big, big), :], kern_ref.at[span(half * big, big), :], kern_sem.at[half])

    @pl.when(i == 0)
    def _():
        for h in range(2):
            fetch(order(h)).start()
        proj_ref[...] = refs[n_in + 6][...] if has_before else jnp.zeros_like(proj_ref)
        now = columns(part, first * tile, tile, params)
        if split:
            for ref, half in ((refs[0], part), (refs[2], 1 - part)):
                build_rhs(ref[...], *now, zb_ref, rhs.at[0], span(half * big, big))
        else:
            @pl.loop(0, 2)
            def _(b):
                rs = span(b * big, big)
                build_rhs(refs[0][rs, :], *now, zb_ref, rhs.at[0], rs)

    mean, _, fact = columns(part, (first + i) * tile, tile, params)
    after = columns(part, (first + jnp.minimum(i + 1, pl.num_programs(0) - 1)) * tile, tile, params)

    def half_step(ref, next_ref, src, half):
        rs = span(half * big, big)

        @pl.when(i == 0)
        def _():
            fetch(half).wait()

        acc = jnp.dot(kern_ref[rs, :], rhs[slot], preferred_element_type=F32)
        build_rhs(next_ref[src, :], *after, zb_ref, rhs.at[1 - slot], rs)
        new = stepped(ref[src, :], acc, mass_ref, rs, *consts)
        out_ref[rs, :] = new
        tb_ref[rs, :] = new.astype(BF16)
        proj_ref[:, rs] += lax.dot_general(fact, (new - mean).astype(BF16), NT, preferred_element_type=F32)

    if split:
        for at, half in ((0, part), (2, 1 - part)):
            half_step(refs[at], refs[at + 1], slice(None), half)
    else:
        @pl.loop(0, 2)
        def _(b):
            half_step(refs[0], refs[1], span(b * big, big), b)


def update(consts, theta, kern, mass, zb, params, width, start, stop, own_out, before=None):
    split = isinstance(theta, tuple)
    n_rows = kern.shape[0]
    rank = params[2].shape[0]
    first, steps = start // BLK, (stop - start) // BLK
    base = 0 if split else first
    held = n_rows // 2 if split else n_rows
    in_specs, args = [], []
    for arr in theta if split else (theta,):
        in_specs += [pl.BlockSpec((held, BLK), lambda i: (0, base + i)),
                     pl.BlockSpec((held, BLK), lambda i: (0, base + jnp.minimum(i + 1, steps - 1)))]
        args += [arr, arr]
    in_specs += [ANY] + [VMEM] * 5
    args += [kern, mass, zb, *params]
    alias = {}
    if before is not None:
        in_specs += [VMEM, ANY]
        args += [before[1], before[0]]
        alias = {len(args) - 1: 1}
        if len(before) > 2:
            in_specs.append(ANY)
            args.append(before[2])
            alias[len(args) - 1] = 0
    col = pl.BlockSpec((n_rows, BLK), lambda i: (0, first + i))
    return pl.pallas_call(
        functools.partial(update_kernel, consts, first, split, before is not None),
        grid=(steps,),
        out_shape=(jax.ShapeDtypeStruct((n_rows, stop - start if own_out else width), F32),
                   jax.ShapeDtypeStruct((n_rows, width), BF16),
                   jax.ShapeDtypeStruct((rank, n_rows), F32)),
        in_specs=in_specs,
        out_specs=(pl.BlockSpec((n_rows, BLK), lambda i: (0, i)) if own_out else col, col, VMEM),
        scratch_shapes=[pltpu.VMEM((2, n_rows, 2 * BLK), BF16), pltpu.VMEM(kern.shape, BF16), pltpu.SemaphoreType.DMA((2,))],
        input_output_aliases=alias,
        compiler_params=pltpu.CompilerParams(vmem_limit_bytes=VMEM_LIMIT),
        cost_estimate=pl.CostEstimate(flops=4 * n_rows * n_rows * (stop - start), bytes_accessed=10 * n_rows * (stop - start), transcendentals=0),
    )(*args)


def last_kernel(consts, start, pos_ref, theta_ref, kern_hbm, mass_ref, zb_ref, mean_ref, prec_ref, fact_ref, *rest):
    out_ref, send_ref, rhs, kern_ref, kern_sem = rest[-5:]

    def fetch(mine):
        rs = pl.ds(pl.multiple_of(lax.rem(1 - pos_ref[0] + mine, 2) * out_ref.shape[0], BLK), out_ref.shape[0])
        return pltpu.make_async_copy(kern_hbm.at[rs, :], kern_ref.at[rs, :], kern_sem.at[mine])

    fetch(0).start()
    fetch(1).start()
    rows = out_ref.shape[0]
    part = pos_ref[0]
    now = columns(part, start, theta_ref.shape[1], (mean_ref, prec_ref, fact_ref))

    @pl.loop(0, 2)
    def _(b):
        rs = pl.ds(pl.multiple_of(b * rows, BLK), rows)
        build_rhs(theta_ref[rs, :], *now, zb_ref, rhs, rs)

    size = BLK if theta_ref.shape[1] < BLK else HALF
    each = rows // size

    @pl.loop(0, 2 * each)
    def _(b):
        mine = b // each

        @pl.when(lax.rem(b, each) == 0)
        def _():
            fetch(mine).wait()

        at = pl.multiple_of(lax.rem(b, each) * size, size)
        rs = pl.ds(pl.multiple_of(lax.rem(1 - part + mine, 2) * rows + at, size), size)
        acc = jnp.dot(kern_ref[rs, :], rhs[...], preferred_element_type=F32)
        new = stepped(theta_ref[rs, :], acc, mass_ref, rs, *consts)

        @pl.when(mine == 0)
        def _():
            send_ref[pl.ds(at, size), :] = new

        @pl.when(mine == 1)
        def _():
            out_ref[pl.ds(at, size), :] = new


def last_update(consts, pos, theta, kern, mass, zb, mean, prec, fact_t, out, start, tile):
    n_rows, width = theta.shape
    chunk = start // tile
    rows, feat = n_rows // 2, width * 2
    per = width // tile
    col = lambda r: pl.BlockSpec((r, tile), lambda i, pos: (0, chunk))
    in_specs = [col(n_rows), ANY, VMEM, VMEM, VMEM, VMEM, VMEM]
    args = [theta, kern, mass, zb, mean, prec, fact_t]
    alias = {}
    if out is not None:
        in_specs.append(ANY)
        args.append(out)
        alias = {8: 0}
    return pl.pallas_call(
        functools.partial(last_kernel, consts, start),
        grid_spec=pltpu.PrefetchScalarGridSpec(
            num_scalar_prefetch=1, grid=(1,), in_specs=in_specs,
            out_specs=(pl.BlockSpec((rows, tile), lambda i, pos: (0, pos[0] * per + chunk)),
                       pl.BlockSpec((rows, tile), lambda i, pos: (0, 0))),
            scratch_shapes=[pltpu.VMEM((n_rows, 2 * tile), BF16), pltpu.VMEM(kern.shape, BF16), pltpu.SemaphoreType.DMA((2,))]),
        out_shape=(jax.ShapeDtypeStruct((rows, feat), F32), jax.ShapeDtypeStruct((rows, tile), F32)),
        input_output_aliases=alias,
        compiler_params=pltpu.CompilerParams(vmem_limit_bytes=VMEM_LIMIT),
        cost_estimate=pl.CostEstimate(flops=4 * n_rows * n_rows * tile, bytes_accessed=10 * n_rows * tile, transcendentals=0),
    )(pos, *args)


def own_kernel(consts, foreign, pos_ref, theta_ref, kern_ref, mass_ref, zb_ref, mean_ref, prec_ref, fact_ref, base_ref, out_ref, rhs):
    rows = out_ref.shape[0]
    half = 1 - pos_ref[0] if foreign else pos_ref[0]
    now = columns(half, pl.program_id(0) * BLK, BLK, (mean_ref, prec_ref, fact_ref))

    @pl.loop(0, theta_ref.shape[0] // BLK)
    def _(b):
        rs = pl.ds(pl.multiple_of(b * BLK, BLK), BLK)
        build_rhs(theta_ref[rs, :], *now, zb_ref, rhs, rs)

    @pl.loop(0, rows // BLK)
    def _(b):
        rs = pl.ds(pl.multiple_of(pos_ref[0] * rows + b * BLK, BLK), BLK)
        acc = jnp.dot(kern_ref[rs, :], rhs[...], preferred_element_type=F32)
        out_ref[pl.ds(pl.multiple_of(b * BLK, BLK), BLK), :] = stepped(theta_ref[rs, :], acc, mass_ref, rs, *consts)


def own_update(consts, pos, theta, kern, mass, zb, mean, prec, fact_t, out, foreign):
    n_rows, cols = theta.shape
    rows, feat = out.shape
    per = feat // (2 * BLK)
    col = lambda r: pl.BlockSpec((r, BLK), lambda i, pos: (0, i))
    where = (lambda i, pos: (0, (1 - pos[0]) * per + i)) if foreign else (lambda i, pos: (0, pos[0] * per + i))
    return pl.pallas_call(
        functools.partial(own_kernel, consts, foreign),
        grid_spec=pltpu.PrefetchScalarGridSpec(
            num_scalar_prefetch=1, grid=(cols // BLK,),
            in_specs=[col(n_rows), VMEM, VMEM, VMEM, VMEM, VMEM, VMEM, ANY],
            out_specs=pl.BlockSpec((rows, BLK), where),
            scratch_shapes=[pltpu.VMEM((n_rows, 2 * BLK), BF16)]),
        out_shape=jax.ShapeDtypeStruct(out.shape, F32),
        input_output_aliases={8: 0},
        compiler_params=pltpu.CompilerParams(vmem_limit_bytes=VMEM_LIMIT),
        cost_estimate=pl.CostEstimate(flops=4 * rows * n_rows * cols, bytes_accessed=10 * n_rows * cols, transcendentals=0),
        name="own_foreign" if foreign else "own_shared",
    )(pos, theta, kern, mass, zb, mean, prec, fact_t, out)


def place_kernel(pos_ref, recv_ref, base_ref, out_ref):
    out_ref[...] = recv_ref[...]


def place(pos, recv, out, start):
    rows, tile = recv.shape
    per = out.shape[1] // 256
    sub = tile // 128
    first = start // 128
    return pl.pallas_call(
        place_kernel,
        grid_spec=pltpu.PrefetchScalarGridSpec(
            num_scalar_prefetch=1, grid=(sub,), in_specs=[pl.BlockSpec((rows, 128), lambda i, pos: (0, i)), ANY],
            out_specs=pl.BlockSpec((rows, 128), lambda i, pos: (0, (1 - pos[0]) * per + first + i))),
        out_shape=jax.ShapeDtypeStruct(out.shape, out.dtype),
        input_output_aliases={2: 0},
        cost_estimate=pl.CostEstimate(flops=1000 * rows * tile, bytes_accessed=8 * rows * tile, transcendentals=0),
    )(pos, recv, out)


def greet(between=lambda: None):
    ens, part, feat = lax.axis_index("ens"), lax.axis_index("part"), lax.axis_index("feat")
    barrier = pltpu.get_barrier_semaphore()
    for i in range(1, 8):
        there = (ens, lax.rem(part + i // 4, 2), lax.rem(feat + i % 4, 4))
        pl.semaphore_signal(barrier, inc=1, device_id=there, device_id_type=MESH)
    between()
    pl.semaphore_wait(barrier, 7)


def kmat_body(from_gram, two_over_h, src_ref, proj_ref, kern_out, zb_ref, mass_ref, *scratch):
    if not from_gram:
        tb, load_sem = scratch[-2:]
    (gbuf, sib_in, r_x1, r_y1, r_x2, r_y2, sq_parts, sq, z_in, z_all, kbuf,
     sib_send, sib_recv, rs_send, rs_recv, sq_send, sq_recv, z_send, z_recv, zb_send, zb_recv,
     k_send, k_recv, _, kern_ref, kern_sem) = scratch[:26]
    n_rows = kern_ref.shape[0]
    n_blk = n_rows // BLK
    ens, part, feat = lax.axis_index("ens"), lax.axis_index("part"), lax.axis_index("feat")
    x, core = feat // 2, lax.rem(feat, 2)

    def chip(rel):
        return lax.rem(part + rel // 2, 2), lax.rem(x + rel % 2, 2)

    def block(rel, flip):
        cy, cx = chip(rel)
        return cy * 4 + cx * 2 + lax.rem(core + flip, 2)

    def device(rel, flip):
        cy, cx = chip(rel)
        return (ens, cy, cx * 2 + lax.rem(core + flip, 2))

    me = block(0, 0)
    sibling, dev_x, dev_y = device(0, 1), device(1, 0), device(2, 0)
    others = [(rel, flip) for rel in (3, 1, 2, 0) for flip in (0, 1) if (rel, flip) != (0, 0)]

    def rcopy(src, dst, ssem, rsem, dev):
        return pltpu.make_async_remote_copy(src_ref=src, dst_ref=dst, send_sem=ssem, recv_sem=rsem,
                                            device_id=dev, device_id_type=MESH)

    def load(b):
        rs = pl.ds(b * BLK, BLK)
        return pltpu.make_async_copy(src_ref.at[rs, :], tb.at[rs, :], load_sem.at[b])

    if not from_gram:
        def load_all():
            for b in range(n_blk):
                load(b).start()

        greet(load_all)

    def z_cols(b):
        return proj_ref.at[:, pl.ds(pl.multiple_of(b * BLK, BLK), BLK)]

    def z_copy(i):
        rel, flip = others[i]
        return rcopy(z_cols(block(rel, flip)), z_in.at[me], z_send.at[i], z_recv.at[me], device(rel, flip))

    for i in range(len(others)):
        z_copy(i).start()
    z_own = pltpu.make_async_copy(z_cols(me), z_in.at[me], z_recv.at[me])
    z_own.start()

    def sib_copy(rel):
        src = src_ref.at[block(rel, 1)] if from_gram else gbuf.at[4 + rel]
        return rcopy(src, sib_in.at[rel], sib_send.at[rel], sib_recv.at[rel], sibling)

    lo, hi = 0, 1
    rs_copies = {
        "d_lo": rcopy(gbuf.at[3, lo], r_x1.at[0], rs_send.at[0], rs_recv.at[0], dev_x),
        "d_hi": rcopy(gbuf.at[3, hi], r_y1.at[0], rs_send.at[1], rs_recv.at[1], dev_y),
        "y_hi": rcopy(gbuf.at[2, hi], r_y1.at[1], rs_send.at[2], rs_recv.at[2], dev_y),
        "x_lo": rcopy(gbuf.at[1, lo], r_x1.at[1], rs_send.at[3], rs_recv.at[3], dev_x),
        "y_lo": rcopy(gbuf.at[2, lo], r_y2, rs_send.at[4], rs_recv.at[4], dev_y),
        "x_hi": rcopy(gbuf.at[1, hi], r_x2, rs_send.at[5], rs_recv.at[5], dev_x),
    }
    eye = (lax.broadcasted_iota(jnp.int32, (HALF, HALF), 0) == lax.broadcasted_iota(jnp.int32, (HALF, HALF), 1)).astype(F32)

    def merge(rel):
        sib_copy(rel).wait_recv()
        gbuf[rel] = src_ref[block(rel, 0)] + sib_in[rel]

    def first_sends(rel):
        for name in {3: ("d_lo", "d_hi"), 2: ("y_hi",), 1: ("x_lo",), 0: ()}[rel]:
            rs_copies[name].start()

    if from_gram:
        for rel in (3, 2, 1, 0):
            sib_copy(rel).start()
        for rel in (3, 2, 1, 0):
            merge(rel)
            first_sends(rel)
    else:
        def rows_at(at, n):
            return tb[pl.ds(pl.multiple_of(at, HALF), n), :]

        for b in range(n_blk):
            load(b).wait()

        @pl.loop(0, 8)
        def _(i):
            rel, own = 3 - i // 2, lax.rem(i, 2)
            cy, cx = lax.rem(part + rel // 2, 2), lax.rem(x + lax.rem(rel, 2), 2)
            b = cy * 4 + cx * 2 + lax.rem(core + 1 - own, 2)
            dst = rel + 4 * (1 - own)
            for h, rows_, cols_, piece in band_pieces(rows_at, b, n_blk):
                gbuf[dst, h, rows_, cols_] = piece
            across = rcopy(gbuf.at[4 + rel], sib_in.at[rel], sib_send.at[rel], sib_recv.at[rel], sibling)

            @pl.when(own == 0)
            def _():
                across.start()

            @pl.when(own == 1)
            def _():
                across.wait_recv()
                gbuf[rel] += sib_in[rel]
                for r in (3, 2, 1):
                    @pl.when(rel == r)
                    def _():
                        first_sends(r)

    for rel in range(4):
        cy, cx = chip(rel)
        for h in range(2):
            sq_parts[me, cy * 2 + cx, :, h * HALF:(h + 1) * HALF] = jnp.sum(gbuf[rel, h, :HALF, :HALF] * eye, axis=0, keepdims=True)

    def sq_copy(i):
        rel, flip = others[i]
        return rcopy(sq_parts.at[me], sq_parts.at[me], sq_send.at[i], sq_recv.at[me], device(rel, flip))

    def recv_from(buf, sem, rel, flip):
        b = block(rel, flip)
        return rcopy(buf.at[b], buf.at[b], sq_send.at[0], sem.at[b], sibling)

    for i in range(len(others)):
        sq_copy(i).start()

    rs_copies["d_lo"].wait_recv()
    gbuf[2, 0] += r_x1[0]
    rs_copies["y_lo"].start()
    rs_copies["d_hi"].wait_recv()
    gbuf[1, 1] += r_y1[0]
    rs_copies["x_hi"].start()

    z_own.wait()
    for rel, flip in others:
        recv_from(z_in, z_recv, rel, flip).wait_recv()
    z_sum = z_in[0]
    for b in range(1, n_blk):
        z_sum = z_sum + z_in[b]
    z_all[me] = z_sum.astype(BF16)

    def zb_copy(i):
        rel, flip = others[i]
        return rcopy(z_all.at[me], z_all.at[me], zb_send.at[i], zb_recv.at[me], device(rel, flip))

    for i in range(len(others)):
        zb_copy(i).start()
    for rel, flip in others:
        recv_from(sq_parts, sq_recv, rel, flip).wait_recv()
    for c in range(2):
        for q in range(4):
            s = sq_parts[c, q] + sq_parts[2 + c, q] + sq_parts[4 + c, q] + sq_parts[6 + c, q]
            b = 2 * q + c
            sq[:, b * BLK:(b + 1) * BLK] = s
            if b < WIDE // BLK:
                sq[:, n_rows + b * BLK:n_rows + (b + 1) * BLK] = s

    def sq_at(at, n):
        return sq[:, pl.ds(pl.multiple_of(at * HALF, HALF), n)]

    def upright(row):
        return jnp.sum(eye * row, axis=1, keepdims=True)

    def kernel_of(gram, col, row):
        return jnp.exp(-jnp.maximum(col + row - 2.0 * gram, 0.0) * (0.5 * two_over_h))

    def make_band(h, gram):
        idx = 2 * me + h
        row = sq_at(idx, WIDE)
        kbuf[idx, :HALF, :] = kernel_of(gram[:HALF], upright(row[:, :HALF]), row).astype(BF16)
        col = upright(sq_at(me, HALF))[h * (HALF // 2):(h + 1) * (HALF // 2)]
        kbuf[idx, HALF:, :] = fold(kernel_of(unfold(gram[HALF:]), col, sq_at(me + n_blk, HALF))).astype(BF16)

    slots = iter(range(14))
    sent = []

    def send_band(idx, dev):
        s = next(slots)
        cp = rcopy(kbuf.at[idx], kbuf.at[idx], k_send.at[s], k_recv.at[idx], dev)
        cp.start()
        sent.append(cp)

    def wait_band(idx):
        rcopy(kbuf.at[idx], kbuf.at[idx], k_send.at[0], k_recv.at[idx], sibling).wait_recv()

    def spread(b, h, unroll=False):
        idx = 2 * b + h
        row0 = pl.multiple_of(idx * HALF, HALF)
        kern_ref[pl.ds(row0, HALF), pl.ds(row0, HALF)] = kbuf[idx, :HALF, :HALF]

        def move(k):
            col0 = pl.multiple_of(lax.rem(idx + k, 2 * n_blk) * HALF, HALF)
            tile = kbuf[idx, :HALF, pl.ds(pl.multiple_of(k * HALF, HALF), HALF)]
            kern_ref[pl.ds(row0, HALF), pl.ds(col0, HALF)] = tile
            kern_ref[pl.ds(col0, HALF), pl.ds(row0, HALF)] = tile.T

        if unroll:
            for k in range(1, WIDE // HALF):
                move(k)
        else:
            pl.loop(1, WIDE // HALF)(move)

    def spread_far(b):
        tile = jnp.concatenate([unfold(kbuf[2 * b + h, HALF:, :].astype(F32)) for h in range(2)], axis=0)
        near = pl.ds(pl.multiple_of(b * HALF, HALF), HALF)
        away = pl.ds(pl.multiple_of((b + n_blk) * HALF, HALF), HALF)
        kern_ref[near, away] = tile.astype(BF16)
        kern_ref[away, near] = tile.T.astype(BF16)

    rs_copies["x_lo"].wait_recv()
    rs_copies["y_lo"].wait_recv()
    make_band(0, gbuf[0, 0] + (r_x1[1] + r_y2[...]))
    for dev in (dev_y, sibling):
        send_band(2 * me, dev)
    rs_copies["y_hi"].wait_recv()
    rs_copies["x_hi"].wait_recv()
    make_band(1, gbuf[0, 1] + (r_y1[1] + r_x2[...]))
    for dev in (dev_x, sibling):
        send_band(2 * me + 1, dev)
    send_band(2 * me, dev_x)
    send_band(2 * me + 1, dev_y)
    spread(me, 0)
    spread(me, 1)
    sib = block(0, 1)
    for h in range(2):
        wait_band(2 * sib + h)
        spread(sib, h)
    bx, by, bd = block(1, 0), block(2, 0), block(3, 0)
    wait_band(2 * by)
    send_band(2 * by, dev_x)
    send_band(2 * by, sibling)
    wait_band(2 * bx + 1)
    send_band(2 * bx + 1, dev_y)
    send_band(2 * bx + 1, sibling)
    spread(by, 0)
    spread(bx, 1)
    for b, h in ((bx, 0), (by, 1)):
        wait_band(2 * b + h)
        send_band(2 * b + h, sibling)
        spread(b, h)
    for rel, h in ((2, 0), (1, 1)):
        b = block(rel, 1)
        wait_band(2 * b + h)
        spread(b, h)
    for h in range(2):
        wait_band(2 * bd + h)
        send_band(2 * bd + h, sibling)
        spread(bd, h)
    for rel, h in ((1, 0), (2, 1)):
        b = block(rel, 1)
        wait_band(2 * b + h)
        spread(b, h)

    @pl.loop(0, 6)
    def _(i):
        rel = i // 2
        cy, cx = lax.rem(part + rel // 2, 2), lax.rem(x + lax.rem(rel, 2), 2)
        spread_far(cy * 4 + cx * 2 + lax.rem(i, 2))

    spread_far(bd)
    last = block(3, 1)
    for h in range(2):
        wait_band(2 * last + h)
        spread(last, h, True)
    spread_far(last)
    for rel, flip in others:
        recv_from(z_all, zb_recv, rel, flip).wait_recv()

    def put(b):
        rs = pl.ds(pl.multiple_of(b * BLK, BLK), BLK)
        return pltpu.make_async_copy(kern_ref.at[rs, :], kern_out.at[rs, :], kern_sem.at[b])

    @pl.loop(0, n_blk)
    def _(b):
        rs = pl.ds(pl.multiple_of(b * BLK, BLK), BLK)
        zb_ref[rs, :] = z_all[b].astype(F32).T.astype(BF16)
        mass_ref[rs, :] = jnp.sum(kern_ref[rs, :].astype(F32), axis=1, keepdims=True)
        put(b).start()

    @pl.loop(0, n_blk)
    def _(b):
        put(b).wait()

    for rel in range(4):
        sib_copy(rel).wait_send()
    for cp in rs_copies.values():
        cp.wait_send()
    for i in range(len(others)):
        z_copy(i).wait_send()
        sq_copy(i).wait_send()
        zb_copy(i).wait_send()
    for cp in sent:
        cp.wait_send()


def kmat_scratch(n_rows, rank, n_own):
    n_blk = n_rows // BLK
    dma = lambda *n: pltpu.SemaphoreType.DMA(n)
    return [
        pltpu.VMEM((n_own, 2, TALL, WIDE), F32), pltpu.VMEM((4, 2, TALL, WIDE), F32),
        pltpu.VMEM((2, TALL, WIDE), F32), pltpu.VMEM((2, TALL, WIDE), F32),
        pltpu.VMEM((TALL, WIDE), F32), pltpu.VMEM((TALL, WIDE), F32),
        pltpu.VMEM((8, 4, 1, BLK), F32), pltpu.VMEM((1, n_rows + WIDE), F32),
        pltpu.VMEM((n_blk, rank, BLK), F32), pltpu.VMEM((n_blk, rank, BLK), BF16),
        pltpu.VMEM((2 * n_blk, TALL, WIDE), BF16),
        dma(4), dma(4), dma(6), dma(6), dma(7), dma(8), dma(7), dma(8), dma(7), dma(8), dma(14), dma(16), dma(4),
        pltpu.VMEM((n_rows, n_rows), BF16), dma(n_blk)]


def kmat_shapes(n_rows, rank):
    return (jax.ShapeDtypeStruct((n_rows, n_rows), BF16), jax.ShapeDtypeStruct((n_rows, rank), BF16),
            jax.ShapeDtypeStruct((n_rows, 1), F32))


def kernel_matrix(tb, proj, two_over_h, collective_id):
    rank, n_rows = proj.shape
    return pl.pallas_call(
        functools.partial(kmat_body, False, two_over_h),
        out_shape=kmat_shapes(n_rows, rank), in_specs=[ANY, VMEM], out_specs=(ANY, VMEM, VMEM),
        scratch_shapes=kmat_scratch(n_rows, rank, 8) + [pltpu.VMEM(tb.shape, BF16), pltpu.SemaphoreType.DMA((n_rows // BLK,))],
        compiler_params=pltpu.CompilerParams(collective_id=collective_id, has_side_effects=True, vmem_limit_bytes=VMEM_LIMIT),
    )(tb, proj)


def opening_kernel(n_early, n_late, two_over_h, theta_ref, mean_ref, fact_ref, col_ref, late_own_ref, late_away_ref,
                   kern_out, zb_ref, mass_ref, gram, proj, *scratch):
    greet()
    exchange_body(n_early, n_late, theta_ref, mean_ref, fact_ref, col_ref, late_own_ref, late_away_ref, gram, proj, *scratch[:12])
    kmat_body(True, two_over_h, gram, proj, kern_out, zb_ref, mass_ref, *scratch[12:])


def opening(theta, mean, fact_t, two_over_h, n_early, n_late):
    rows, feat = theta.shape
    rank = fact_t.shape[0]
    width = feat // 2
    n_rows = rows * 2
    cw = width // (n_early + n_late)
    dma = lambda *n: pltpu.SemaphoreType.DMA(n)
    return pl.pallas_call(
        functools.partial(opening_kernel, n_early, n_late, two_over_h),
        out_shape=(jax.ShapeDtypeStruct((n_rows, n_early * cw), F32),
                   jax.ShapeDtypeStruct((rows, n_late * cw), F32),
                   jax.ShapeDtypeStruct((rows, n_late * cw), F32)) + kmat_shapes(n_rows, rank),
        in_specs=[ANY, VMEM, VMEM], out_specs=(ANY, ANY, ANY, ANY, VMEM, VMEM),
        scratch_shapes=[
            pltpu.VMEM((n_rows // BLK, 2, TALL, WIDE), F32), pltpu.VMEM((rank, n_rows), F32),
            pltpu.VMEM((n_rows, cw), F32), pltpu.VMEM((n_rows, cw), BF16), pltpu.VMEM((rows, cw), F32),
            pltpu.VMEM((n_late, rows, cw), BF16), pltpu.VMEM((n_late, rows, cw), BF16),
            dma(n_early), dma(n_early), dma(n_late), dma(n_late),
            pltpu.SemaphoreType.DMA, pltpu.SemaphoreType.DMA, pltpu.SemaphoreType.DMA] + kmat_scratch(n_rows, rank, 4),
        compiler_params=pltpu.CompilerParams(collective_id=0, has_side_effects=True, vmem_limit_bytes=VMEM_LIMIT),
        name="opening",
    )(theta, mean, fact_t)


def solution(mesh):
    part_size = mesh.shape["part"]
    feat_size = mesh.shape["feat"]

    def local_steps(theta, prec_loc, mean_loc, factor_loc):
        rows, feat_loc = theta.shape
        n_total = rows * part_size
        feat_total = feat_loc * feat_size
        width = feat_loc // part_size
        kern_width = 2.0 * feat_total / math.log(n_total)
        step_size = 0.15 * n_total * feat_total / math.log(n_total)
        consts = (1.0 / n_total, 2.0 / kern_width, step_size)
        part = lax.axis_index("part")
        pos = part.astype(jnp.int32).reshape(1)
        params = (mean_loc.reshape(1, feat_loc), prec_loc.reshape(1, feat_loc), factor_loc.T)
        shared = 2 * BLK
        chunks = [(shared, HALF)] + [(at, 2 * BLK) for at in range(2 * shared, width, 2 * BLK)] + [(shared + BLK, BLK), (shared + HALF, HALF)]
        swap = [(0, 1), (1, 0)]
        late = 3 * BLK
        early = width - late

        cur, late_own, late_away, kern, zb, mass = opening(theta, params[0], params[2], consts[1], early // BLK, late // BLK)
        recv = lax.ppermute(late_away, "part", swap)
        new, tb, proj = update(consts, cur, kern, mass, zb, params, width, 0, early, False)
        cur, tb, proj = update(consts, (late_own, recv), kern, mass, zb, params, width, early, width, False, (tb, proj, new))
        kern, zb, mass = kernel_matrix(tb, proj, consts[1], 2)
        both, tb, proj = update(consts, cur, kern, mass, zb, params, width, 0, shared, True)
        foreign = lax.ppermute(both, "part", swap)
        cur, tb, proj = update(consts, cur, kern, mass, zb, params, width, shared, width, False, (tb, proj))
        kern, zb, mass = kernel_matrix(tb, proj, consts[1], 3)
        out = None
        received = []
        for start, tile in chunks:
            out, send = last_update(consts, pos, cur, kern, mass, zb, *params, out, start, tile)
            received.append(lax.ppermute(send, "part", swap))
        out = own_update(consts, pos, both, kern, mass, zb, *params, out, False)
        out = own_update(consts, pos, foreign, kern, mass, zb, *params, out, True)
        for (start, tile), recv in zip(chunks, received):
            out = place(pos, recv, out, start)
        return out

    row_spec = P(("ens", "part"), "feat")
    vec_spec = P(("ens", "feat"))
    fac_spec = P(("ens", "feat"), None)
    return jax.shard_map(local_steps, mesh=mesh, in_specs=(row_spec, vec_spec, vec_spec, fac_spec), out_specs=row_spec, check_vma=False)
```

```python
import functools
import math
import jax
import jax.numpy as jnp
from jax import lax
from jax.experimental import pallas as pl
from jax.experimental.pallas import tpu as pltpu
from jax.sharding import PartitionSpec as P

BLK = 256
HALF = BLK // 2
WIDE = 8 * HALF
TALL = HALF + 8
MESH = pl.DeviceIdType.MESH
F32 = jnp.float32
BF16 = jnp.bfloat16
ANY = pl.BlockSpec(memory_space=pl.ANY)
VMEM = pl.BlockSpec(memory_space=pltpu.VMEM)
VMEM_LIMIT = 63 * 1024 * 1024
NT = (((1,), (1,)), ((), ()))


def fold(tile):
    return jnp.concatenate([tile[8 * g:8 * g + 8] for g in range(8)], axis=1)


def unfold(rows):
    return jnp.concatenate([rows[:, HALF * g:HALF * (g + 1)] for g in range(8)], axis=0)


def band_pieces(rows_at, b, n_blk, ready=lambda n: None):
    def dot(left, right):
        return lax.dot_general(left, right, NT, preferred_element_type=F32)

    def wrap(j):
        return j % n_blk if isinstance(j, int) else lax.rem(j, n_blk)

    main = slice(0, HALF)
    ready(0)
    both = rows_at(b * BLK, BLK)
    for k in range(4):
        if k > 0:
            ready(k)
        val = dot(both, rows_at(wrap(b + k) * BLK, BLK))
        yield 0, main, slice(k * BLK, (k + 1) * BLK), val[:HALF]
        if k == 0:
            yield 1, main, slice(0, HALF), val[HALF:, HALF:]
        else:
            yield 1, main, slice(k * BLK - HALF, k * BLK + HALF), val[HALF:]
    ready(4)
    yield 1, main, slice(WIDE - HALF, WIDE), dot(rows_at(b * BLK + HALF, HALF), rows_at(wrap(b + 4) * BLK, HALF))
    for n in range(5, n_blk):
        ready(n)
    far = dot(rows_at(b * HALF, HALF), rows_at((b + n_blk) * HALF, HALF))
    for h in range(2):
        yield h, slice(HALF, TALL), slice(0, WIDE), fold(far[h * (HALF // 2):(h + 1) * (HALF // 2)])


def exchange_body(n_early, n_late, theta_ref, mean_ref, fact_ref, col_ref, late_own_ref, late_away_ref, gram_ref, proj_ref,
                  buf, tb, away, away_b, late_b, send_sem, recv_sem, lsend_sem, lrecv_sem, own_sem, put_sem, other_sem):
    part = lax.axis_index("part")
    other = 1 - part
    peer = (lax.axis_index("ens"), other, lax.axis_index("feat"))
    rows, width = theta_ref.shape[0], theta_ref.shape[1] // 2
    n_rows = col_ref.shape[0]
    cw = width // (n_early + n_late)
    n_blk = n_rows // BLK
    own_rows = pl.ds(pl.multiple_of(part * rows, BLK), rows)
    other_rows = pl.ds(pl.multiple_of(other * rows, BLK), rows)

    def chunk(half, c):
        return pl.ds(pl.multiple_of(half * width + c * cw, 128), cw)

    def remote(c):
        return pltpu.make_async_remote_copy(
            src_ref=theta_ref.at[:, chunk(other, c)], dst_ref=col_ref.at[own_rows, chunk(0, c)],
            send_sem=send_sem.at[c], recv_sem=recv_sem.at[c], device_id=peer, device_id_type=MESH)

    def remote_late(c):
        return pltpu.make_async_remote_copy(
            src_ref=away_b.at[c], dst_ref=late_b.at[c],
            send_sem=lsend_sem.at[c], recv_sem=lrecv_sem.at[c], device_id=peer, device_id_type=MESH)

    def fetch_own(c):
        return pltpu.make_async_copy(theta_ref.at[:, chunk(part, c)], buf.at[own_rows, :], own_sem)

    def put_own(c):
        return pltpu.make_async_copy(buf.at[own_rows, :], col_ref.at[own_rows, chunk(0, c)], put_sem)

    def put_late(c):
        return pltpu.make_async_copy(buf.at[own_rows, :], late_own_ref.at[:, chunk(0, c - n_early)], put_sem)

    def fetch_other(c):
        return pltpu.make_async_copy(col_ref.at[other_rows, chunk(0, c)], buf.at[other_rows, :], other_sem)

    def project(src, row0, half, c, dst_row0):
        x = src[pl.ds(pl.multiple_of(row0, BLK), BLK), :] - mean_ref[:, chunk(half, c)]
        proj_ref[:, pl.ds(pl.multiple_of(dst_row0, BLK), BLK)] += lax.dot_general(
            fact_ref[:, chunk(half, c)], x.astype(BF16), NT, preferred_element_type=F32)

    def add_gram():
        for b in range(n_blk):
            for h, rows_, cols_, piece in band_pieces(lambda at, n: tb[at:at + n, :], b, n_blk):
                gram_ref[b, h, rows_, cols_] += piece

    @pl.loop(0, n_early)
    def _(c):
        remote(c).start()

    gram_ref[...] = jnp.zeros_like(gram_ref)
    proj_ref[...] = jnp.zeros_like(proj_ref)

    @pl.loop(0, n_late)
    def _(c):
        fetch = pltpu.make_async_copy(theta_ref.at[:, chunk(other, n_early + c)], away, other_sem)
        fetch.start()
        fetch.wait()
        keep = pltpu.make_async_copy(away, late_away_ref.at[:, chunk(0, c)], own_sem)
        keep.start()

        @pl.loop(0, rows // BLK)
        def _(b):
            rs = pl.ds(pl.multiple_of(b * BLK, BLK), BLK)
            away_b[c, rs, :] = away[rs, :].astype(BF16)
            project(away, b * BLK, other, n_early + c, part * rows + b * BLK)

        keep.wait()

    @pl.loop(0, n_late)
    def _(c):
        remote_late(c).start()

    @pl.loop(0, n_early + n_late)
    def _(c):
        fetch_own(c).start()
        fetch_own(c).wait()

        @pl.when(c < n_early)
        def _():
            put_own(c).start()

        @pl.when(c >= n_early)
        def _():
            put_late(c).start()

        @pl.loop(0, rows // BLK)
        def _(b):
            row0 = part * rows + b * BLK
            rs = pl.ds(pl.multiple_of(row0, BLK), BLK)
            tb[rs, :] = buf[rs, :].astype(BF16)
            project(buf, row0, part, c, row0)

        @pl.when(c < n_early)
        def _():
            remote(c).wait_recv()
            fetch_other(c).start()
            fetch_other(c).wait()

            @pl.loop(0, rows // BLK)
            def _(b):
                row0 = other * rows + b * BLK
                rs = pl.ds(pl.multiple_of(row0, BLK), BLK)
                tb[rs, :] = buf[rs, :].astype(BF16)
                project(buf, row0, part, c, row0)

        @pl.when(c >= n_early)
        def _():
            remote_late(c - n_early).wait_recv()
            tb[other_rows, :] = late_b[c - n_early]

        add_gram()

        @pl.when(c < n_early)
        def _():
            put_own(c).wait()

        @pl.when(c >= n_early)
        def _():
            put_late(c).wait()

    @pl.loop(0, n_early)
    def _(c):
        remote(c).wait_send()

    @pl.loop(0, n_late)
    def _(c):
        remote_late(c).wait_send()


def columns(half, start, tile, refs):
    cols = pl.ds(pl.multiple_of(half * (refs[0].shape[1] // 2) + start, 128), tile)
    return tuple(ref[:, cols] for ref in refs)


def build_rhs(th, mean, prec, fact, zb_ref, rhs, rs):
    tile = th.shape[1]
    low = jnp.dot(zb_ref[rs, :], fact, preferred_element_type=F32)
    rhs[rs, :tile] = (-((th - mean) * prec + low)).astype(BF16)
    rhs[rs, tile:] = th.astype(BF16)


def stepped(th, acc, mass_ref, rs, inv_n, two_over_h, step_size):
    tile = th.shape[1]
    pull = mass_ref[rs, :] * th.astype(BF16).astype(F32) - acc[:, tile:]
    return th + step_size * ((acc[:, :tile] + two_over_h * pull) * inv_n)


def update_kernel(consts, first, split, has_before, *refs):
    n_in = 2 * (2 if split else 1)
    kern_hbm, mass_ref, zb_ref = refs[n_in:n_in + 3]
    params = refs[n_in + 3:n_in + 6]
    out_ref, tb_ref, proj_ref, rhs, kern_ref, kern_sem = refs[-6:]
    tile = out_ref.shape[1]
    big = out_ref.shape[0] // 2
    i = pl.program_id(0)
    slot = lax.rem(i, 2)
    part = lax.axis_index("part")

    def span(at, size):
        return pl.ds(pl.multiple_of(at, BLK), size)

    def order(h):
        return lax.rem(part + h, 2) if split else h

    def fetch(half):
        return pltpu.make_async_copy(kern_hbm.at[span(half * big, big), :], kern_ref.at[span(half * big, big), :], kern_sem.at[half])

    @pl.when(i == 0)
    def _():
        for h in range(2):
            fetch(order(h)).start()
        proj_ref[...] = refs[n_in + 6][...] if has_before else jnp.zeros_like(proj_ref)
        now = columns(part, first * tile, tile, params)
        if split:
            for ref, half in ((refs[0], part), (refs[2], 1 - part)):
                build_rhs(ref[...], *now, zb_ref, rhs.at[0], span(half * big, big))
        else:
            @pl.loop(0, 2)
            def _(b):
                rs = span(b * big, big)
                build_rhs(refs[0][rs, :], *now, zb_ref, rhs.at[0], rs)

    mean, _, fact = columns(part, (first + i) * tile, tile, params)
    after = columns(part, (first + jnp.minimum(i + 1, pl.num_programs(0) - 1)) * tile, tile, params)

    def half_step(ref, next_ref, src, half):
        rs = span(half * big, big)

        @pl.when(i == 0)
        def _():
            fetch(half).wait()

        acc = jnp.dot(kern_ref[rs, :], rhs[slot], preferred_element_type=F32)
        build_rhs(next_ref[src, :], *after, zb_ref, rhs.at[1 - slot], rs)
        new = stepped(ref[src, :], acc, mass_ref, rs, *consts)
        out_ref[rs, :] = new
        tb_ref[rs, :] = new.astype(BF16)
        proj_ref[:, rs] += lax.dot_general(fact, (new - mean).astype(BF16), NT, preferred_element_type=F32)

    if split:
        for at, half in ((0, part), (2, 1 - part)):
            half_step(refs[at], refs[at + 1], slice(None), half)
    else:
        @pl.loop(0, 2)
        def _(b):
            half_step(refs[0], refs[1], span(b * big, big), b)


def update(consts, theta, kern, mass, zb, params, width, start, stop, own_out, before=None):
    split = isinstance(theta, tuple)
    n_rows = kern.shape[0]
    rank = params[2].shape[0]
    first, steps = start // BLK, (stop - start) // BLK
    base = 0 if split else first
    held = n_rows // 2 if split else n_rows
    in_specs, args = [], []
    for arr in theta if split else (theta,):
        in_specs += [pl.BlockSpec((held, BLK), lambda i: (0, base + i)),
                     pl.BlockSpec((held, BLK), lambda i: (0, base + jnp.minimum(i + 1, steps - 1)))]
        args += [arr, arr]
    in_specs += [ANY] + [VMEM] * 5
    args += [kern, mass, zb, *params]
    alias = {}
    if before is not None:
        in_specs += [VMEM, ANY]
        args += [before[1], before[0]]
        alias = {len(args) - 1: 1}
        if len(before) > 2:
            in_specs.append(ANY)
            args.append(before[2])
            alias[len(args) - 1] = 0
    col = pl.BlockSpec((n_rows, BLK), lambda i: (0, first + i))
    return pl.pallas_call(
        functools.partial(update_kernel, consts, first, split, before is not None),
        grid=(steps,),
        out_shape=(jax.ShapeDtypeStruct((n_rows, stop - start if own_out else width), F32),
                   jax.ShapeDtypeStruct((n_rows, width), BF16),
                   jax.ShapeDtypeStruct((rank, n_rows), F32)),
        in_specs=in_specs,
        out_specs=(pl.BlockSpec((n_rows, BLK), lambda i: (0, i)) if own_out else col, col, VMEM),
        scratch_shapes=[pltpu.VMEM((2, n_rows, 2 * BLK), BF16), pltpu.VMEM(kern.shape, BF16), pltpu.SemaphoreType.DMA((2,))],
        input_output_aliases=alias,
        compiler_params=pltpu.CompilerParams(vmem_limit_bytes=VMEM_LIMIT),
        cost_estimate=pl.CostEstimate(flops=4 * n_rows * n_rows * (stop - start), bytes_accessed=10 * n_rows * (stop - start), transcendentals=0),
    )(*args)


def last_kernel(consts, start, pos_ref, theta_ref, kern_hbm, mass_ref, zb_ref, mean_ref, prec_ref, fact_ref, *rest):
    out_ref, send_ref, rhs, kern_ref, kern_sem = rest[-5:]

    def fetch(mine):
        rs = pl.ds(pl.multiple_of(lax.rem(1 - pos_ref[0] + mine, 2) * out_ref.shape[0], BLK), out_ref.shape[0])
        return pltpu.make_async_copy(kern_hbm.at[rs, :], kern_ref.at[rs, :], kern_sem.at[mine])

    fetch(0).start()
    fetch(1).start()
    rows = out_ref.shape[0]
    part = pos_ref[0]
    now = columns(part, start, theta_ref.shape[1], (mean_ref, prec_ref, fact_ref))

    @pl.loop(0, 2)
    def _(b):
        rs = pl.ds(pl.multiple_of(b * rows, BLK), rows)
        build_rhs(theta_ref[rs, :], *now, zb_ref, rhs, rs)

    size = BLK if theta_ref.shape[1] < BLK else HALF
    each = rows // size

    @pl.loop(0, 2 * each)
    def _(b):
        mine = b // each

        @pl.when(lax.rem(b, each) == 0)
        def _():
            fetch(mine).wait()

        at = pl.multiple_of(lax.rem(b, each) * size, size)
        rs = pl.ds(pl.multiple_of(lax.rem(1 - part + mine, 2) * rows + at, size), size)
        acc = jnp.dot(kern_ref[rs, :], rhs[...], preferred_element_type=F32)
        new = stepped(theta_ref[rs, :], acc, mass_ref, rs, *consts)

        @pl.when(mine == 0)
        def _():
            send_ref[pl.ds(at, size), :] = new

        @pl.when(mine == 1)
        def _():
            out_ref[pl.ds(at, size), :] = new


def last_update(consts, pos, theta, kern, mass, zb, mean, prec, fact_t, out, start, tile):
    n_rows, width = theta.shape
    chunk = start // tile
    rows, feat = n_rows // 2, width * 2
    per = width // tile
    col = lambda r: pl.BlockSpec((r, tile), lambda i, pos: (0, chunk))
    in_specs = [col(n_rows), ANY, VMEM, VMEM, VMEM, VMEM, VMEM]
    args = [theta, kern, mass, zb, mean, prec, fact_t]
    alias = {}
    if out is not None:
        in_specs.append(ANY)
        args.append(out)
        alias = {8: 0}
    return pl.pallas_call(
        functools.partial(last_kernel, consts, start),
        grid_spec=pltpu.PrefetchScalarGridSpec(
            num_scalar_prefetch=1, grid=(1,), in_specs=in_specs,
            out_specs=(pl.BlockSpec((rows, tile), lambda i, pos: (0, pos[0] * per + chunk)),
                       pl.BlockSpec((rows, tile), lambda i, pos: (0, 0))),
            scratch_shapes=[pltpu.VMEM((n_rows, 2 * tile), BF16), pltpu.VMEM(kern.shape, BF16), pltpu.SemaphoreType.DMA((2,))]),
        out_shape=(jax.ShapeDtypeStruct((rows, feat), F32), jax.ShapeDtypeStruct((rows, tile), F32)),
        input_output_aliases=alias,
        compiler_params=pltpu.CompilerParams(vmem_limit_bytes=VMEM_LIMIT),
        cost_estimate=pl.CostEstimate(flops=4 * n_rows * n_rows * tile, bytes_accessed=10 * n_rows * tile, transcendentals=0),
    )(pos, *args)


def own_kernel(consts, foreign, pos_ref, theta_ref, kern_ref, mass_ref, zb_ref, mean_ref, prec_ref, fact_ref, base_ref, out_ref, rhs):
    rows = out_ref.shape[0]
    half = 1 - pos_ref[0] if foreign else pos_ref[0]
    now = columns(half, pl.program_id(0) * BLK, BLK, (mean_ref, prec_ref, fact_ref))

    @pl.loop(0, theta_ref.shape[0] // BLK)
    def _(b):
        rs = pl.ds(pl.multiple_of(b * BLK, BLK), BLK)
        build_rhs(theta_ref[rs, :], *now, zb_ref, rhs, rs)

    @pl.loop(0, rows // BLK)
    def _(b):
        rs = pl.ds(pl.multiple_of(pos_ref[0] * rows + b * BLK, BLK), BLK)
        acc = jnp.dot(kern_ref[rs, :], rhs[...], preferred_element_type=F32)
        out_ref[pl.ds(pl.multiple_of(b * BLK, BLK), BLK), :] = stepped(theta_ref[rs, :], acc, mass_ref, rs, *consts)


def own_update(consts, pos, theta, kern, mass, zb, mean, prec, fact_t, out, foreign):
    n_rows, cols = theta.shape
    rows, feat = out.shape
    per = feat // (2 * BLK)
    col = lambda r: pl.BlockSpec((r, BLK), lambda i, pos: (0, i))
    where = (lambda i, pos: (0, (1 - pos[0]) * per + i)) if foreign else (lambda i, pos: (0, pos[0] * per + i))
    return pl.pallas_call(
        functools.partial(own_kernel, consts, foreign),
        grid_spec=pltpu.PrefetchScalarGridSpec(
            num_scalar_prefetch=1, grid=(cols // BLK,),
            in_specs=[col(n_rows), VMEM, VMEM, VMEM, VMEM, VMEM, VMEM, ANY],
            out_specs=pl.BlockSpec((rows, BLK), where),
            scratch_shapes=[pltpu.VMEM((n_rows, 2 * BLK), BF16)]),
        out_shape=jax.ShapeDtypeStruct(out.shape, F32),
        input_output_aliases={8: 0},
        compiler_params=pltpu.CompilerParams(vmem_limit_bytes=VMEM_LIMIT),
        cost_estimate=pl.CostEstimate(flops=4 * rows * n_rows * cols, bytes_accessed=10 * n_rows * cols, transcendentals=0),
        name="own_foreign" if foreign else "own_shared",
    )(pos, theta, kern, mass, zb, mean, prec, fact_t, out)


def place_kernel(pos_ref, recv_ref, base_ref, out_ref):
    out_ref[...] = recv_ref[...]


def place(pos, recv, out, start):
    rows, tile = recv.shape
    per = out.shape[1] // 256
    sub = tile // 128
    first = start // 128
    return pl.pallas_call(
        place_kernel,
        grid_spec=pltpu.PrefetchScalarGridSpec(
            num_scalar_prefetch=1, grid=(sub,), in_specs=[pl.BlockSpec((rows, 128), lambda i, pos: (0, i)), ANY],
            out_specs=pl.BlockSpec((rows, 128), lambda i, pos: (0, (1 - pos[0]) * per + first + i))),
        out_shape=jax.ShapeDtypeStruct(out.shape, out.dtype),
        input_output_aliases={2: 0},
        cost_estimate=pl.CostEstimate(flops=1000 * rows * tile, bytes_accessed=8 * rows * tile, transcendentals=0),
    )(pos, recv, out)


def greet(between=lambda: None):
    ens, part, feat = lax.axis_index("ens"), lax.axis_index("part"), lax.axis_index("feat")
    barrier = pltpu.get_barrier_semaphore()
    for i in range(1, 8):
        there = (ens, lax.rem(part + i // 4, 2), lax.rem(feat + i % 4, 4))
        pl.semaphore_signal(barrier, inc=1, device_id=there, device_id_type=MESH)
    between()
    pl.semaphore_wait(barrier, 7)


def kmat_body(from_gram, two_over_h, src_ref, proj_ref, kern_out, zb_ref, mass_ref, *scratch):
    if not from_gram:
        tb, load_sem = scratch[-2:]
    (gbuf, sib_in, r_x1, r_y1, r_x2, r_y2, sq_parts, sq, z_in, z_all, kbuf,
     sib_send, sib_recv, rs_send, rs_recv, sq_send, sq_recv, z_send, z_recv, zb_send, zb_recv,
     k_send, k_recv, _, kern_ref, kern_sem) = scratch[:26]
    n_rows = kern_ref.shape[0]
    n_blk = n_rows // BLK
    ens, part, feat = lax.axis_index("ens"), lax.axis_index("part"), lax.axis_index("feat")
    x, core = feat // 2, lax.rem(feat, 2)

    def chip(rel):
        return lax.rem(part + rel // 2, 2), lax.rem(x + rel % 2, 2)

    def block(rel, flip):
        cy, cx = chip(rel)
        return cy * 4 + cx * 2 + lax.rem(core + flip, 2)

    def device(rel, flip):
        cy, cx = chip(rel)
        return (ens, cy, cx * 2 + lax.rem(core + flip, 2))

    me = block(0, 0)
    sibling, dev_x, dev_y = device(0, 1), device(1, 0), device(2, 0)
    others = [(rel, flip) for rel in (3, 1, 2, 0) for flip in (0, 1) if (rel, flip) != (0, 0)]

    def rcopy(src, dst, ssem, rsem, dev):
        return pltpu.make_async_remote_copy(src_ref=src, dst_ref=dst, send_sem=ssem, recv_sem=rsem,
                                            device_id=dev, device_id_type=MESH)

    cy_far, cx_far = chip(3)
    first_band = cy_far * 4 + cx_far * 2 + 1 - core

    def load(n):
        b = lax.rem(first_band + n, n_blk)
        rs = pl.ds(pl.multiple_of(b * BLK, BLK), BLK)
        return pltpu.make_async_copy(src_ref.at[rs, :], tb.at[rs, :], load_sem.at[n])

    if not from_gram:
        def load_all():
            for b in range(n_blk):
                load(b).start()

        greet(load_all)

    def z_cols(b):
        return proj_ref.at[:, pl.ds(pl.multiple_of(b * BLK, BLK), BLK)]

    def z_copy(i):
        rel, flip = others[i]
        return rcopy(z_cols(block(rel, flip)), z_in.at[me], z_send.at[i], z_recv.at[me], device(rel, flip))

    for i in range(len(others)):
        z_copy(i).start()
    z_own = pltpu.make_async_copy(z_cols(me), z_in.at[me], z_recv.at[me])
    z_own.start()

    def sib_copy(rel):
        src = src_ref.at[block(rel, 1)] if from_gram else gbuf.at[4 + rel]
        return rcopy(src, sib_in.at[rel], sib_send.at[rel], sib_recv.at[rel], sibling)

    lo, hi = 0, 1
    rs_copies = {
        "d_lo": rcopy(gbuf.at[3, lo], r_x1.at[0], rs_send.at[0], rs_recv.at[0], dev_x),
        "d_hi": rcopy(gbuf.at[3, hi], r_y1.at[0], rs_send.at[1], rs_recv.at[1], dev_y),
        "y_hi": rcopy(gbuf.at[2, hi], r_y1.at[1], rs_send.at[2], rs_recv.at[2], dev_y),
        "x_lo": rcopy(gbuf.at[1, lo], r_x1.at[1], rs_send.at[3], rs_recv.at[3], dev_x),
        "y_lo": rcopy(gbuf.at[2, lo], r_y2, rs_send.at[4], rs_recv.at[4], dev_y),
        "x_hi": rcopy(gbuf.at[1, hi], r_x2, rs_send.at[5], rs_recv.at[5], dev_x),
    }
    eye = (lax.broadcasted_iota(jnp.int32, (HALF, HALF), 0) == lax.broadcasted_iota(jnp.int32, (HALF, HALF), 1)).astype(F32)

    def merge(rel):
        sib_copy(rel).wait_recv()
        gbuf[rel] = src_ref[block(rel, 0)] + sib_in[rel]

    def first_sends(rel):
        for name in {3: ("d_lo", "d_hi"), 2: ("y_hi",), 1: ("x_lo",), 0: ()}[rel]:
            rs_copies[name].start()

    if from_gram:
        for rel in (3, 2, 1, 0):
            sib_copy(rel).start()
        for rel in (3, 2, 1, 0):
            merge(rel)
            first_sends(rel)
    else:
        def rows_at(at, n):
            return tb[pl.ds(pl.multiple_of(at, HALF), n), :]

        for h, rows_, cols_, piece in band_pieces(rows_at, first_band, n_blk, lambda n: load(n).wait()):
            gbuf[7, h, rows_, cols_] = piece
        sib_copy(3).start()

        @pl.loop(1, 8)
        def _(i):
            rel, own = 3 - i // 2, lax.rem(i, 2)
            cy, cx = lax.rem(part + rel // 2, 2), lax.rem(x + lax.rem(rel, 2), 2)
            b = cy * 4 + cx * 2 + lax.rem(core + 1 - own, 2)
            dst = rel + 4 * (1 - own)
            for h, rows_, cols_, piece in band_pieces(rows_at, b, n_blk):
                gbuf[dst, h, rows_, cols_] = piece
            across = rcopy(gbuf.at[4 + rel], sib_in.at[rel], sib_send.at[rel], sib_recv.at[rel], sibling)

            @pl.when(own == 0)
            def _():
                across.start()

            @pl.when(own == 1)
            def _():
                across.wait_recv()
                gbuf[rel] += sib_in[rel]
                for r in (3, 2, 1):
                    @pl.when(rel == r)
                    def _():
                        first_sends(r)

    for rel in range(4):
        cy, cx = chip(rel)
        for h in range(2):
            sq_parts[me, cy * 2 + cx, :, h * HALF:(h + 1) * HALF] = jnp.sum(gbuf[rel, h, :HALF, :HALF] * eye, axis=0, keepdims=True)

    def sq_copy(i):
        rel, flip = others[i]
        return rcopy(sq_parts.at[me], sq_parts.at[me], sq_send.at[i], sq_recv.at[me], device(rel, flip))

    def recv_from(buf, sem, rel, flip):
        b = block(rel, flip)
        return rcopy(buf.at[b], buf.at[b], sq_send.at[0], sem.at[b], sibling)

    for i in range(len(others)):
        sq_copy(i).start()

    rs_copies["d_lo"].wait_recv()
    gbuf[2, 0] += r_x1[0]
    rs_copies["y_lo"].start()
    rs_copies["d_hi"].wait_recv()
    gbuf[1, 1] += r_y1[0]
    rs_copies["x_hi"].start()

    z_own.wait()
    for rel, flip in others:
        recv_from(z_in, z_recv, rel, flip).wait_recv()
    z_sum = z_in[0]
    for b in range(1, n_blk):
        z_sum = z_sum + z_in[b]
    z_all[me] = z_sum.astype(BF16)

    def zb_copy(i):
        rel, flip = others[i]
        return rcopy(z_all.at[me], z_all.at[me], zb_send.at[i], zb_recv.at[me], device(rel, flip))

    for i in range(len(others)):
        zb_copy(i).start()
    for rel, flip in others:
        recv_from(sq_parts, sq_recv, rel, flip).wait_recv()
    for c in range(2):
        for q in range(4):
            s = sq_parts[c, q] + sq_parts[2 + c, q] + sq_parts[4 + c, q] + sq_parts[6 + c, q]
            b = 2 * q + c
            sq[:, b * BLK:(b + 1) * BLK] = s
            if b < WIDE // BLK:
                sq[:, n_rows + b * BLK:n_rows + (b + 1) * BLK] = s

    def sq_at(at, n):
        return sq[:, pl.ds(pl.multiple_of(at * HALF, HALF), n)]

    def upright(row):
        return jnp.sum(eye * row, axis=1, keepdims=True)

    def kernel_of(gram, col, row):
        return jnp.exp(-jnp.maximum(col + row - 2.0 * gram, 0.0) * (0.5 * two_over_h))

    def make_band(h, gram):
        idx = 2 * me + h
        row = sq_at(idx, WIDE)
        kbuf[idx, :HALF, :] = kernel_of(gram[:HALF], upright(row[:, :HALF]), row).astype(BF16)
        col = upright(sq_at(me, HALF))[h * (HALF // 2):(h + 1) * (HALF // 2)]
        kbuf[idx, HALF:, :] = fold(kernel_of(unfold(gram[HALF:]), col, sq_at(me + n_blk, HALF))).astype(BF16)

    slots = iter(range(14))
    sent = []

    def send_band(idx, dev):
        s = next(slots)
        cp = rcopy(kbuf.at[idx], kbuf.at[idx], k_send.at[s], k_recv.at[idx], dev)
        cp.start()
        sent.append(cp)

    def wait_band(idx):
        rcopy(kbuf.at[idx], kbuf.at[idx], k_send.at[0], k_recv.at[idx], sibling).wait_recv()

    def spread(b, h, unroll=False):
        idx = 2 * b + h
        row0 = pl.multiple_of(idx * HALF, HALF)
        kern_ref[pl.ds(row0, HALF), pl.ds(row0, HALF)] = kbuf[idx, :HALF, :HALF]

        def move(k):
            col0 = pl.multiple_of(lax.rem(idx + k, 2 * n_blk) * HALF, HALF)
            tile = kbuf[idx, :HALF, pl.ds(pl.multiple_of(k * HALF, HALF), HALF)]
            kern_ref[pl.ds(row0, HALF), pl.ds(col0, HALF)] = tile
            kern_ref[pl.ds(col0, HALF), pl.ds(row0, HALF)] = tile.T

        if unroll:
            for k in range(1, WIDE // HALF):
                move(k)
        else:
            pl.loop(1, WIDE // HALF)(move)

    def spread_far(b):
        tile = jnp.concatenate([unfold(kbuf[2 * b + h, HALF:, :].astype(F32)) for h in range(2)], axis=0)
        near = pl.ds(pl.multiple_of(b * HALF, HALF), HALF)
        away = pl.ds(pl.multiple_of((b + n_blk) * HALF, HALF), HALF)
        kern_ref[near, away] = tile.astype(BF16)
        kern_ref[away, near] = tile.T.astype(BF16)

    rs_copies["x_lo"].wait_recv()
    rs_copies["y_lo"].wait_recv()
    make_band(0, gbuf[0, 0] + (r_x1[1] + r_y2[...]))
    for dev in (dev_y, sibling):
        send_band(2 * me, dev)
    rs_copies["y_hi"].wait_recv()
    rs_copies["x_hi"].wait_recv()
    make_band(1, gbuf[0, 1] + (r_y1[1] + r_x2[...]))
    for dev in (dev_x, sibling):
        send_band(2 * me + 1, dev)
    send_band(2 * me, dev_x)
    send_band(2 * me + 1, dev_y)
    spread(me, 0)
    spread(me, 1)
    sib = block(0, 1)
    for h in range(2):
        wait_band(2 * sib + h)
        spread(sib, h)
    bx, by, bd = block(1, 0), block(2, 0), block(3, 0)
    wait_band(2 * by)
    send_band(2 * by, dev_x)
    send_band(2 * by, sibling)
    wait_band(2 * bx + 1)
    send_band(2 * bx + 1, dev_y)
    send_band(2 * bx + 1, sibling)
    spread(by, 0)
    spread(bx, 1)
    for b, h in ((bx, 0), (by, 1)):
        wait_band(2 * b + h)
        send_band(2 * b + h, sibling)
        spread(b, h)
    for rel, h in ((2, 0), (1, 1)):
        b = block(rel, 1)
        wait_band(2 * b + h)
        spread(b, h)
    for h in range(2):
        wait_band(2 * bd + h)
        send_band(2 * bd + h, sibling)
        spread(bd, h)
    for rel, h in ((1, 0), (2, 1)):
        b = block(rel, 1)
        wait_band(2 * b + h)
        spread(b, h)

    @pl.loop(0, 6)
    def _(i):
        rel = i // 2
        cy, cx = lax.rem(part + rel // 2, 2), lax.rem(x + lax.rem(rel, 2), 2)
        spread_far(cy * 4 + cx * 2 + lax.rem(i, 2))

    spread_far(bd)
    last = block(3, 1)
    for h in range(2):
        wait_band(2 * last + h)
        spread(last, h, True)
    spread_far(last)
    for rel, flip in others:
        recv_from(z_all, zb_recv, rel, flip).wait_recv()

    def put(b):
        rs = pl.ds(pl.multiple_of(b * BLK, BLK), BLK)
        return pltpu.make_async_copy(kern_ref.at[rs, :], kern_out.at[rs, :], kern_sem.at[b])

    @pl.loop(0, n_blk)
    def _(b):
        rs = pl.ds(pl.multiple_of(b * BLK, BLK), BLK)
        zb_ref[rs, :] = z_all[b].astype(F32).T.astype(BF16)
        mass_ref[rs, :] = jnp.sum(kern_ref[rs, :].astype(F32), axis=1, keepdims=True)
        put(b).start()

    @pl.loop(0, n_blk)
    def _(b):
        put(b).wait()

    for rel in range(4):
        sib_copy(rel).wait_send()
    for cp in rs_copies.values():
        cp.wait_send()
    for i in range(len(others)):
        z_copy(i).wait_send()
        sq_copy(i).wait_send()
        zb_copy(i).wait_send()
    for cp in sent:
        cp.wait_send()


def kmat_scratch(n_rows, rank, n_own):
    n_blk = n_rows // BLK
    dma = lambda *n: pltpu.SemaphoreType.DMA(n)
    return [
        pltpu.VMEM((n_own, 2, TALL, WIDE), F32), pltpu.VMEM((4, 2, TALL, WIDE), F32),
        pltpu.VMEM((2, TALL, WIDE), F32), pltpu.VMEM((2, TALL, WIDE), F32),
        pltpu.VMEM((TALL, WIDE), F32), pltpu.VMEM((TALL, WIDE), F32),
        pltpu.VMEM((8, 4, 1, BLK), F32), pltpu.VMEM((1, n_rows + WIDE), F32),
        pltpu.VMEM((n_blk, rank, BLK), F32), pltpu.VMEM((n_blk, rank, BLK), BF16),
        pltpu.VMEM((2 * n_blk, TALL, WIDE), BF16),
        dma(4), dma(4), dma(6), dma(6), dma(7), dma(8), dma(7), dma(8), dma(7), dma(8), dma(14), dma(16), dma(4),
        pltpu.VMEM((n_rows, n_rows), BF16), dma(n_blk)]


def kmat_shapes(n_rows, rank):
    return (jax.ShapeDtypeStruct((n_rows, n_rows), BF16), jax.ShapeDtypeStruct((n_rows, rank), BF16),
            jax.ShapeDtypeStruct((n_rows, 1), F32))


def kernel_matrix(tb, proj, two_over_h, collective_id):
    rank, n_rows = proj.shape
    return pl.pallas_call(
        functools.partial(kmat_body, False, two_over_h),
        out_shape=kmat_shapes(n_rows, rank), in_specs=[ANY, VMEM], out_specs=(ANY, VMEM, VMEM),
        scratch_shapes=kmat_scratch(n_rows, rank, 8) + [pltpu.VMEM(tb.shape, BF16), pltpu.SemaphoreType.DMA((n_rows // BLK,))],
        compiler_params=pltpu.CompilerParams(collective_id=collective_id, has_side_effects=True, vmem_limit_bytes=VMEM_LIMIT),
    )(tb, proj)


def opening_kernel(n_early, n_late, two_over_h, theta_ref, mean_ref, fact_ref, col_ref, late_own_ref, late_away_ref,
                   kern_out, zb_ref, mass_ref, gram, proj, *scratch):
    greet()
    exchange_body(n_early, n_late, theta_ref, mean_ref, fact_ref, col_ref, late_own_ref, late_away_ref, gram, proj, *scratch[:12])
    kmat_body(True, two_over_h, gram, proj, kern_out, zb_ref, mass_ref, *scratch[12:])


def opening(theta, mean, fact_t, two_over_h, n_early, n_late):
    rows, feat = theta.shape
    rank = fact_t.shape[0]
    width = feat // 2
    n_rows = rows * 2
    cw = width // (n_early + n_late)
    dma = lambda *n: pltpu.SemaphoreType.DMA(n)
    return pl.pallas_call(
        functools.partial(opening_kernel, n_early, n_late, two_over_h),
        out_shape=(jax.ShapeDtypeStruct((n_rows, n_early * cw), F32),
                   jax.ShapeDtypeStruct((rows, n_late * cw), F32),
                   jax.ShapeDtypeStruct((rows, n_late * cw), F32)) + kmat_shapes(n_rows, rank),
        in_specs=[ANY, VMEM, VMEM], out_specs=(ANY, ANY, ANY, ANY, VMEM, VMEM),
        scratch_shapes=[
            pltpu.VMEM((n_rows // BLK, 2, TALL, WIDE), F32), pltpu.VMEM((rank, n_rows), F32),
            pltpu.VMEM((n_rows, cw), F32), pltpu.VMEM((n_rows, cw), BF16), pltpu.VMEM((rows, cw), F32),
            pltpu.VMEM((n_late, rows, cw), BF16), pltpu.VMEM((n_late, rows, cw), BF16),
            dma(n_early), dma(n_early), dma(n_late), dma(n_late),
            pltpu.SemaphoreType.DMA, pltpu.SemaphoreType.DMA, pltpu.SemaphoreType.DMA] + kmat_scratch(n_rows, rank, 4),
        compiler_params=pltpu.CompilerParams(collective_id=0, has_side_effects=True, vmem_limit_bytes=VMEM_LIMIT),
        name="opening",
    )(theta, mean, fact_t)


def solution(mesh):
    part_size = mesh.shape["part"]
    feat_size = mesh.shape["feat"]

    def local_steps(theta, prec_loc, mean_loc, factor_loc):
        rows, feat_loc = theta.shape
        n_total = rows * part_size
        feat_total = feat_loc * feat_size
        width = feat_loc // part_size
        kern_width = 2.0 * feat_total / math.log(n_total)
        step_size = 0.15 * n_total * feat_total / math.log(n_total)
        consts = (1.0 / n_total, 2.0 / kern_width, step_size)
        part = lax.axis_index("part")
        pos = part.astype(jnp.int32).reshape(1)
        params = (mean_loc.reshape(1, feat_loc), prec_loc.reshape(1, feat_loc), factor_loc.T)
        shared = 2 * BLK
        chunks = [(shared, HALF)] + [(at, 2 * BLK) for at in range(2 * shared, width, 2 * BLK)] + [(shared + BLK, BLK), (shared + HALF, HALF)]
        swap = [(0, 1), (1, 0)]
        late = 3 * BLK
        early = width - late

        cur, late_own, late_away, kern, zb, mass = opening(theta, params[0], params[2], consts[1], early // BLK, late // BLK)
        recv = lax.ppermute(late_away, "part", swap)
        new, tb, proj = update(consts, cur, kern, mass, zb, params, width, 0, early, False)
        cur, tb, proj = update(consts, (late_own, recv), kern, mass, zb, params, width, early, width, False, (tb, proj, new))
        kern, zb, mass = kernel_matrix(tb, proj, consts[1], 2)
        both, tb, proj = update(consts, cur, kern, mass, zb, params, width, 0, shared, True)
        foreign = lax.ppermute(both, "part", swap)
        cur, tb, proj = update(consts, cur, kern, mass, zb, params, width, shared, width, False, (tb, proj))
        kern, zb, mass = kernel_matrix(tb, proj, consts[1], 3)
        out = None
        received = []
        for start, tile in chunks:
            out, send = last_update(consts, pos, cur, kern, mass, zb, *params, out, start, tile)
            received.append(lax.ppermute(send, "part", swap))
        out = own_update(consts, pos, both, kern, mass, zb, *params, out, False)
        out = own_update(consts, pos, foreign, kern, mass, zb, *params, out, True)
        for (start, tile), recv in zip(chunks, received):
            out = place(pos, recv, out, start)
        return out

    row_spec = P(("ens", "part"), "feat")
    vec_spec = P(("ens", "feat"))
    fac_spec = P(("ens", "feat"), None)
    return jax.shard_map(local_steps, mesh=mesh, in_specs=(row_spec, vec_spec, vec_spec, fac_spec), out_specs=row_spec, check_vma=False)
```

```python
import functools
import math
import jax
import jax.numpy as jnp
from jax import lax
from jax.experimental import pallas as pl
from jax.experimental.pallas import tpu as pltpu
from jax.sharding import PartitionSpec as P

BLK = 256
HALF = BLK // 2
WIDE = 8 * HALF
TALL = HALF + 8
MESH = pl.DeviceIdType.MESH
F32 = jnp.float32
BF16 = jnp.bfloat16
ANY = pl.BlockSpec(memory_space=pl.ANY)
VMEM = pl.BlockSpec(memory_space=pltpu.VMEM)
VMEM_LIMIT = 63 * 1024 * 1024
NT = (((1,), (1,)), ((), ()))


def fold(tile):
    return jnp.concatenate([tile[8 * g:8 * g + 8] for g in range(8)], axis=1)


def unfold(rows):
    return jnp.concatenate([rows[:, HALF * g:HALF * (g + 1)] for g in range(8)], axis=0)


def band_pieces(rows_at, b, n_blk):
    def dot(left, right):
        return lax.dot_general(left, right, NT, preferred_element_type=F32)

    def wrap(j):
        return j % n_blk if isinstance(j, int) else lax.rem(j, n_blk)

    main = slice(0, HALF)
    both = rows_at(b * BLK, BLK)
    for k in range(4):
        val = dot(both, rows_at(wrap(b + k) * BLK, BLK))
        yield 0, main, slice(k * BLK, (k + 1) * BLK), val[:HALF]
        if k == 0:
            yield 1, main, slice(0, HALF), val[HALF:, HALF:]
        else:
            yield 1, main, slice(k * BLK - HALF, k * BLK + HALF), val[HALF:]
    yield 1, main, slice(WIDE - HALF, WIDE), dot(rows_at(b * BLK + HALF, HALF), rows_at(wrap(b + 4) * BLK, HALF))
    far = dot(rows_at(b * HALF, HALF), rows_at((b + n_blk) * HALF, HALF))
    for h in range(2):
        yield h, slice(HALF, TALL), slice(0, WIDE), fold(far[h * (HALF // 2):(h + 1) * (HALF // 2)])


def exchange_body(n_early, n_late, theta_ref, mean_ref, fact_ref, col_ref, late_own_ref, late_away_ref, gram_ref, proj_ref,
                  buf, tb, away, away_b, late_b, send_sem, recv_sem, lsend_sem, lrecv_sem, own_sem, put_sem, other_sem):
    part = lax.axis_index("part")
    other = 1 - part
    peer = (lax.axis_index("ens"), other, lax.axis_index("feat"))
    rows, width = theta_ref.shape[0], theta_ref.shape[1] // 2
    n_rows = col_ref.shape[0]
    cw = width // (n_early + n_late)
    n_blk = n_rows // BLK
    own_rows = pl.ds(pl.multiple_of(part * rows, BLK), rows)
    other_rows = pl.ds(pl.multiple_of(other * rows, BLK), rows)

    def chunk(half, c):
        return pl.ds(pl.multiple_of(half * width + c * cw, 128), cw)

    def remote(c):
        return pltpu.make_async_remote_copy(
            src_ref=theta_ref.at[:, chunk(other, c)], dst_ref=col_ref.at[own_rows, chunk(0, c)],
            send_sem=send_sem.at[c], recv_sem=recv_sem.at[c], device_id=peer, device_id_type=MESH)

    def remote_late(c):
        return pltpu.make_async_remote_copy(
            src_ref=away_b.at[c], dst_ref=late_b.at[c],
            send_sem=lsend_sem.at[c], recv_sem=lrecv_sem.at[c], device_id=peer, device_id_type=MESH)

    def fetch_own(c):
        return pltpu.make_async_copy(theta_ref.at[:, chunk(part, c)], buf.at[own_rows, :], own_sem)

    def put_own(c):
        return pltpu.make_async_copy(buf.at[own_rows, :], col_ref.at[own_rows, chunk(0, c)], put_sem)

    def put_late(c):
        return pltpu.make_async_copy(buf.at[own_rows, :], late_own_ref.at[:, chunk(0, c - n_early)], put_sem)

    def fetch_other(c):
        return pltpu.make_async_copy(col_ref.at[other_rows, chunk(0, c)], buf.at[other_rows, :], other_sem)

    def project(src, row0, half, c, dst_row0):
        x = src[pl.ds(pl.multiple_of(row0, BLK), BLK), :] - mean_ref[:, chunk(half, c)]
        proj_ref[:, pl.ds(pl.multiple_of(dst_row0, BLK), BLK)] += lax.dot_general(
            fact_ref[:, chunk(half, c)], x.astype(BF16), NT, preferred_element_type=F32)

    def add_gram():
        for b in range(n_blk):
            for h, rows_, cols_, piece in band_pieces(lambda at, n: tb[at:at + n, :], b, n_blk):
                gram_ref[b, h, rows_, cols_] += piece

    @pl.loop(0, n_early)
    def _(c):
        remote(c).start()

    gram_ref[...] = jnp.zeros_like(gram_ref)
    proj_ref[...] = jnp.zeros_like(proj_ref)

    @pl.loop(0, n_late)
    def _(c):
        fetch = pltpu.make_async_copy(theta_ref.at[:, chunk(other, n_early + c)], away, other_sem)
        fetch.start()
        fetch.wait()
        keep = pltpu.make_async_copy(away, late_away_ref.at[:, chunk(0, c)], own_sem)
        keep.start()

        @pl.loop(0, rows // BLK)
        def _(b):
            rs = pl.ds(pl.multiple_of(b * BLK, BLK), BLK)
            away_b[c, rs, :] = away[rs, :].astype(BF16)
            project(away, b * BLK, other, n_early + c, part * rows + b * BLK)

        keep.wait()

    @pl.loop(0, n_late)
    def _(c):
        remote_late(c).start()

    @pl.loop(0, n_early + n_late)
    def _(c):
        fetch_own(c).start()
        fetch_own(c).wait()

        @pl.when(c < n_early)
        def _():
            put_own(c).start()

        @pl.when(c >= n_early)
        def _():
            put_late(c).start()

        @pl.loop(0, rows // BLK)
        def _(b):
            row0 = part * rows + b * BLK
            rs = pl.ds(pl.multiple_of(row0, BLK), BLK)
            tb[rs, :] = buf[rs, :].astype(BF16)
            project(buf, row0, part, c, row0)

        @pl.when(c < n_early)
        def _():
            remote(c).wait_recv()
            fetch_other(c).start()
            fetch_other(c).wait()

            @pl.loop(0, rows // BLK)
            def _(b):
                row0 = other * rows + b * BLK
                rs = pl.ds(pl.multiple_of(row0, BLK), BLK)
                tb[rs, :] = buf[rs, :].astype(BF16)
                project(buf, row0, part, c, row0)

        @pl.when(c >= n_early)
        def _():
            remote_late(c - n_early).wait_recv()
            tb[other_rows, :] = late_b[c - n_early]

        add_gram()

        @pl.when(c < n_early)
        def _():
            put_own(c).wait()

        @pl.when(c >= n_early)
        def _():
            put_late(c).wait()

    @pl.loop(0, n_early)
    def _(c):
        remote(c).wait_send()

    @pl.loop(0, n_late)
    def _(c):
        remote_late(c).wait_send()


def columns(half, start, tile, refs):
    cols = pl.ds(pl.multiple_of(half * (refs[0].shape[1] // 2) + start, 128), tile)
    return tuple(ref[:, cols] for ref in refs)


def build_rhs(th, mean, prec, fact, zb_ref, rhs, rs):
    tile = th.shape[1]
    low = jnp.dot(zb_ref[rs, :], fact, preferred_element_type=F32)
    rhs[rs, :tile] = (-((th - mean) * prec + low)).astype(BF16)
    rhs[rs, tile:] = th.astype(BF16)


def stepped(th, acc, mass_ref, rs, inv_n, two_over_h, step_size):
    tile = th.shape[1]
    pull = mass_ref[rs, :] * th.astype(BF16).astype(F32) - acc[:, tile:]
    return th + step_size * ((acc[:, :tile] + two_over_h * pull) * inv_n)


def update_kernel(consts, first, split, has_before, *refs):
    n_in = 2 * (2 if split else 1)
    kern_hbm, mass_ref, zb_ref = refs[n_in:n_in + 3]
    params = refs[n_in + 3:n_in + 6]
    out_ref, tb_ref, proj_ref, rhs, kern_ref, kern_sem = refs[-6:]
    tile = out_ref.shape[1]
    big = out_ref.shape[0] // 2
    i = pl.program_id(0)
    slot = lax.rem(i, 2)
    part = lax.axis_index("part")

    def span(at, size):
        return pl.ds(pl.multiple_of(at, BLK), size)

    def order(h):
        return lax.rem(part + h, 2) if split else h

    def fetch(half):
        return pltpu.make_async_copy(kern_hbm.at[span(half * big, big), :], kern_ref.at[span(half * big, big), :], kern_sem.at[half])

    @pl.when(i == 0)
    def _():
        for h in range(2):
            fetch(order(h)).start()
        proj_ref[...] = refs[n_in + 6][...] if has_before else jnp.zeros_like(proj_ref)
        now = columns(part, first * tile, tile, params)
        if split:
            for ref, half in ((refs[0], part), (refs[2], 1 - part)):
                build_rhs(ref[...], *now, zb_ref, rhs.at[0], span(half * big, big))
        else:
            @pl.loop(0, 2)
            def _(b):
                rs = span(b * big, big)
                build_rhs(refs[0][rs, :], *now, zb_ref, rhs.at[0], rs)

    mean, _, fact = columns(part, (first + i) * tile, tile, params)
    after = columns(part, (first + jnp.minimum(i + 1, pl.num_programs(0) - 1)) * tile, tile, params)

    def half_step(ref, next_ref, src, half):
        rs = span(half * big, big)

        @pl.when(i == 0)
        def _():
            fetch(half).wait()

        acc = jnp.dot(kern_ref[rs, :], rhs[slot], preferred_element_type=F32)
        build_rhs(next_ref[src, :], *after, zb_ref, rhs.at[1 - slot], rs)
        new = stepped(ref[src, :], acc, mass_ref, rs, *consts)
        out_ref[rs, :] = new
        tb_ref[rs, :] = new.astype(BF16)
        proj_ref[:, rs] += lax.dot_general(fact, (new - mean).astype(BF16), NT, preferred_element_type=F32)

    if split:
        for at, half in ((0, part), (2, 1 - part)):
            half_step(refs[at], refs[at + 1], slice(None), half)
    else:
        @pl.loop(0, 2)
        def _(b):
            half_step(refs[0], refs[1], span(b * big, big), b)


def update(consts, theta, kern, mass, zb, params, width, start, stop, own_out, before=None):
    split = isinstance(theta, tuple)
    n_rows = kern.shape[0]
    rank = params[2].shape[0]
    first, steps = start // BLK, (stop - start) // BLK
    base = 0 if split else first
    held = n_rows // 2 if split else n_rows
    in_specs, args = [], []
    for arr in theta if split else (theta,):
        in_specs += [pl.BlockSpec((held, BLK), lambda i: (0, base + i)),
                     pl.BlockSpec((held, BLK), lambda i: (0, base + jnp.minimum(i + 1, steps - 1)))]
        args += [arr, arr]
    in_specs += [ANY] + [VMEM] * 5
    args += [kern, mass, zb, *params]
    alias = {}
    if before is not None:
        in_specs += [VMEM, ANY]
        args += [before[1], before[0]]
        alias = {len(args) - 1: 1}
        if len(before) > 2:
            in_specs.append(ANY)
            args.append(before[2])
            alias[len(args) - 1] = 0
    col = pl.BlockSpec((n_rows, BLK), lambda i: (0, first + i))
    return pl.pallas_call(
        functools.partial(update_kernel, consts, first, split, before is not None),
        grid=(steps,),
        out_shape=(jax.ShapeDtypeStruct((n_rows, stop - start if own_out else width), F32),
                   jax.ShapeDtypeStruct((n_rows, width), BF16),
                   jax.ShapeDtypeStruct((rank, n_rows), F32)),
        in_specs=in_specs,
        out_specs=(pl.BlockSpec((n_rows, BLK), lambda i: (0, i)) if own_out else col, col, VMEM),
        scratch_shapes=[pltpu.VMEM((2, n_rows, 2 * BLK), BF16), pltpu.VMEM(kern.shape, BF16), pltpu.SemaphoreType.DMA((2,))],
        input_output_aliases=alias,
        compiler_params=pltpu.CompilerParams(vmem_limit_bytes=VMEM_LIMIT),
        cost_estimate=pl.CostEstimate(flops=4 * n_rows * n_rows * (stop - start), bytes_accessed=10 * n_rows * (stop - start), transcendentals=0),
    )(*args)


def last_kernel(consts, start, pos_ref, theta_ref, kern_hbm, mass_ref, zb_ref, mean_ref, prec_ref, fact_ref, *rest):
    out_ref, send_ref, rhs, kern_ref, kern_sem = rest[-5:]

    def fetch(mine):
        rs = pl.ds(pl.multiple_of(lax.rem(1 - pos_ref[0] + mine, 2) * out_ref.shape[0], BLK), out_ref.shape[0])
        return pltpu.make_async_copy(kern_hbm.at[rs, :], kern_ref.at[rs, :], kern_sem.at[mine])

    fetch(0).start()
    fetch(1).start()
    rows = out_ref.shape[0]
    part = pos_ref[0]
    now = columns(part, start, theta_ref.shape[1], (mean_ref, prec_ref, fact_ref))

    @pl.loop(0, 2)
    def _(b):
        rs = pl.ds(pl.multiple_of(b * rows, BLK), rows)
        build_rhs(theta_ref[rs, :], *now, zb_ref, rhs, rs)

    size = BLK if theta_ref.shape[1] < BLK else HALF
    each = rows // size

    @pl.loop(0, 2 * each)
    def _(b):
        mine = b // each

        @pl.when(lax.rem(b, each) == 0)
        def _():
            fetch(mine).wait()

        at = pl.multiple_of(lax.rem(b, each) * size, size)
        rs = pl.ds(pl.multiple_of(lax.rem(1 - part + mine, 2) * rows + at, size), size)
        acc = jnp.dot(kern_ref[rs, :], rhs[...], preferred_element_type=F32)
        new = stepped(theta_ref[rs, :], acc, mass_ref, rs, *consts)

        @pl.when(mine == 0)
        def _():
            send_ref[pl.ds(at, size), :] = new

        @pl.when(mine == 1)
        def _():
            out_ref[pl.ds(at, size), :] = new


def last_update(consts, pos, theta, kern, mass, zb, mean, prec, fact_t, out, start, tile):
    n_rows, width = theta.shape
    chunk = start // tile
    rows, feat = n_rows // 2, width * 2
    per = width // tile
    col = lambda r: pl.BlockSpec((r, tile), lambda i, pos: (0, chunk))
    in_specs = [col(n_rows), ANY, VMEM, VMEM, VMEM, VMEM, VMEM]
    args = [theta, kern, mass, zb, mean, prec, fact_t]
    alias = {}
    if out is not None:
        in_specs.append(ANY)
        args.append(out)
        alias = {8: 0}
    return pl.pallas_call(
        functools.partial(last_kernel, consts, start),
        grid_spec=pltpu.PrefetchScalarGridSpec(
            num_scalar_prefetch=1, grid=(1,), in_specs=in_specs,
            out_specs=(pl.BlockSpec((rows, tile), lambda i, pos: (0, pos[0] * per + chunk)),
                       pl.BlockSpec((rows, tile), lambda i, pos: (0, 0))),
            scratch_shapes=[pltpu.VMEM((n_rows, 2 * tile), BF16), pltpu.VMEM(kern.shape, BF16), pltpu.SemaphoreType.DMA((2,))]),
        out_shape=(jax.ShapeDtypeStruct((rows, feat), F32), jax.ShapeDtypeStruct((rows, tile), F32)),
        input_output_aliases=alias,
        compiler_params=pltpu.CompilerParams(vmem_limit_bytes=VMEM_LIMIT),
        cost_estimate=pl.CostEstimate(flops=4 * n_rows * n_rows * tile, bytes_accessed=10 * n_rows * tile, transcendentals=0),
    )(pos, *args)


def send_kernel(consts, start, pos_ref, theta_ref, kern_hbm, mass_ref, zb_ref, mean_ref, prec_ref, fact_ref, send_ref, rhs, kern_ref, kern_sem):
    rows = send_ref.shape[0]
    theirs = pl.ds(pl.multiple_of((1 - pos_ref[0]) * rows, BLK), rows)
    fetch = pltpu.make_async_copy(kern_hbm.at[theirs, :], kern_ref, kern_sem)
    fetch.start()
    now = columns(pos_ref[0], start, theta_ref.shape[1], (mean_ref, prec_ref, fact_ref))

    @pl.loop(0, 2)
    def _(b):
        rs = pl.ds(pl.multiple_of(b * rows, BLK), rows)
        build_rhs(theta_ref[rs, :], *now, zb_ref, rhs, rs)

    fetch.wait()

    @pl.loop(0, rows // BLK)
    def _(b):
        at = pl.ds(pl.multiple_of(b * BLK, BLK), BLK)
        rs = pl.ds(pl.multiple_of((1 - pos_ref[0]) * rows + b * BLK, BLK), BLK)
        acc = jnp.dot(kern_ref[at, :], rhs[...], preferred_element_type=F32)
        send_ref[at, :] = stepped(theta_ref[rs, :], acc, mass_ref, rs, *consts)


def send_update(consts, pos, theta, kern, mass, zb, mean, prec, fact_t, start, tile):
    n_rows = theta.shape[0]
    rows = n_rows // 2
    return pl.pallas_call(
        functools.partial(send_kernel, consts, start),
        grid_spec=pltpu.PrefetchScalarGridSpec(
            num_scalar_prefetch=1, grid=(1,),
            in_specs=[pl.BlockSpec((n_rows, tile), lambda i, pos: (0, start // tile)), ANY] + [VMEM] * 5,
            out_specs=pl.BlockSpec((rows, tile), lambda i, pos: (0, 0)),
            scratch_shapes=[pltpu.VMEM((n_rows, 2 * tile), BF16), pltpu.VMEM((rows, n_rows), BF16), pltpu.SemaphoreType.DMA]),
        out_shape=jax.ShapeDtypeStruct((rows, tile), F32),
        compiler_params=pltpu.CompilerParams(vmem_limit_bytes=VMEM_LIMIT),
        cost_estimate=pl.CostEstimate(flops=4 * n_rows * rows * tile, bytes_accessed=10 * n_rows * tile, transcendentals=0),
        name="send_first",
    )(pos, theta, kern, mass, zb, mean, prec, fact_t)


def own_kernel(consts, foreign, start, pos_ref, theta_ref, kern_ref, mass_ref, zb_ref, mean_ref, prec_ref, fact_ref, base_ref, out_ref, rhs):
    rows = out_ref.shape[0]
    half = 1 - pos_ref[0] if foreign else pos_ref[0]
    tile = theta_ref.shape[1]
    now = columns(half, start + pl.program_id(0) * tile, tile, (mean_ref, prec_ref, fact_ref))

    @pl.loop(0, theta_ref.shape[0] // BLK)
    def _(b):
        rs = pl.ds(pl.multiple_of(b * BLK, BLK), BLK)
        build_rhs(theta_ref[rs, :], *now, zb_ref, rhs, rs)

    @pl.loop(0, rows // BLK)
    def _(b):
        rs = pl.ds(pl.multiple_of(pos_ref[0] * rows + b * BLK, BLK), BLK)
        acc = jnp.dot(kern_ref[rs, :], rhs[...], preferred_element_type=F32)
        out_ref[pl.ds(pl.multiple_of(b * BLK, BLK), BLK), :] = stepped(theta_ref[rs, :], acc, mass_ref, rs, *consts)


def own_update(consts, pos, theta, kern, mass, zb, mean, prec, fact_t, out, foreign, start, cols, tile):
    n_rows = theta.shape[0]
    first = start // tile
    rows, feat = out.shape
    per = feat // (2 * tile)
    col = lambda r: pl.BlockSpec((r, tile), lambda i, pos: (0, first + i))
    where = (lambda i, pos: (0, (1 - pos[0]) * per + first + i)) if foreign else (lambda i, pos: (0, pos[0] * per + first + i))
    return pl.pallas_call(
        functools.partial(own_kernel, consts, foreign, start),
        grid_spec=pltpu.PrefetchScalarGridSpec(
            num_scalar_prefetch=1, grid=(cols // tile,),
            in_specs=[col(n_rows), VMEM, VMEM, VMEM, VMEM, VMEM, VMEM, ANY],
            out_specs=pl.BlockSpec((rows, tile), where),
            scratch_shapes=[pltpu.VMEM((n_rows, 2 * tile), BF16)]),
        out_shape=jax.ShapeDtypeStruct(out.shape, F32),
        input_output_aliases={8: 0},
        compiler_params=pltpu.CompilerParams(vmem_limit_bytes=VMEM_LIMIT),
        cost_estimate=pl.CostEstimate(flops=4 * rows * n_rows * cols, bytes_accessed=10 * n_rows * cols, transcendentals=0),
    )(pos, theta, kern, mass, zb, mean, prec, fact_t, out)


def place_kernel(pos_ref, recv_ref, base_ref, out_ref):
    out_ref[...] = recv_ref[...]


def place(pos, recv, out, start):
    rows, tile = recv.shape
    per = out.shape[1] // 256
    sub = tile // 128
    first = start // 128
    return pl.pallas_call(
        place_kernel,
        grid_spec=pltpu.PrefetchScalarGridSpec(
            num_scalar_prefetch=1, grid=(sub,), in_specs=[pl.BlockSpec((rows, 128), lambda i, pos: (0, i)), ANY],
            out_specs=pl.BlockSpec((rows, 128), lambda i, pos: (0, (1 - pos[0]) * per + first + i))),
        out_shape=jax.ShapeDtypeStruct(out.shape, out.dtype),
        input_output_aliases={2: 0},
        cost_estimate=pl.CostEstimate(flops=1000 * rows * tile, bytes_accessed=8 * rows * tile, transcendentals=0),
    )(pos, recv, out)


def greet(between=lambda: None):
    ens, part, feat = lax.axis_index("ens"), lax.axis_index("part"), lax.axis_index("feat")
    barrier = pltpu.get_barrier_semaphore()
    for i in range(1, 8):
        there = (ens, lax.rem(part + i // 4, 2), lax.rem(feat + i % 4, 4))
        pl.semaphore_signal(barrier, inc=1, device_id=there, device_id_type=MESH)
    between()
    pl.semaphore_wait(barrier, 7)


def kmat_body(from_gram, two_over_h, src_ref, proj_ref, kern_out, zb_ref, mass_ref, *scratch):
    if not from_gram:
        tb, load_sem = scratch[-2:]
    (gbuf, sib_in, r_x1, r_y1, r_x2, r_y2, sq_parts, sq, z_in, z_all, kbuf,
     sib_send, sib_recv, rs_send, rs_recv, sq_send, sq_recv, z_send, z_recv, zb_send, zb_recv,
     k_send, k_recv, _, kern_ref, kern_sem) = scratch[:26]
    n_rows = kern_ref.shape[0]
    n_blk = n_rows // BLK
    ens, part, feat = lax.axis_index("ens"), lax.axis_index("part"), lax.axis_index("feat")
    x, core = feat // 2, lax.rem(feat, 2)

    def chip(rel):
        return lax.rem(part + rel // 2, 2), lax.rem(x + rel % 2, 2)

    def block(rel, flip):
        cy, cx = chip(rel)
        return cy * 4 + cx * 2 + lax.rem(core + flip, 2)

    def device(rel, flip):
        cy, cx = chip(rel)
        return (ens, cy, cx * 2 + lax.rem(core + flip, 2))

    me = block(0, 0)
    sibling, dev_x, dev_y = device(0, 1), device(1, 0), device(2, 0)
    others = [(rel, flip) for rel in (3, 1, 2, 0) for flip in (0, 1) if (rel, flip) != (0, 0)]

    def rcopy(src, dst, ssem, rsem, dev):
        return pltpu.make_async_remote_copy(src_ref=src, dst_ref=dst, send_sem=ssem, recv_sem=rsem,
                                            device_id=dev, device_id_type=MESH)

    def load(b):
        rs = pl.ds(b * BLK, BLK)
        return pltpu.make_async_copy(src_ref.at[rs, :], tb.at[rs, :], load_sem.at[b])

    if not from_gram:
        def load_all():
            for b in range(n_blk):
                load(b).start()

        greet(load_all)

    def z_cols(b):
        return proj_ref.at[:, pl.ds(pl.multiple_of(b * BLK, BLK), BLK)]

    def z_copy(i):
        rel, flip = others[i]
        return rcopy(z_cols(block(rel, flip)), z_in.at[me], z_send.at[i], z_recv.at[me], device(rel, flip))

    for i in range(len(others)):
        z_copy(i).start()
    z_own = pltpu.make_async_copy(z_cols(me), z_in.at[me], z_recv.at[me])
    z_own.start()

    def sib_copy(rel):
        src = src_ref.at[block(rel, 1)] if from_gram else gbuf.at[4 + rel]
        return rcopy(src, sib_in.at[rel], sib_send.at[rel], sib_recv.at[rel], sibling)

    lo, hi = 0, 1
    rs_copies = {
        "d_lo": rcopy(gbuf.at[3, lo], r_x1.at[0], rs_send.at[0], rs_recv.at[0], dev_x),
        "d_hi": rcopy(gbuf.at[3, hi], r_y1.at[0], rs_send.at[1], rs_recv.at[1], dev_y),
        "y_hi": rcopy(gbuf.at[2, hi], r_y1.at[1], rs_send.at[2], rs_recv.at[2], dev_y),
        "x_lo": rcopy(gbuf.at[1, lo], r_x1.at[1], rs_send.at[3], rs_recv.at[3], dev_x),
        "y_lo": rcopy(gbuf.at[2, lo], r_y2, rs_send.at[4], rs_recv.at[4], dev_y),
        "x_hi": rcopy(gbuf.at[1, hi], r_x2, rs_send.at[5], rs_recv.at[5], dev_x),
    }
    eye = (lax.broadcasted_iota(jnp.int32, (HALF, HALF), 0) == lax.broadcasted_iota(jnp.int32, (HALF, HALF), 1)).astype(F32)

    def merge(rel):
        sib_copy(rel).wait_recv()
        gbuf[rel] = src_ref[block(rel, 0)] + sib_in[rel]

    def first_sends(rel):
        for name in {3: ("d_lo", "d_hi"), 2: ("y_hi",), 1: ("x_lo",), 0: ()}[rel]:
            rs_copies[name].start()

    if from_gram:
        for rel in (3, 2, 1, 0):
            sib_copy(rel).start()
        for rel in (3, 2, 1, 0):
            merge(rel)
            first_sends(rel)
    else:
        def rows_at(at, n):
            return tb[pl.ds(pl.multiple_of(at, HALF), n), :]

        for b in range(n_blk):
            load(b).wait()

        @pl.loop(0, 8)
        def _(i):
            rel, own = 3 - i // 2, lax.rem(i, 2)
            cy, cx = lax.rem(part + rel // 2, 2), lax.rem(x + lax.rem(rel, 2), 2)
            b = cy * 4 + cx * 2 + lax.rem(core + 1 - own, 2)
            dst = rel + 4 * (1 - own)
            for h, rows_, cols_, piece in band_pieces(rows_at, b, n_blk):
                gbuf[dst, h, rows_, cols_] = piece
            across = rcopy(gbuf.at[4 + rel], sib_in.at[rel], sib_send.at[rel], sib_recv.at[rel], sibling)

            @pl.when(own == 0)
            def _():
                across.start()

            @pl.when(own == 1)
            def _():
                across.wait_recv()
                gbuf[rel] += sib_in[rel]
                for r in (3, 2, 1):
                    @pl.when(rel == r)
                    def _():
                        first_sends(r)

    for rel in range(4):
        cy, cx = chip(rel)
        for h in range(2):
            sq_parts[me, cy * 2 + cx, :, h * HALF:(h + 1) * HALF] = jnp.sum(gbuf[rel, h, :HALF, :HALF] * eye, axis=0, keepdims=True)

    def sq_copy(i):
        rel, flip = others[i]
        return rcopy(sq_parts.at[me], sq_parts.at[me], sq_send.at[i], sq_recv.at[me], device(rel, flip))

    def recv_from(buf, sem, rel, flip):
        b = block(rel, flip)
        return rcopy(buf.at[b], buf.at[b], sq_send.at[0], sem.at[b], sibling)

    for i in range(len(others)):
        sq_copy(i).start()

    rs_copies["d_lo"].wait_recv()
    gbuf[2, 0] += r_x1[0]
    rs_copies["y_lo"].start()
    rs_copies["d_hi"].wait_recv()
    gbuf[1, 1] += r_y1[0]
    rs_copies["x_hi"].start()

    z_own.wait()
    for rel, flip in others:
        recv_from(z_in, z_recv, rel, flip).wait_recv()
    z_sum = z_in[0]
    for b in range(1, n_blk):
        z_sum = z_sum + z_in[b]
    z_all[me] = z_sum.astype(BF16)

    def zb_copy(i):
        rel, flip = others[i]
        return rcopy(z_all.at[me], z_all.at[me], zb_send.at[i], zb_recv.at[me], device(rel, flip))

    for i in range(len(others)):
        zb_copy(i).start()
    for rel, flip in others:
        recv_from(sq_parts, sq_recv, rel, flip).wait_recv()
    for c in range(2):
        for q in range(4):
            s = sq_parts[c, q] + sq_parts[2 + c, q] + sq_parts[4 + c, q] + sq_parts[6 + c, q]
            b = 2 * q + c
            sq[:, b * BLK:(b + 1) * BLK] = s
            if b < WIDE // BLK:
                sq[:, n_rows + b * BLK:n_rows + (b + 1) * BLK] = s

    def sq_at(at, n):
        return sq[:, pl.ds(pl.multiple_of(at * HALF, HALF), n)]

    def upright(row):
        return jnp.sum(eye * row, axis=1, keepdims=True)

    def kernel_of(gram, col, row):
        return jnp.exp(-jnp.maximum(col + row - 2.0 * gram, 0.0) * (0.5 * two_over_h))

    def make_band(h, gram):
        idx = 2 * me + h
        row = sq_at(idx, WIDE)
        kbuf[idx, :HALF, :] = kernel_of(gram[:HALF], upright(row[:, :HALF]), row).astype(BF16)
        col = upright(sq_at(me, HALF))[h * (HALF // 2):(h + 1) * (HALF // 2)]
        kbuf[idx, HALF:, :] = fold(kernel_of(unfold(gram[HALF:]), col, sq_at(me + n_blk, HALF))).astype(BF16)

    slots = iter(range(14))
    sent = []

    def send_band(idx, dev):
        s = next(slots)
        cp = rcopy(kbuf.at[idx], kbuf.at[idx], k_send.at[s], k_recv.at[idx], dev)
        cp.start()
        sent.append(cp)

    def wait_band(idx):
        rcopy(kbuf.at[idx], kbuf.at[idx], k_send.at[0], k_recv.at[idx], sibling).wait_recv()

    def spread(b, h, unroll=False):
        idx = 2 * b + h
        row0 = pl.multiple_of(idx * HALF, HALF)
        kern_ref[pl.ds(row0, HALF), pl.ds(row0, HALF)] = kbuf[idx, :HALF, :HALF]

        def move(k):
            col0 = pl.multiple_of(lax.rem(idx + k, 2 * n_blk) * HALF, HALF)
            tile = kbuf[idx, :HALF, pl.ds(pl.multiple_of(k * HALF, HALF), HALF)]
            kern_ref[pl.ds(row0, HALF), pl.ds(col0, HALF)] = tile
            kern_ref[pl.ds(col0, HALF), pl.ds(row0, HALF)] = tile.T

        if unroll:
            for k in range(1, WIDE // HALF):
                move(k)
        else:
            pl.loop(1, WIDE // HALF)(move)

    def spread_far(b):
        tile = jnp.concatenate([unfold(kbuf[2 * b + h, HALF:, :].astype(F32)) for h in range(2)], axis=0)
        near = pl.ds(pl.multiple_of(b * HALF, HALF), HALF)
        away = pl.ds(pl.multiple_of((b + n_blk) * HALF, HALF), HALF)
        kern_ref[near, away] = tile.astype(BF16)
        kern_ref[away, near] = tile.T.astype(BF16)

    rs_copies["x_lo"].wait_recv()
    rs_copies["y_lo"].wait_recv()
    make_band(0, gbuf[0, 0] + (r_x1[1] + r_y2[...]))
    for dev in (dev_y, sibling):
        send_band(2 * me, dev)
    rs_copies["y_hi"].wait_recv()
    rs_copies["x_hi"].wait_recv()
    make_band(1, gbuf[0, 1] + (r_y1[1] + r_x2[...]))
    for dev in (dev_x, sibling):
        send_band(2 * me + 1, dev)
    send_band(2 * me, dev_x)
    send_band(2 * me + 1, dev_y)
    spread(me, 0)
    spread(me, 1)
    sib = block(0, 1)
    for h in range(2):
        wait_band(2 * sib + h)
        spread(sib, h)
    bx, by, bd = block(1, 0), block(2, 0), block(3, 0)
    wait_band(2 * by)
    send_band(2 * by, dev_x)
    send_band(2 * by, sibling)
    wait_band(2 * bx + 1)
    send_band(2 * bx + 1, dev_y)
    send_band(2 * bx + 1, sibling)
    spread(by, 0)
    spread(bx, 1)
    for b, h in ((bx, 0), (by, 1)):
        wait_band(2 * b + h)
        send_band(2 * b + h, sibling)
        spread(b, h)
    for rel, h in ((2, 0), (1, 1)):
        b = block(rel, 1)
        wait_band(2 * b + h)
        spread(b, h)
    for h in range(2):
        wait_band(2 * bd + h)
        send_band(2 * bd + h, sibling)
        spread(bd, h)
    for rel, h in ((1, 0), (2, 1)):
        b = block(rel, 1)
        wait_band(2 * b + h)
        spread(b, h)

    @pl.loop(0, 6)
    def _(i):
        rel = i // 2
        cy, cx = lax.rem(part + rel // 2, 2), lax.rem(x + lax.rem(rel, 2), 2)
        spread_far(cy * 4 + cx * 2 + lax.rem(i, 2))

    spread_far(bd)
    last = block(3, 1)
    for h in range(2):
        wait_band(2 * last + h)
        spread(last, h, True)
    spread_far(last)
    for rel, flip in others:
        recv_from(z_all, zb_recv, rel, flip).wait_recv()

    def put(b):
        rs = pl.ds(pl.multiple_of(b * BLK, BLK), BLK)
        return pltpu.make_async_copy(kern_ref.at[rs, :], kern_out.at[rs, :], kern_sem.at[b])

    @pl.loop(0, n_blk)
    def _(b):
        rs = pl.ds(pl.multiple_of(b * BLK, BLK), BLK)
        zb_ref[rs, :] = z_all[b].astype(F32).T.astype(BF16)
        mass_ref[rs, :] = jnp.sum(kern_ref[rs, :].astype(F32), axis=1, keepdims=True)
        put(b).start()

    @pl.loop(0, n_blk)
    def _(b):
        put(b).wait()

    for rel in range(4):
        sib_copy(rel).wait_send()
    for cp in rs_copies.values():
        cp.wait_send()
    for i in range(len(others)):
        z_copy(i).wait_send()
        sq_copy(i).wait_send()
        zb_copy(i).wait_send()
    for cp in sent:
        cp.wait_send()


def kmat_scratch(n_rows, rank, n_own):
    n_blk = n_rows // BLK
    dma = lambda *n: pltpu.SemaphoreType.DMA(n)
    return [
        pltpu.VMEM((n_own, 2, TALL, WIDE), F32), pltpu.VMEM((4, 2, TALL, WIDE), F32),
        pltpu.VMEM((2, TALL, WIDE), F32), pltpu.VMEM((2, TALL, WIDE), F32),
        pltpu.VMEM((TALL, WIDE), F32), pltpu.VMEM((TALL, WIDE), F32),
        pltpu.VMEM((8, 4, 1, BLK), F32), pltpu.VMEM((1, n_rows + WIDE), F32),
        pltpu.VMEM((n_blk, rank, BLK), F32), pltpu.VMEM((n_blk, rank, BLK), BF16),
        pltpu.VMEM((2 * n_blk, TALL, WIDE), BF16),
        dma(4), dma(4), dma(6), dma(6), dma(7), dma(8), dma(7), dma(8), dma(7), dma(8), dma(14), dma(16), dma(4),
        pltpu.VMEM((n_rows, n_rows), BF16), dma(n_blk)]


def kmat_shapes(n_rows, rank):
    return (jax.ShapeDtypeStruct((n_rows, n_rows), BF16), jax.ShapeDtypeStruct((n_rows, rank), BF16),
            jax.ShapeDtypeStruct((n_rows, 1), F32))


def kernel_matrix(tb, proj, two_over_h, collective_id):
    rank, n_rows = proj.shape
    return pl.pallas_call(
        functools.partial(kmat_body, False, two_over_h),
        out_shape=kmat_shapes(n_rows, rank), in_specs=[ANY, VMEM], out_specs=(ANY, VMEM, VMEM),
        scratch_shapes=kmat_scratch(n_rows, rank, 8) + [pltpu.VMEM(tb.shape, BF16), pltpu.SemaphoreType.DMA((n_rows // BLK,))],
        compiler_params=pltpu.CompilerParams(collective_id=collective_id, has_side_effects=True, vmem_limit_bytes=VMEM_LIMIT),
    )(tb, proj)


def opening_kernel(n_early, n_late, two_over_h, theta_ref, mean_ref, fact_ref, col_ref, late_own_ref, late_away_ref,
                   kern_out, zb_ref, mass_ref, gram, proj, *scratch):
    greet()
    exchange_body(n_early, n_late, theta_ref, mean_ref, fact_ref, col_ref, late_own_ref, late_away_ref, gram, proj, *scratch[:12])
    kmat_body(True, two_over_h, gram, proj, kern_out, zb_ref, mass_ref, *scratch[12:])


def opening(theta, mean, fact_t, two_over_h, n_early, n_late):
    rows, feat = theta.shape
    rank = fact_t.shape[0]
    width = feat // 2
    n_rows = rows * 2
    cw = width // (n_early + n_late)
    dma = lambda *n: pltpu.SemaphoreType.DMA(n)
    return pl.pallas_call(
        functools.partial(opening_kernel, n_early, n_late, two_over_h),
        out_shape=(jax.ShapeDtypeStruct((n_rows, n_early * cw), F32),
                   jax.ShapeDtypeStruct((rows, n_late * cw), F32),
                   jax.ShapeDtypeStruct((rows, n_late * cw), F32)) + kmat_shapes(n_rows, rank),
        in_specs=[ANY, VMEM, VMEM], out_specs=(ANY, ANY, ANY, ANY, VMEM, VMEM),
        scratch_shapes=[
            pltpu.VMEM((n_rows // BLK, 2, TALL, WIDE), F32), pltpu.VMEM((rank, n_rows), F32),
            pltpu.VMEM((n_rows, cw), F32), pltpu.VMEM((n_rows, cw), BF16), pltpu.VMEM((rows, cw), F32),
            pltpu.VMEM((n_late, rows, cw), BF16), pltpu.VMEM((n_late, rows, cw), BF16),
            dma(n_early), dma(n_early), dma(n_late), dma(n_late),
            pltpu.SemaphoreType.DMA, pltpu.SemaphoreType.DMA, pltpu.SemaphoreType.DMA] + kmat_scratch(n_rows, rank, 4),
        compiler_params=pltpu.CompilerParams(collective_id=0, has_side_effects=True, vmem_limit_bytes=VMEM_LIMIT),
        name="opening",
    )(theta, mean, fact_t)


def solution(mesh):
    part_size = mesh.shape["part"]
    feat_size = mesh.shape["feat"]

    def local_steps(theta, prec_loc, mean_loc, factor_loc):
        rows, feat_loc = theta.shape
        n_total = rows * part_size
        feat_total = feat_loc * feat_size
        width = feat_loc // part_size
        kern_width = 2.0 * feat_total / math.log(n_total)
        step_size = 0.15 * n_total * feat_total / math.log(n_total)
        consts = (1.0 / n_total, 2.0 / kern_width, step_size)
        part = lax.axis_index("part")
        pos = part.astype(jnp.int32).reshape(1)
        params = (mean_loc.reshape(1, feat_loc), prec_loc.reshape(1, feat_loc), factor_loc.T)
        shared = 2 * BLK
        chunks = [(shared, HALF)] + [(at, 2 * BLK) for at in range(2 * shared, width, 2 * BLK)] + [(shared + BLK, BLK), (shared + HALF, HALF)]
        swap = [(0, 1), (1, 0)]
        late = 3 * BLK
        early = width - late

        cur, late_own, late_away, kern, zb, mass = opening(theta, params[0], params[2], consts[1], early // BLK, late // BLK)
        recv = lax.ppermute(late_away, "part", swap)
        new, tb, proj = update(consts, cur, kern, mass, zb, params, width, 0, early, False)
        cur, tb, proj = update(consts, (late_own, recv), kern, mass, zb, params, width, early, width, False, (tb, proj, new))
        kern, zb, mass = kernel_matrix(tb, proj, consts[1], 2)
        both, tb, proj = update(consts, cur, kern, mass, zb, params, width, 0, shared, True)
        foreign = lax.ppermute(both, "part", swap)
        cur, tb, proj = update(consts, cur, kern, mass, zb, params, width, shared, width, False, (tb, proj))
        kern, zb, mass = kernel_matrix(tb, proj, consts[1], 3)
        out = None
        received = []
        for i, (start, tile) in enumerate(chunks):
            if i == 0:
                send = send_update(consts, pos, cur, kern, mass, zb, *params, start, tile)
            else:
                out, send = last_update(consts, pos, cur, kern, mass, zb, *params, out, start, tile)
            received.append(lax.ppermute(send, "part", swap))
        out = own_update(consts, pos, cur, kern, mass, zb, *params, out, False, chunks[0][0], chunks[0][1], chunks[0][1])
        out = own_update(consts, pos, both, kern, mass, zb, *params, out, False, 0, shared, BLK)
        out = own_update(consts, pos, foreign, kern, mass, zb, *params, out, True, 0, shared, BLK)
        for (start, tile), recv in zip(chunks, received):
            out = place(pos, recv, out, start)
        return out

    row_spec = P(("ens", "part"), "feat")
    vec_spec = P(("ens", "feat"))
    fac_spec = P(("ens", "feat"), None)
    return jax.shard_map(local_steps, mesh=mesh, in_specs=(row_spec, vec_spec, vec_spec, fac_spec), out_specs=row_spec, check_vma=False)
```
